32 devices in a mesh: dp: 2 (over x), tp: 4 (over z), sp: 4 (over y, core).
Axes of the slice: x: 2, y: 2, z: 4, core: 2. Of those that a mesh axis runs over, the one named last changes fastest.
Arguments:
- x_in: bfloat16 [16384, 2560], P(('dp', 'sp')), parts along dimension 0
- w_z: bfloat16 [2560, 5120], P(None, 'tp')
- w_x: bfloat16 [2560, 5120], P(None, 'tp')
- w_bc: bfloat16 [2560, 256], replicated
- w_dt: bfloat16 [2560, 80], P(None, 'tp')
- a_neg: float32 [80], P('tp')
- dt_bias: float32 [80], P('tp')
- d_skip: float32 [80], P('tp')
- w_out: bfloat16 [5120, 2560], P('tp')
Outputs:
- output: bfloat16 [16384, 2560], P(('dp', 'sp', 'tp')), parts along dimension 0
There are 2 independent parts. The reference program is written for one: setup_inputs(seed, part) draws one part's arguments, and reference() takes and returns one part's arrays. A program takes and returns all parts, laid end to end along the dimension named above; an argument that names none is the same for every part.
All inputs are finite; a program needn't handle non-finite values.
Results may differ from the reference program's by a relative error of at most 0.0112365.
Values are sent between devices in bfloat16 or wider.
A program may use at most 1 GiB of HBM per device.

```python
import jax
import jax.numpy as jnp
from jax import lax

D_MODEL = 2560
N_HEADS = 80
HEAD_DIM = 64
D_STATE = 128
TOKENS_DEV = 2048
SEQ_DEVS = 4
PIECE_LEN = 64
D_INNER = N_HEADS * HEAD_DIM
SEQ_LEN = SEQ_DEVS * TOKENS_DEV


def setup_inputs(seed: int = 0, part: int = 0) -> dict:
    keys = jax.random.split(jax.random.key(seed), 9)
    x_key = jax.random.fold_in(keys[0], part)
    x_in = jax.random.normal(x_key, (SEQ_LEN, D_MODEL), jnp.float32)
    w_z = jax.random.normal(keys[1], (D_MODEL, D_INNER), jnp.float32) * D_MODEL ** -0.5
    w_x = jax.random.normal(keys[2], (D_MODEL, D_INNER), jnp.float32) * D_MODEL ** -0.5
    bc_scale = D_MODEL ** -0.5 * (D_STATE * TOKENS_DEV) ** -0.25
    w_bc = jax.random.normal(keys[3], (D_MODEL, 2 * D_STATE), jnp.float32) * bc_scale
    w_dt = jax.random.normal(keys[4], (D_MODEL, N_HEADS), jnp.float32) * (0.5 * D_MODEL ** -0.5)
    a_neg = -jax.random.uniform(keys[5], (N_HEADS,), jnp.float32, minval=0.4, maxval=1.6) / TOKENS_DEV
    dt_bias = jax.random.uniform(keys[6], (N_HEADS,), jnp.float32, minval=-1.0, maxval=1.0)
    d_skip = jax.random.uniform(keys[7], (N_HEADS,), jnp.float32, minval=0.5, maxval=1.5)
    w_out = jax.random.normal(keys[8], (D_INNER, D_MODEL), jnp.float32) * D_INNER ** -0.5
    return dict(x_in=x_in.astype(jnp.bfloat16), w_z=w_z.astype(jnp.bfloat16), w_x=w_x.astype(jnp.bfloat16), w_bc=w_bc.astype(jnp.bfloat16), w_dt=w_dt.astype(jnp.bfloat16), a_neg=a_neg, dt_bias=dt_bias, d_skip=d_skip, w_out=w_out.astype(jnp.bfloat16))


def ssd_scan(x_heads, dt_step, log_a, b_mat, c_mat):
    n_pieces = SEQ_LEN // PIECE_LEN
    pieces = (x_heads.reshape(n_pieces, PIECE_LEN, N_HEADS, HEAD_DIM), dt_step.reshape(n_pieces, PIECE_LEN, N_HEADS), log_a.reshape(n_pieces, PIECE_LEN, N_HEADS), b_mat.reshape(n_pieces, PIECE_LEN, D_STATE), c_mat.reshape(n_pieces, PIECE_LEN, D_STATE))
    positions = jnp.arange(PIECE_LEN)
    causal = (positions[:, None] >= positions[None, :])[:, :, None]

    def piece_step(state, piece):
        x_piece, dt_piece, la_piece, b_piece, c_piece = piece
        cum_log = jnp.cumsum(la_piece, axis=0)
        decay = jnp.where(causal, jnp.exp(jnp.minimum(cum_log[:, None, :] - cum_log[None, :, :], 0.0)), 0.0)
        gram = jnp.einsum('tn,sn->ts', c_piece, b_piece)
        weights = gram[:, :, None] * decay * dt_piece[None, :, :]
        y_piece = jnp.einsum('tsh,shp->thp', weights, x_piece)
        y_piece = y_piece + jnp.exp(cum_log)[:, :, None] * jnp.einsum('hpn,tn->thp', state, c_piece)
        to_end = jnp.exp(cum_log[-1][None, :] - cum_log) * dt_piece
        new_state = jnp.exp(cum_log[-1])[:, None, None] * state + jnp.einsum('sh,shp,sn->hpn', to_end, x_piece, b_piece)
        return new_state, y_piece

    init = jnp.zeros((N_HEADS, HEAD_DIM, D_STATE), jnp.float32)
    _, y_all = lax.scan(piece_step, init, pieces)
    return y_all.reshape(SEQ_LEN, N_HEADS, HEAD_DIM)


def reference(x_in, w_z, w_x, w_bc, w_dt, a_neg, dt_bias, d_skip, w_out):
    z_gate = jnp.dot(x_in, w_z, preferred_element_type=jnp.float32).astype(jnp.bfloat16)
    x_proj = jnp.dot(x_in, w_x, preferred_element_type=jnp.float32).astype(jnp.bfloat16)
    bc_val = jnp.dot(x_in, w_bc, preferred_element_type=jnp.float32).astype(jnp.bfloat16).astype(jnp.float32)
    dt_step = jax.nn.softplus(jnp.dot(x_in, w_dt, preferred_element_type=jnp.float32) + dt_bias)
    log_a = dt_step * a_neg
    x_heads = x_proj.astype(jnp.float32).reshape(SEQ_LEN, N_HEADS, HEAD_DIM)
    b_mat = bc_val[:, :D_STATE]
    c_mat = bc_val[:, D_STATE:]
    y_fwd = ssd_scan(x_heads, dt_step, log_a, b_mat, c_mat)
    y_bwd = ssd_scan(x_heads[::-1], dt_step[::-1], log_a[::-1], b_mat[::-1], c_mat[::-1])[::-1]
    y_sum = y_fwd + y_bwd + 2.0 * d_skip[:, None] * x_heads
    gated = (y_sum.reshape(SEQ_LEN, D_INNER) * jax.nn.silu(z_gate.astype(jnp.float32))).astype(jnp.bfloat16)
    mixed = jnp.dot(gated, w_out, preferred_element_type=jnp.float32)
    return (x_in.astype(jnp.float32) + mixed).astype(jnp.bfloat16)
```

```python
import functools

import jax
import jax.numpy as jnp
from jax import lax
from jax.experimental import pallas as pl
from jax.experimental.pallas import tpu as pltpu
from jax.sharding import PartitionSpec as P


CHUNK = 128
LANES = 128
SLOT = 32
LOG2E = 1.4426950408889634
F32 = jnp.float32
BF16 = jnp.bfloat16


def prep_kernel(x_ref, wbc_ref, wdt_ref, par_ref, bc_ref, cols_ref, rows_ref, log_ref):
    x_val = x_ref[...]
    bc_ref[...] = jnp.dot(x_val, wbc_ref[...], preferred_element_type=F32).astype(BF16)
    raw = lax.dot_general(x_val, wdt_ref[...], (((1,), (1,)), ((), ())), preferred_element_type=F32) + par_ref[0:1, :]
    dt_val = jnp.maximum(raw, 0.0) + jnp.log1p(jnp.exp(-jnp.abs(raw)))
    la_val = jnp.maximum(dt_val * par_ref[1:2, :] * LOG2E, -1024.0)
    row = lax.broadcasted_iota(jnp.int32, (CHUNK, CHUNK), 0)
    lane = lax.broadcasted_iota(jnp.int32, (CHUNK, CHUNK), 1)
    tri = jnp.where(row >= lane, 1.0, 0.0).astype(F32)

    @pl.when(pl.program_id(0) == 0)
    def _():
        log_ref[...] = jnp.zeros_like(log_ref)

    for c in range(x_val.shape[0] // CHUNK):
        part = slice(c * CHUNK, (c + 1) * CHUNK)
        la_c = la_val[part, :]
        cum = jnp.dot(tri, la_c, preferred_element_type=F32, precision=lax.Precision.HIGHEST)
        col = jnp.where(lane < SLOT, cum, jnp.where(lane < 2 * SLOT, cum - la_c, dt_val[part, :]))
        cols_ref[part, :] = col
        rows_ref[:, part] = col.T
        log_ref[...] += col[CHUNK - 1:CHUNK, :]


def proj_kernel(n_tiles, x_ref, *refs):
    o_ref = refs[-1]
    x_val = x_ref[...]
    for i in range(n_tiles):
        o_ref[:, i * 256:(i + 1) * 256] = jnp.dot(x_val, refs[i][...], preferred_element_type=F32).astype(BF16)


def sum_kernel(n_tiles, n_pieces, acc_ref, *refs):
    o_ref = refs[-1]
    total = acc_ref[...].astype(F32)
    for i in range(n_pieces):
        g_ref, w_refs = refs[sum(n_tiles[:i]) + i], refs[sum(n_tiles[:i]) + i + 1:sum(n_tiles[:i + 1]) + i + 1]
        for t in range(n_tiles[i]):
            total = total + jnp.dot(g_ref[:, t * 256:(t + 1) * 256], w_refs[t][...], preferred_element_type=F32)
    o_ref[...] = total.astype(o_ref.dtype)


def pair_cols(cols, head, low):
    first = jnp.broadcast_to(cols[:, head:head + 1], (cols.shape[0], LANES))
    second = jnp.broadcast_to(cols[:, head + 1:head + 2], (cols.shape[0], LANES))
    return first, second, jnp.where(low, first, second)


def state_kernel(first_head, n_pairs, u_ref, bc_ref, cols_ref, after_ref, gloc_ref, suf_ref, sf_ref, sb_ref, g_acc, f_acc, suf_acc, v_buf):
    step = pl.program_id(0)
    width = n_pairs * LANES

    @pl.when(step == 0)
    def _():
        g_acc[...] = jnp.zeros_like(g_acc)
        f_acc[...] = jnp.zeros_like(f_acc)
        suf_acc[...] = jnp.zeros_like(suf_acc)

    cols = cols_ref[...]
    low = lax.broadcasted_iota(jnp.int32, (CHUNK, LANES), 1) < LANES // 2
    suffix = suf_acc[...]
    suf_ref[0] = suffix
    gloc_ref[0] = g_acc[...]
    totals = []
    for p in range(n_pairs):
        head = first_head + 2 * p
        part = slice(p * LANES, (p + 1) * LANES)
        cum = pair_cols(cols, head, low)[2]
        exc = pair_cols(cols, SLOT + head, low)[2]
        dt_val = pair_cols(cols, 2 * SLOT + head, low)[2]
        scaled = u_ref[:, part].astype(F32) * dt_val
        total = cum[CHUNK - 1:CHUNK, :]
        totals.append(total)
        v_buf[:, part] = (scaled * jnp.exp2(exc)).astype(BF16)
        v_buf[:, slice(width + p * LANES, width + (p + 1) * LANES)] = (scaled * jnp.exp2(total + suffix[0:1, part] - cum)).astype(BF16)
    total = jnp.concatenate(totals, axis=1)
    sums = lax.dot_general(bc_ref[:, :LANES], v_buf[...], (((0,), (0,)), ((), ())), preferred_element_type=F32)
    g_acc[...] = g_acc[...] * jnp.exp2(total) + sums[:, :width]
    f_acc[...] += sums[:, width:]
    suf_acc[...] = suffix + total

    @pl.when(step == pl.num_programs(0) - 1)
    def _():
        sf_ref[...] = f_acc[...].astype(BF16)
        sb_ref[...] = g_acc[...].astype(BF16)


def out_kernel(first_head, n_pairs, u_ref, z_ref, bc_ref, cols_ref, rows_ref, gloc_ref, suf_ref, r1_ref, r2_ref, r3_ref, mix_ref, after_ref, g_ref, f_acc, hb_acc, wide, v_buf):
    step = pl.program_id(0)

    @pl.when(step == 0)
    def _():
        for p in range(n_pairs):
            wide[:, p * LANES:(p + 1) * LANES] = pair_cols(mix_ref[...], first_head + 2 * p, lax.broadcasted_iota(jnp.int32, (8, LANES), 1) < LANES // 2)[2]
        got = [r[...].astype(F32) for r in (r1_ref, r2_ref, r3_ref)]
        f_acc[...] = sum(got[s] * wide[s:s + 1, :] for s in range(3))
        hb_acc[...] = sum(got[s] * wide[3 + s:4 + s, :] for s in range(3))

    cols = cols_ref[...]
    row = lax.broadcasted_iota(jnp.int32, (CHUNK, LANES), 0)
    lane = lax.broadcasted_iota(jnp.int32, (CHUNK, LANES), 1)
    low = lane < LANES // 2
    b_val = bc_ref[:, :LANES]
    c_val = bc_ref[:, LANES:]
    gram = lax.dot_general(c_val, b_val, (((1,), (1,)), ((), ())), preferred_element_type=F32)
    gram = jnp.where(row == lane, 2.0 * gram, gram)
    back = (gloc_ref[0] + hb_acc[...] * jnp.exp2(suf_ref[0, 0:1, :])).astype(BF16)
    y_fwd = jnp.dot(c_val, f_acc[...].astype(BF16), preferred_element_type=F32)
    y_bwd = jnp.dot(c_val, back, preferred_element_type=F32)
    totals = []
    for p in range(n_pairs):
        head = first_head + 2 * p
        part = slice(p * LANES, (p + 1) * LANES)
        cum0, cum1, cum = pair_cols(cols, head, low)
        exc0, exc1, exc = pair_cols(cols, SLOT + head, low)
        dt_val = pair_cols(cols, 2 * SLOT + head, low)[2]
        u_val = u_ref[:, part].astype(F32)
        scaled = u_val * dt_val
        m0 = jnp.exp2(jnp.minimum(cum0 - rows_ref[head:head + 1, :], rows_ref[SLOT + head:SLOT + head + 1, :] - exc0)) * gram
        m1 = jnp.exp2(jnp.minimum(cum1 - rows_ref[head + 1:head + 2, :], rows_ref[SLOT + head + 1:SLOT + head + 2, :] - exc1)) * gram
        mix = jnp.concatenate([m0.astype(BF16), m1.astype(BF16)], axis=1)
        rhs = jnp.concatenate([jnp.where(low, scaled, 0.0).astype(BF16), jnp.where(low, 0.0, scaled).astype(BF16)], axis=0)
        total = cum[CHUNK - 1:CHUNK, :]
        totals.append(total)
        y_val = jnp.dot(mix, rhs, preferred_element_type=F32)
        y_val = y_val + jnp.exp2(cum) * y_fwd[:, part] + jnp.exp2(total - exc) * y_bwd[:, part]
        y_val = y_val + wide[6:7, part] * u_val
        z_val = z_ref[:, part].astype(F32)
        g_ref[:, part] = (y_val * (z_val * jax.nn.sigmoid(z_val))).astype(BF16)
        v_buf[:, part] = (scaled * jnp.exp2(total - cum)).astype(BF16)
    total = jnp.concatenate(totals, axis=1)
    sums = lax.dot_general(b_val, v_buf[...], (((0,), (0,)), ((), ())), preferred_element_type=F32)
    f_acc[...] = f_acc[...] * jnp.exp2(total) + sums


def params():
    return pltpu.CompilerParams(dimension_semantics=("arbitrary",), vmem_limit_bytes=62 << 20)


def cost(flops, moved):
    return pl.CostEstimate(flops=int(flops), bytes_accessed=int(moved), transcendentals=0)


ANY = pl.BlockSpec(memory_space=pl.ANY)


def prep(x_blk, w_bc, w_dt_rows, par):
    tokens, d_model = x_blk.shape
    tile = min(512, tokens)
    whole = lambda a: pl.BlockSpec(a.shape, lambda i: (0, 0))
    return pl.pallas_call(
        prep_kernel,
        grid=(tokens // tile,),
        in_specs=[pl.BlockSpec((tile, d_model), lambda i: (i, 0)), whole(w_bc), whole(w_dt_rows), whole(par)],
        out_specs=[pl.BlockSpec((tile, 2 * LANES), lambda i: (i, 0)), pl.BlockSpec((tile, LANES), lambda i: (i, 0)), pl.BlockSpec((LANES, tile), lambda i: (0, i)), pl.BlockSpec((8, LANES), lambda i: (0, 0))],
        out_shape=[jax.ShapeDtypeStruct((tokens, 2 * LANES), BF16), jax.ShapeDtypeStruct((tokens, LANES), F32), jax.ShapeDtypeStruct((LANES, tokens), F32), jax.ShapeDtypeStruct((8, LANES), F32)],
        compiler_params=params(),
        cost_estimate=cost(2 * tokens * d_model * 512, 2 * tokens * d_model),
        name="prep",
    )(x_blk, w_bc, w_dt_rows, par)


def project(x_blk, w, first_tile, n_tiles, after):
    tokens, d_model = x_blk.shape
    tile = min(512, tokens)
    width = 256 * n_tiles
    w_specs = [pl.BlockSpec((d_model, 256), functools.partial(lambda t, i: (0, t), first_tile + t)) for t in range(n_tiles)]
    return pl.pallas_call(
        functools.partial(proj_kernel, n_tiles),
        grid=(tokens // tile,),
        in_specs=[pl.BlockSpec((tile, d_model), lambda i: (i, 0))] + w_specs + [ANY],
        out_specs=pl.BlockSpec((tile, width), lambda i: (i, 0)),
        out_shape=jax.ShapeDtypeStruct((tokens, width), BF16),
        compiler_params=params(),
        cost_estimate=cost(2 * tokens * d_model * width, 2 * tokens * d_model),
        name="project",
    )(x_blk, *([w] * n_tiles), after)


def add_products(acc, pieces, out_dtype):
    rows, d_model = acc.shape
    tile = min(512, d_model)
    n_tiles = [g.shape[1] // 256 for g, _, _ in pieces]
    specs, args = [pl.BlockSpec((rows, tile), lambda i: (0, i))], [acc]
    for (g, w, tile0), count in zip(pieces, n_tiles):
        specs.append(pl.BlockSpec(g.shape, lambda i: (0, 0)))
        specs += [pl.BlockSpec((256, tile), functools.partial(lambda t, i: (t, i), tile0 + t)) for t in range(count)]
        args += [g] + [w] * count
    return pl.pallas_call(
        functools.partial(sum_kernel, n_tiles, len(pieces)),
        grid=(d_model // tile,),
        in_specs=specs,
        out_specs=pl.BlockSpec((rows, tile), lambda i: (0, i)),
        out_shape=jax.ShapeDtypeStruct((rows, d_model), out_dtype),
        compiler_params=params(),
        cost_estimate=cost(2 * rows * d_model * 256 * sum(n_tiles), 2 * rows * d_model),
        name="add_products",
    )(*args)


def chunk_states(u, bc, cols, after, first_head, n_pairs):
    tokens, width = u.shape
    n_chunks = tokens // CHUNK
    last = n_chunks - 1
    tok = lambda w: pl.BlockSpec((CHUNK, w), lambda i: (last - i, 0))
    whole = pl.BlockSpec((LANES, width), lambda i: (0, 0))
    return pl.pallas_call(
        functools.partial(state_kernel, first_head, n_pairs),
        grid=(n_chunks,),
        in_specs=[tok(width), tok(2 * LANES), tok(LANES), ANY],
        out_specs=[pl.BlockSpec((1, LANES, width), lambda i: (last - i, 0, 0)), pl.BlockSpec((1, 8, width), lambda i: (last - i, 0, 0)), whole, whole],
        out_shape=[jax.ShapeDtypeStruct((n_chunks, LANES, width), F32), jax.ShapeDtypeStruct((n_chunks, 8, width), F32), jax.ShapeDtypeStruct((LANES, width), BF16), jax.ShapeDtypeStruct((LANES, width), BF16)],
        scratch_shapes=[pltpu.VMEM((LANES, width), F32), pltpu.VMEM((LANES, width), F32), pltpu.VMEM((8, width), F32), pltpu.VMEM((CHUNK, 2 * width), BF16)],
        compiler_params=params(),
        cost_estimate=cost(16 * tokens * width * 256, 8 * tokens * width),
        name="states",
    )(u, bc, cols, after)


def chunk_outputs(u, z, bc, cols, rows, gloc, suf, got, mix, after, first_head, n_pairs):
    tokens, width = u.shape
    n_chunks = tokens // CHUNK
    tok = lambda w: pl.BlockSpec((CHUNK, w), lambda i: (i, 0))
    state = pl.BlockSpec((LANES, width), lambda i: (0, 0))
    return pl.pallas_call(
        functools.partial(out_kernel, first_head, n_pairs),
        grid=(n_chunks,),
        in_specs=[tok(width), tok(width), tok(2 * LANES), tok(LANES), pl.BlockSpec((2 * SLOT, CHUNK), lambda i: (0, i)), pl.BlockSpec((1, LANES, width), lambda i: (i, 0, 0)), pl.BlockSpec((1, 8, width), lambda i: (i, 0, 0)), state, state, state, pl.BlockSpec((8, LANES), lambda i: (0, 0)), ANY],
        out_specs=tok(width),
        out_shape=jax.ShapeDtypeStruct((tokens, width), BF16),
        scratch_shapes=[pltpu.VMEM((LANES, width), F32), pltpu.VMEM((LANES, width), F32), pltpu.VMEM((8, width), F32), pltpu.VMEM((CHUNK, width), BF16)],
        compiler_params=params(),
        cost_estimate=cost(24 * tokens * width * 256, 8 * tokens * width),
        name="outputs",
    )(u, z, bc, cols, rows, gloc, suf, *got, mix, after)


def solution(mesh):
    n_tp, n_sp, n_dp = mesh.shape['tp'], mesh.shape['sp'], mesh.shape['dp']

    def swap(val, axis, slot):
        return lax.ppermute(val, axis, [(i, i ^ slot) for i in range(4)])

    def later(vals, after):
        return list(lax.optimization_barrier((*vals, after)))[:-1]

    def device_fn(x_blk, w_z, w_x, w_bc, w_dt, a_neg, dt_bias, d_skip, w_out):
        tokens, _ = x_blk.shape
        heads = a_neg.shape[0]
        head_dim = w_x.shape[1] // heads
        rows_out = tokens // n_tp
        tp_index = lax.axis_index('tp')
        sp_index = lax.axis_index('sp')

        piece_rows = w_out.shape[0] // (n_dp * n_sp)
        mine = lax.axis_index('dp') * n_sp + sp_index
        piece = lax.dynamic_slice_in_dim(w_out, mine * piece_rows, piece_rows, axis=0)
        right = lax.ppermute(piece, 'tp', [(0, 1), (1, 2), (2, 3)])
        left = lax.ppermute(piece, 'tp', [(1, 0), (2, 1), (3, 2)])

        w_dt_rows = jnp.pad(w_dt.T, ((0, SLOT - heads), (0, 0)))
        w_dt_rows = jnp.concatenate([w_dt_rows] * 3 + [jnp.zeros_like(w_dt_rows)], axis=0)
        spread = lambda v: jnp.concatenate([jnp.pad(v, (0, SLOT - heads))] * 4)[None, :]
        par = jnp.concatenate([spread(dt_bias), spread(a_neg), jnp.zeros((6, LANES), F32)], axis=0)
        bc, cols, rows, block_log = prep(x_blk, w_bc, w_dt_rows, par)

        logs = [swap(block_log, 'sp', s) for s in (1, 2, 3)]
        w_fwd, w_bwd = [], []
        for s in (1, 2, 3):
            peer = sp_index ^ s
            between = jnp.zeros((1, LANES), F32)
            for o in (1, 2, 3):
                other = sp_index ^ o
                inside = (other > jnp.minimum(peer, sp_index)) & (other < jnp.maximum(peer, sp_index))
                between = between + jnp.where(inside, logs[o - 1][:1], 0.0)
            decay = jnp.exp2(between)
            w_fwd.append(jnp.where(peer < sp_index, decay, 0.0))
            w_bwd.append(jnp.where(peer > sp_index, decay, 0.0))
        mix = jnp.concatenate(w_fwd + w_bwd + [spread(2.0 * d_skip), jnp.zeros((1, LANES), F32)], axis=0)

        n_tiles = w_x.shape[1] // 256
        first = n_tiles * 2 // 5
        (t_a, n_a), (t_b, n_b) = (0, first), (first, n_tiles - first)
        head_b = first * 256 // head_dim

        def exchange(s_fwd, s_bwd):
            return [swap(jnp.where(sp_index < (sp_index ^ s), s_fwd, s_bwd), 'sp', s) for s in (1, 2, 3)]

        def send(g):
            rows_of = lambda who: lax.dynamic_slice_in_dim(g, who * rows_out, rows_out, axis=0)
            return [rows_of(tp_index)] + [swap(rows_of(tp_index ^ s), 'tp', s) for s in (1, 2, 3)]

        plane = lambda v: lax.all_gather(v, ('dp', 'sp'), tiled=True)

        u_a = project(x_blk, w_x, t_a, n_a, block_log)
        gloc_a, suf_a, s_fwd, s_bwd = chunk_states(u_a, bc, cols, block_log, 0, 2 * n_a)
        got_a = exchange(s_fwd, s_bwd)
        right, left = later((right, left), s_fwd)
        one = jnp.where(tp_index % 2 == 1, right, left)
        right2 = lax.ppermute(right, 'tp', [(1, 2), (2, 3)])
        left2 = lax.ppermute(left, 'tp', [(1, 0), (2, 1)])
        w_one = plane(one)
        z_a = project(x_blk, w_z, t_a, n_a, one)
        u_b = project(x_blk, w_x, t_b, n_b, z_a)
        right2, left2 = later((right2, left2), u_b)
        two = jnp.where(tp_index >= 2, right2, left2)
        right3 = lax.ppermute(right2, 'tp', [(2, 3)])
        left3 = lax.ppermute(left2, 'tp', [(1, 0)])
        w_two = plane(two)
        g_a = chunk_outputs(u_a, z_a, bc, cols, rows, gloc_a, suf_a, got_a, mix, two, 0, 2 * n_a)
        got_g_a = send(g_a)
        gloc_b, suf_b, s_fwd, s_bwd = chunk_states(u_b, bc, cols, g_a, head_b, 2 * n_b)
        got_b = exchange(s_fwd, s_bwd)
        z_b = project(x_blk, w_z, t_b, n_b, s_fwd)
        right3, left3 = later((right3, left3), z_b)
        three = jnp.where(tp_index == 0, left3, jnp.where(tp_index == 1, left, jnp.where(tp_index == 2, right, right3)))
        w_three = plane(three)
        g_b = chunk_outputs(u_b, z_b, bc, cols, rows, gloc_b, suf_b, got_b, mix, three, head_b, 2 * n_b)
        got_g_b = send(g_b)

        own = lax.dynamic_slice_in_dim(x_blk, tp_index * rows_out, rows_out, axis=0)
        total = add_products(own, [(got_g_a[0], w_out, t_a), (got_g_b[0], w_out, t_b)], F32)
        total = add_products(total, [(got_g_a[1], w_one, t_a), (got_g_a[2], w_two, t_a)], F32)
        total = add_products(total, [(got_g_a[3], w_three, t_a), (got_g_b[1], w_one, t_b)], F32)
        return add_products(total, [(got_g_b[2], w_two, t_b), (got_g_b[3], w_three, t_b)], BF16)

    in_specs = (P(('dp', 'sp'), None), P(None, 'tp'), P(None, 'tp'), P(None, None), P(None, 'tp'), P('tp'), P('tp'), P('tp'), P('tp', None))
    out_specs = P(('dp', 'sp', 'tp'), None)
    return jax.shard_map(device_fn, mesh=mesh, in_specs=in_specs, out_specs=out_specs, check_vma=False)
```

```python
import functools

import jax
import jax.numpy as jnp
from jax import lax
from jax.experimental import pallas as pl
from jax.experimental.pallas import tpu as pltpu
from jax.sharding import PartitionSpec as P


CHUNK = 128
LANES = 128
SLOT = 32
STATE_CHUNKS = 4
OUT_CHUNKS = 2
OUT_AHEAD = 2
F32 = jnp.float32
BF16 = jnp.bfloat16


def split3(val, lane, last):
    first = val.astype(BF16).astype(F32)
    rest = val - first
    second = rest.astype(BF16).astype(F32)
    third = rest - second
    return jnp.where(lane < SLOT, first, jnp.where(lane < 2 * SLOT, second, jnp.where(lane < 3 * SLOT, third, last))).astype(BF16)


def prep_kernel(n_tiles, x_ref, wbc_ref, wdt_ref, bias_ref, a_ref, *refs):
    bc_ref, cum_ref, nexc_ref, dt_ref, tail1_ref, tail2_ref, log_ref, u_ref, w_buf, par, pick = refs[n_tiles:]
    heads = bias_ref.shape[1]
    row = lax.broadcasted_iota(jnp.int32, (CHUNK, LANES), 0)
    lane = lax.broadcasted_iota(jnp.int32, (CHUNK, LANES), 1)

    @pl.when(pl.program_id(0) == 0)
    def _():
        log_ref[...] = jnp.zeros_like(log_ref)
        w_buf[...] = jnp.zeros_like(w_buf)
        par[...] = jnp.zeros_like(par)
        for k in range(3):
            w_buf[k * SLOT:k * SLOT + heads, :] = wdt_ref[...]
            par[0:1, k * SLOT:k * SLOT + heads] = bias_ref[...]
            par[1:2, k * SLOT:k * SLOT + heads] = a_ref[...]
        out_row = lax.broadcasted_iota(jnp.int32, pick.shape, 0)
        term = lax.broadcasted_iota(jnp.int32, pick.shape, 1)
        head, which = out_row // 16, out_row % 16
        pick[...] = jnp.where((which < 3) & (term == which * SLOT + head), -1.0, 0.0).astype(BF16)

    x_val = x_ref[...]
    raw = lax.dot_general(x_val, w_buf[...], (((1,), (1,)), ((), ())), preferred_element_type=F32) + par[0:1, :]
    bc_ref[...] = jnp.dot(x_val, wbc_ref[...], preferred_element_type=F32).astype(BF16)
    dt_val = jnp.maximum(raw, 0.0) + jnp.log1p(jnp.exp(-jnp.abs(raw)))
    la_val = jnp.maximum(dt_val * par[1:2, :], -1000.0)
    tri = jnp.where(row >= lane, 1.0, 0.0).astype(BF16)
    for c in range(x_val.shape[0] // CHUNK):
        part = slice(c * CHUNK, (c + 1) * CHUNK)
        la_c = la_val[part, :]
        first = la_c.astype(BF16)
        rest = la_c - first.astype(F32)
        second = rest.astype(BF16)
        third = (rest - second.astype(F32)).astype(BF16)
        cum = sum(jnp.dot(tri, t, preferred_element_type=F32) for t in (first, second, third))
        one = jnp.where(lane < 3 * SLOT + 3, 1.0, 0.0)
        cum3 = split3(cum, lane, one)
        nexc3 = split3(la_c - cum, lane, one)
        cum_ref[part, :] = cum3
        nexc_ref[part, :] = nexc3
        dt_ref[part, :] = split3(dt_val[part, :], lane, 0.0)
        across = (((1,), (1,)), ((), ()))
        tail1_ref[:, part] = lax.dot_general(pick[...], cum3, across, preferred_element_type=F32).astype(BF16)
        tail2_ref[:, part] = lax.dot_general(pick[...], nexc3, across, preferred_element_type=F32).astype(BF16)
        log_ref[...] += cum[CHUNK - 1:CHUNK, :]
    for i in range(n_tiles):
        u_ref[:, i * 256:(i + 1) * 256] = jnp.dot(x_val, refs[i][...], preferred_element_type=F32).astype(BF16)


def proj_kernel(counts, x_ref, *refs):
    x_val = x_ref[...]
    o_refs = refs[sum(counts) + 1:]
    k = 0
    for o_ref, count in zip(o_refs, counts):
        for i in range(count):
            o_ref[:, i * 256:(i + 1) * 256] = jnp.dot(x_val, refs[k][...], preferred_element_type=F32).astype(BF16)
            k += 1


def sum_kernel(n_tiles, n_pieces, acc_ref, *refs):
    o_ref = refs[-1]
    total = acc_ref[...].astype(F32)
    for i in range(n_pieces):
        g_ref, w_refs = refs[sum(n_tiles[:i]) + i], refs[sum(n_tiles[:i]) + i + 1:sum(n_tiles[:i + 1]) + i + 1]
        for t in range(n_tiles[i]):
            total = total + jnp.dot(g_ref[:, t * 256:(t + 1) * 256], w_refs[t][...], preferred_element_type=F32)
    o_ref[...] = total.astype(o_ref.dtype)


def spread_matrix(shape, first_head, lanes_per_head):
    term = lax.broadcasted_iota(jnp.int32, shape, 0)
    lane = lax.broadcasted_iota(jnp.int32, shape, 1)
    return jnp.where((term % SLOT == first_head + lane // lanes_per_head) & (term < 3 * SLOT), 1.0, 0.0).astype(BF16)


def pair_cols(cols, head, low):
    return jnp.where(low, jnp.broadcast_to(cols[:, head:head + 1], low.shape), jnp.broadcast_to(cols[:, head + 1:head + 2], low.shape))


def state_kernel(first_head, n_pairs, u_ref, bc_ref, cum_ref, nexc_ref, dt_ref, gloc_ref, suf_ref, sf_ref, sb_ref, ut_ref, vf_ref, g_acc, f_acc, suf_acc, v_buf, spread):
    step = pl.program_id(0)
    width = n_pairs * LANES

    @pl.when(step == 0)
    def _():
        g_acc[...] = jnp.zeros_like(g_acc)
        f_acc[...] = jnp.zeros_like(f_acc)
        suf_acc[...] = jnp.zeros_like(suf_acc)
        spread[...] = spread_matrix(spread.shape, first_head, LANES // 2)

    def terms_of(c, p):
        rows = slice(c * CHUNK, (c + 1) * CHUNK)
        wide = slice(p * LANES, min(p + 2, n_pairs) * LANES)
        return [jnp.dot(r[rows, :], spread[:, wide], preferred_element_type=F32) for r in (cum_ref, nexc_ref, dt_ref)]

    def finish(c, total):
        rows = slice(c * CHUNK, (c + 1) * CHUNK)
        suffix = suf_acc[...]
        suf_ref[c, 0:1, :] = suffix[0:1, :]
        suf_ref[c, 1:2, :] = total
        sums = lax.dot_general(bc_ref[rows, :LANES], v_buf[rows, :], (((0,), (0,)), ((), ())), preferred_element_type=F32)
        back = g_acc[...]
        gloc_ref[c] = back
        g_acc[...] = back * jnp.exp(total) + sums[:, :width]
        f_acc[...] += sums[:, width:] * jnp.exp(suffix[0:1, :])
        suf_acc[...] = suffix + total

    order = [(c, p) for c in reversed(range(STATE_CHUNKS)) for p in range(0, n_pairs, 2)]
    ahead = terms_of(*order[0])
    for i, (c, p0) in enumerate(order):
        terms = ahead
        if i + 1 < len(order):
            ahead = terms_of(*order[i + 1])
        rows = slice(c * CHUNK, (c + 1) * CHUNK)
        if p0 == 0:
            totals = []
        for p in range(p0, min(p0 + 2, n_pairs)):
            part = slice(p * LANES, (p + 1) * LANES)
            half = slice((p - p0) * LANES, (p - p0 + 1) * LANES)
            cum, nexc, dt_val = [t[:, half] for t in terms]
            scaled = u_ref[rows, part].astype(F32) * dt_val
            total = cum[CHUNK - 1:CHUNK, :]
            totals.append(total)
            ut_ref[rows, part] = scaled.astype(BF16)
            v_buf[rows, part] = (scaled * jnp.exp(-nexc)).astype(BF16)
            end = (scaled * jnp.exp(total - cum)).astype(BF16)
            vf_ref[rows, part] = end
            v_buf[rows, slice(width + p * LANES, width + (p + 1) * LANES)] = end
        if p0 + 2 >= n_pairs:
            finish(c, jnp.concatenate(totals, axis=1))

    @pl.when(step == pl.num_programs(0) - 1)
    def _():
        sf_ref[...] = f_acc[...].astype(BF16)
        sb_ref[...] = g_acc[...].astype(BF16)


def peer_weights(sp_index, logs):
    fwd, bwd = [], []
    for s in (1, 2, 3):
        peer = sp_index ^ s
        between = jnp.zeros_like(logs[0])
        for o in (1, 2, 3):
            other = sp_index ^ o
            inside = (other > jnp.minimum(peer, sp_index)) & (other < jnp.maximum(peer, sp_index))
            between = between + jnp.where(inside, logs[o - 1], 0.0)
        decay = jnp.exp(between)
        fwd.append(jnp.where(peer < sp_index, decay, 0.0))
        bwd.append(jnp.where(peer > sp_index, decay, 0.0))
    return fwd, bwd


def out_kernel(first_head, n_pairs, who_ref, u_ref, z_ref, ut_ref, vf_ref, bc_ref, cum_ref, nexc_ref, tail1_ref, tail2_ref, gloc_ref, suf_ref, r1_ref, r2_ref, r3_ref, l1_ref, l2_ref, l3_ref, skip_ref, after_ref, o0_ref, o1_ref, o2_ref, o3_ref, f_acc, hb_acc, skip_buf, g_buf, spread, pick, fwd_buf, bwd_buf):
    step = pl.program_id(0)

    @pl.when(step == 0)
    def _():
        low8 = lax.broadcasted_iota(jnp.int32, (8, LANES), 1) < LANES // 2
        fwd, bwd = peer_weights(who_ref[1], [r[...] for r in (l1_ref, l2_ref, l3_ref)])
        got = (r1_ref, r2_ref, r3_ref)
        spread[...] = spread_matrix(spread.shape, first_head, LANES // 2)
        pick[...] = spread_matrix(pick.shape, first_head, LANES)
        for p in range(n_pairs):
            part = slice(p * LANES, (p + 1) * LANES)
            over = lambda v: pair_cols(v, first_head + 2 * p, low8)
            skip_buf[:, part] = 2.0 * over(jnp.broadcast_to(skip_ref[...], (8, skip_ref.shape[1])))
            f_acc[:, part] = sum(got[s][:, part].astype(F32) * over(fwd[s])[0:1, :] for s in range(3))
            hb_acc[:, part] = sum(got[s][:, part].astype(F32) * over(bwd[s])[0:1, :] for s in range(3))

    row = lax.broadcasted_iota(jnp.int32, (CHUNK, LANES), 0)
    lane = lax.broadcasted_iota(jnp.int32, (CHUNK, LANES), 1)
    low = lane < LANES // 2
    zeros = jnp.zeros((16, 2 * LANES), BF16)
    grams = []
    for c in range(OUT_CHUNKS):
        rows = slice(c * CHUNK, (c + 1) * CHUNK)
        b_val = bc_ref[rows, :LANES]
        gram = lax.dot_general(bc_ref[rows, LANES:], b_val, (((1,), (1,)), ((), ())), preferred_element_type=F32)
        grams.append(jnp.where(row == lane, 2.0 * gram, gram))
        sums = lax.dot_general(b_val, vf_ref[rows, :], (((0,), (0,)), ((), ())), preferred_element_type=F32)
        state = f_acc[...]
        fwd_buf[c] = state.astype(BF16)
        bwd_buf[c] = (gloc_ref[c] + hb_acc[...] * jnp.exp(suf_ref[c, 0:1, :])).astype(BF16)
        f_acc[...] = state * jnp.exp(suf_ref[c, 1:2, :]) + sums

    def weights(c, p):
        rows = slice(c * CHUNK, (c + 1) * CHUNK)
        head = first_head + 2 * p

        def differences(terms_ref, tail_ref):
            tails = jnp.concatenate([tail_ref[16 * h:16 * h + 16, rows] for h in (head, head + 1)], axis=1)
            chosen = pick[0:3 * SLOT, slice(2 * p * LANES, 2 * (p + 1) * LANES)]
            return jnp.dot(terms_ref[rows, :], jnp.concatenate([chosen, tails, zeros], axis=0), preferred_element_type=F32)

        decay = jnp.exp(jnp.minimum(differences(cum_ref, tail1_ref), differences(nexc_ref, tail2_ref)))
        return jnp.concatenate([(decay[:, :LANES] * grams[c]).astype(BF16), (decay[:, LANES:] * grams[c]).astype(BF16)], axis=1)

    def passed(c, p):
        rows = slice(c * CHUNK, (c + 1) * CHUNK)
        part = slice(p * LANES, (p + 1) * LANES)
        c_val = bc_ref[rows, LANES:]
        cum = jnp.dot(cum_ref[rows, :], spread[:, part], preferred_element_type=F32)
        nexc = jnp.dot(nexc_ref[rows, :], spread[:, part], preferred_element_type=F32)
        y_fwd = jnp.dot(c_val, fwd_buf[c, :, part], preferred_element_type=F32)
        y_bwd = jnp.dot(c_val, bwd_buf[c, :, part], preferred_element_type=F32)
        y_val = jnp.exp(cum) * y_fwd + jnp.exp(suf_ref[c, 1:2, part] + nexc) * y_bwd
        return y_val + skip_buf[0:1, part] * u_ref[rows, part].astype(F32)

    order = [(c, p) for c in range(OUT_CHUNKS) for p in range(n_pairs)]
    ahead = [weights(*order[i]) for i in range(OUT_AHEAD)]
    for i, (c, p) in enumerate(order):
        mix = ahead.pop(0)
        if i + OUT_AHEAD < len(order):
            ahead.append(weights(*order[i + OUT_AHEAD]))
        y_val = passed(c, p)
        rows = slice(c * CHUNK, (c + 1) * CHUNK)
        part = slice(p * LANES, (p + 1) * LANES)
        scaled = ut_ref[rows, part]
        none = jnp.zeros_like(scaled)
        rhs = jnp.concatenate([jnp.where(low, scaled, none), jnp.where(low, none, scaled)], axis=0)
        y_val = jnp.dot(mix, rhs, preferred_element_type=F32) + y_val
        z_val = z_ref[rows, part].astype(F32)
        g_buf[rows, part] = (y_val * (z_val * jax.nn.sigmoid(z_val))).astype(BF16)

    steps = pl.num_programs(0) // 4
    slot = (step // steps) ^ who_ref[0]
    length = OUT_CHUNKS * CHUNK
    for s, o_ref in enumerate((o0_ref, o1_ref, o2_ref, o3_ref)):
        @pl.when(slot == s)
        def _():
            o_ref[pl.ds(pl.multiple_of((step % steps) * length, length), length), :] = g_buf[...]


def params():
    return pltpu.CompilerParams(dimension_semantics=("arbitrary",), vmem_limit_bytes=62 << 20)


def cost(flops, moved):
    return pl.CostEstimate(flops=int(flops), bytes_accessed=int(moved), transcendentals=0)


ANY = pl.BlockSpec(memory_space=pl.ANY)


def w_specs(w, first_tile, n_tiles):
    return [pl.BlockSpec((w.shape[0], 256), functools.partial(lambda t, i: (0, t), first_tile + t), pipeline_mode=pl.Buffered(1)) for t in range(n_tiles)]


def prep(x_blk, w_bc, w_dt_rows, bias, a_neg, w_x, n_tiles):
    tokens, d_model = x_blk.shape
    tile = min(512, tokens)
    width = 256 * n_tiles
    whole = lambda a: pl.BlockSpec(a.shape, lambda i: (0, 0), pipeline_mode=pl.Buffered(1))
    tok = lambda w: pl.BlockSpec((tile, w), lambda i: (i, 0))
    heads = bias.shape[1]
    tail = pl.BlockSpec((16 * heads, tile), lambda i: (0, i))
    return pl.pallas_call(
        functools.partial(prep_kernel, n_tiles),
        grid=(tokens // tile,),
        in_specs=[tok(d_model), whole(w_bc), whole(w_dt_rows), whole(bias), whole(a_neg)] + w_specs(w_x, 0, n_tiles),
        out_specs=[tok(2 * LANES), tok(LANES), tok(LANES), tok(LANES), tail, tail, pl.BlockSpec((8, LANES), lambda i: (0, 0)), tok(width)],
        out_shape=[jax.ShapeDtypeStruct((tokens, 2 * LANES), BF16)] + [jax.ShapeDtypeStruct((tokens, LANES), BF16)] * 3 + [jax.ShapeDtypeStruct((16 * heads, tokens), BF16)] * 2 + [jax.ShapeDtypeStruct((8, LANES), F32), jax.ShapeDtypeStruct((tokens, width), BF16)],
        scratch_shapes=[pltpu.VMEM((LANES, d_model), BF16), pltpu.VMEM((8, LANES), F32), pltpu.VMEM((16 * heads, LANES), BF16)],
        compiler_params=params(),
        cost_estimate=cost(2 * tokens * d_model * (512 + width), 2 * tokens * d_model),
        name="prep",
    )(x_blk, w_bc, w_dt_rows, bias, a_neg, *([w_x] * n_tiles))


def project(x_blk, parts, after):
    tokens, d_model = x_blk.shape
    tile = min(512, tokens)
    counts = [n for _, _, n in parts]
    specs = [spec for w, t, n in parts for spec in w_specs(w, t, n)]
    return pl.pallas_call(
        functools.partial(proj_kernel, counts),
        grid=(tokens // tile,),
        in_specs=[pl.BlockSpec((tile, d_model), lambda i: (i, 0))] + specs + [ANY],
        out_specs=[pl.BlockSpec((tile, 256 * n), lambda i: (i, 0)) for n in counts],
        out_shape=[jax.ShapeDtypeStruct((tokens, 256 * n), BF16) for n in counts],
        compiler_params=params(),
        cost_estimate=cost(512 * tokens * d_model * sum(counts), 2 * tokens * d_model),
        name="project",
    )(x_blk, *[w for w, _, n in parts for _ in range(n)], after)


def add_products(acc, pieces, out_dtype):
    rows, d_model = acc.shape
    tile = min(512, d_model)
    n_tiles = [g.shape[1] // 256 for g, _, _ in pieces]
    specs, args = [pl.BlockSpec((rows, tile), lambda i: (0, i))], [acc]
    for (g, w, tile0), count in zip(pieces, n_tiles):
        specs.append(pl.BlockSpec(g.shape, lambda i: (0, 0)))
        specs += [pl.BlockSpec((256, tile), functools.partial(lambda t, i: (t, i), tile0 + t)) for t in range(count)]
        args += [g] + [w] * count
    return pl.pallas_call(
        functools.partial(sum_kernel, n_tiles, len(pieces)),
        grid=(d_model // tile,),
        in_specs=specs,
        out_specs=pl.BlockSpec((rows, tile), lambda i: (0, i)),
        out_shape=jax.ShapeDtypeStruct((rows, d_model), out_dtype),
        compiler_params=params(),
        cost_estimate=cost(2 * rows * d_model * 256 * sum(n_tiles), 2 * rows * d_model),
        name="add_products",
    )(*args)


def chunk_states(u, bc, sums, after, first_head, n_pairs):
    tokens, width = u.shape
    n_chunks = tokens // CHUNK
    last = n_chunks // STATE_CHUNKS - 1
    tok = lambda w: pl.BlockSpec((STATE_CHUNKS * CHUNK, w), lambda i: (last - i, 0))
    whole = pl.BlockSpec((LANES, width), lambda i: (0, 0))

    def body(u_ref, bc_ref, cum_ref, nexc_ref, dt_ref, after_ref, *refs):
        state_kernel(first_head, n_pairs, u_ref, bc_ref, cum_ref, nexc_ref, dt_ref, *refs)

    return pl.pallas_call(
        body,
        grid=(last + 1,),
        in_specs=[tok(width), tok(2 * LANES)] + [tok(LANES)] * 3 + [ANY],
        out_specs=[pl.BlockSpec((STATE_CHUNKS, LANES, width), lambda i: (last - i, 0, 0)), pl.BlockSpec((STATE_CHUNKS, 8, width), lambda i: (last - i, 0, 0)), whole, whole, tok(width), tok(width)],
        out_shape=[jax.ShapeDtypeStruct((n_chunks, LANES, width), F32), jax.ShapeDtypeStruct((n_chunks, 8, width), F32)] + [jax.ShapeDtypeStruct((LANES, width), BF16)] * 2 + [jax.ShapeDtypeStruct((tokens, width), BF16)] * 2,
        scratch_shapes=[pltpu.VMEM((LANES, width), F32), pltpu.VMEM((LANES, width), F32), pltpu.VMEM((8, width), F32), pltpu.VMEM((STATE_CHUNKS * CHUNK, 2 * width), BF16), pltpu.VMEM((LANES, width), BF16)],
        compiler_params=params(),
        cost_estimate=cost(16 * tokens * width * 256, 8 * tokens * width),
        name="states",
    )(u, bc, *sums, after)


def chunk_outputs(who, u, z, bc, sums, tails, local, got, logs, skip, after, first_head, n_pairs):
    tokens, width = u.shape
    n_steps = tokens // (OUT_CHUNKS * CHUNK)
    gloc, suf, scaled, ends = local
    tail = pl.BlockSpec((tails[0].shape[0], OUT_CHUNKS * CHUNK), lambda i, who: (0, i))
    tok = lambda w: pl.BlockSpec((OUT_CHUNKS * CHUNK, w), lambda i, who: (i, 0))
    state = pl.BlockSpec((LANES, width), lambda i, who: (0, 0))
    small = lambda a: pl.BlockSpec(a.shape, lambda i, who: (0, 0))
    rows_out = tokens // 4
    return pl.pallas_call(
        functools.partial(out_kernel, first_head, n_pairs),
        grid_spec=pltpu.PrefetchScalarGridSpec(
            num_scalar_prefetch=1,
            grid=(n_steps,),
            in_specs=[tok(width)] * 4 + [tok(2 * LANES), tok(LANES), tok(LANES), tail, tail, pl.BlockSpec((OUT_CHUNKS, LANES, width), lambda i, who: (i, 0, 0)), pl.BlockSpec((OUT_CHUNKS, 8, width), lambda i, who: (i, 0, 0)), state, state, state] + [small(v) for v in logs] + [small(skip), ANY],
            out_specs=[pl.BlockSpec((rows_out, width), lambda i, who: (0, 0))] * 4,
            scratch_shapes=[pltpu.VMEM((LANES, width), F32), pltpu.VMEM((LANES, width), F32), pltpu.VMEM((8, width), F32), pltpu.VMEM((OUT_CHUNKS * CHUNK, width), BF16), pltpu.VMEM((LANES, width), BF16), pltpu.VMEM((LANES, 2 * width), BF16)] + [pltpu.VMEM((OUT_CHUNKS, LANES, width), BF16)] * 2,
        ),
        out_shape=[jax.ShapeDtypeStruct((rows_out, width), BF16)] * 4,
        compiler_params=params(),
        cost_estimate=cost(24 * tokens * width * 256, 8 * tokens * width),
        name="outputs",
    )(who, u, z, scaled, ends, bc, sums[0], sums[1], *tails, gloc, suf, *got, *logs, skip, after)


def solution(mesh):
    n_tp, n_sp, n_dp = mesh.shape['tp'], mesh.shape['sp'], mesh.shape['dp']

    def swap(val, axis, slot):
        return lax.ppermute(val, axis, [(i, i ^ slot) for i in range(4)])

    def later(vals, after):
        return list(lax.optimization_barrier((*vals, after)))[:-1]

    def device_fn(x_blk, w_z, w_x, w_bc, w_dt, a_neg, dt_bias, d_skip, w_out):
        tokens, _ = x_blk.shape
        heads = a_neg.shape[0]
        head_dim = w_x.shape[1] // heads
        rows_out = tokens // n_tp
        tp_index = lax.axis_index('tp')
        sp_index = lax.axis_index('sp')

        piece_rows = w_out.shape[0] // (n_dp * n_sp)
        mine = lax.axis_index('dp') * n_sp + sp_index
        piece = lax.dynamic_slice_in_dim(w_out, mine * piece_rows, piece_rows, axis=0)
        one = swap(piece, 'tp', 1)
        two = swap(piece, 'tp', 2)
        three = swap(piece, 'tp', 3)
        plane = lambda v: lax.all_gather(v, ('dp', 'sp'), tiled=True)

        n_tiles = w_x.shape[1] // 256
        first = n_tiles * 2 // 5
        (t_a, n_a), (t_b, n_b) = (0, first), (first, n_tiles - first)
        head_b = first * 256 // head_dim
        who = jnp.stack([tp_index, sp_index])
        skip = d_skip[None, :]

        def exchange(s_fwd, s_bwd):
            return [swap(jnp.where(sp_index < (sp_index ^ s), s_fwd, s_bwd), 'sp', s) for s in (1, 2, 3)]

        def send(pieces):
            return [pieces[0]] + [swap(pieces[s], 'tp', s) for s in (1, 2, 3)]

        bc, cum3, nexc3, dt3, tail1, tail2, block_log, u_a = prep(x_blk, w_bc, w_dt.T, dt_bias[None, :], a_neg[None, :], w_x, n_a)
        logs = [swap(block_log, 'sp', s) for s in (1, 2, 3)]
        one, = later((one,), block_log)
        w_one = plane(one)
        gloc_a, suf_a, s_fwd, s_bwd, ut_a, vf_a = chunk_states(u_a, bc, (cum3, nexc3, dt3), one, 0, 2 * n_a)
        got_a = exchange(s_fwd, s_bwd)
        z_a, u_b = project(x_blk, [(w_z, t_a, n_a), (w_x, t_b, n_b)], s_fwd)
        two, = later((two,), z_a)
        w_two = plane(two)
        g_a = chunk_outputs(who, u_a, z_a, bc, (cum3, nexc3), (tail1, tail2), (gloc_a, suf_a, ut_a, vf_a), got_a, logs, skip, two, 0, 2 * n_a)
        got_g_a = send(g_a)
        three, = later((three,), g_a[0])
        w_three = plane(three)
        gloc_b, suf_b, s_fwd, s_bwd, ut_b, vf_b = chunk_states(u_b, bc, (cum3, nexc3, dt3), three, head_b, 2 * n_b)
        got_b = exchange(s_fwd, s_bwd)
        z_b, = project(x_blk, [(w_z, t_b, n_b)], s_fwd)
        g_b = chunk_outputs(who, u_b, z_b, bc, (cum3, nexc3), (tail1, tail2), (gloc_b, suf_b, ut_b, vf_b), got_b, logs, skip, z_b, head_b, 2 * n_b)
        got_g_b = send(g_b)

        own = lax.dynamic_slice_in_dim(x_blk, tp_index * rows_out, rows_out, axis=0)
        total = add_products(own, [(got_g_a[0], w_out, t_a), (got_g_b[0], w_out, t_b)], F32)
        total = add_products(total, [(got_g_a[1], w_one, t_a), (got_g_a[2], w_two, t_a)], F32)
        total = add_products(total, [(got_g_a[3], w_three, t_a), (got_g_b[1], w_one, t_b)], F32)
        return add_products(total, [(got_g_b[2], w_two, t_b), (got_g_b[3], w_three, t_b)], BF16)

    in_specs = (P(('dp', 'sp'), None), P(None, 'tp'), P(None, 'tp'), P(None, None), P(None, 'tp'), P('tp'), P('tp'), P('tp'), P('tp', None))
    out_specs = P(('dp', 'sp', 'tp'), None)
    return jax.shard_map(device_fn, mesh=mesh, in_specs=in_specs, out_specs=out_specs, check_vma=False)
```

```python
import functools

import jax
import jax.numpy as jnp
from jax import lax
from jax.experimental import pallas as pl
from jax.experimental.pallas import tpu as pltpu
from jax.sharding import PartitionSpec as P


CHUNK = 128
LANES = 128
SLOT = 32
STATE_CHUNKS = 4
OUT_CHUNKS = 2
OUT_AHEAD = 2
SUM_MIB = 24
F32 = jnp.float32
BF16 = jnp.bfloat16


def split3(val, lane, last):
    first = val.astype(BF16).astype(F32)
    rest = val - first
    second = rest.astype(BF16).astype(F32)
    third = rest - second
    return jnp.where(lane < SLOT, first, jnp.where(lane < 2 * SLOT, second, jnp.where(lane < 3 * SLOT, third, last))).astype(BF16)


def prep_kernel(n_tiles, x_ref, wbc_ref, wdt_ref, bias_ref, a_ref, *refs):
    bc_ref, cum_ref, nexc_ref, dt_ref, tail1_ref, tail2_ref, log_ref, u_ref, w_buf, par, pick = refs[n_tiles:]
    heads = bias_ref.shape[1]
    row = lax.broadcasted_iota(jnp.int32, (CHUNK, LANES), 0)
    lane = lax.broadcasted_iota(jnp.int32, (CHUNK, LANES), 1)

    @pl.when(pl.program_id(0) == 0)
    def _():
        log_ref[...] = jnp.zeros_like(log_ref)
        w_buf[...] = jnp.zeros_like(w_buf)
        par[...] = jnp.zeros_like(par)
        for k in range(3):
            w_buf[k * SLOT:k * SLOT + heads, :] = wdt_ref[...]
            par[0:1, k * SLOT:k * SLOT + heads] = bias_ref[...]
            par[1:2, k * SLOT:k * SLOT + heads] = a_ref[...]
        out_row = lax.broadcasted_iota(jnp.int32, pick.shape, 0)
        term = lax.broadcasted_iota(jnp.int32, pick.shape, 1)
        head, which = out_row // 16, out_row % 16
        pick[...] = jnp.where((which < 3) & (term == which * SLOT + head), -1.0, 0.0).astype(BF16)

    x_val = x_ref[...]
    raw = lax.dot_general(x_val, w_buf[...], (((1,), (1,)), ((), ())), preferred_element_type=F32) + par[0:1, :]

    def u_tile(i):
        u_ref[:, i * 256:(i + 1) * 256] = jnp.dot(x_val, refs[i][...], preferred_element_type=F32).astype(BF16)

    u_tile(0)
    dt_val = jnp.maximum(raw, 0.0) + jnp.log1p(jnp.exp(-jnp.abs(raw)))
    la_val = jnp.maximum(dt_val * par[1:2, :], -1000.0)
    tri = jnp.where(row >= lane, 1.0, 0.0).astype(BF16)
    parts = [slice(c * CHUNK, (c + 1) * CHUNK) for c in range(x_val.shape[0] // CHUNK)]
    sums = []
    for part in parts:
        la_c = la_val[part, :]
        first = la_c.astype(BF16)
        rest = la_c - first.astype(F32)
        second = rest.astype(BF16)
        third = (rest - second.astype(F32)).astype(BF16)
        sums.append(sum(jnp.dot(tri, t, preferred_element_type=F32) for t in (first, second, third)))
    for i in range(1, n_tiles):
        u_tile(i)
    one = jnp.where(lane < 3 * SLOT + 3, 1.0, 0.0)
    for part, cum in zip(parts, sums):
        cum_ref[part, :] = split3(cum, lane, one)
        nexc_ref[part, :] = split3(la_val[part, :] - cum, lane, one)
        dt_ref[part, :] = split3(dt_val[part, :], lane, 0.0)
        log_ref[...] += cum[CHUNK - 1:CHUNK, :]
    bc_ref[...] = jnp.dot(x_val, wbc_ref[...], preferred_element_type=F32).astype(BF16)
    across = (((1,), (1,)), ((), ()))
    tail1_ref[...] = lax.dot_general(pick[...], cum_ref[...], across, preferred_element_type=F32).astype(BF16)
    tail2_ref[...] = lax.dot_general(pick[...], nexc_ref[...], across, preferred_element_type=F32).astype(BF16)


def proj_kernel(counts, x_ref, *refs):
    x_val = x_ref[...]
    o_refs = refs[sum(counts) + 1:]
    k = 0
    for o_ref, count in zip(o_refs, counts):
        for i in range(count):
            o_ref[:, i * 256:(i + 1) * 256] = jnp.dot(x_val, refs[k][...], preferred_element_type=F32).astype(BF16)
            k += 1


def sum_kernel(n_tiles, n_pieces, acc_ref, *refs):
    o_ref = refs[-1]
    total = acc_ref[...].astype(F32)
    for i in range(n_pieces):
        g_ref, w_refs = refs[sum(n_tiles[:i]) + i], refs[sum(n_tiles[:i]) + i + 1:sum(n_tiles[:i + 1]) + i + 1]
        for t in range(n_tiles[i]):
            total = total + jnp.dot(g_ref[:, t * 256:(t + 1) * 256], w_refs[t][...], preferred_element_type=F32)
    o_ref[...] = total.astype(o_ref.dtype)


def spread_matrix(shape, first_head, lanes_per_head):
    term = lax.broadcasted_iota(jnp.int32, shape, 0)
    lane = lax.broadcasted_iota(jnp.int32, shape, 1)
    return jnp.where((term % SLOT == first_head + lane // lanes_per_head) & (term < 3 * SLOT), 1.0, 0.0).astype(BF16)


def pair_cols(cols, head, low):
    return jnp.where(low, jnp.broadcast_to(cols[:, head:head + 1], low.shape), jnp.broadcast_to(cols[:, head + 1:head + 2], low.shape))


def state_kernel(first_head, n_pairs, u_ref, bc_ref, cum_ref, nexc_ref, dt_ref, gloc_ref, suf_ref, sf_ref, sb_ref, ut_ref, vf_ref, g_acc, f_acc, suf_acc, v_buf, spread):
    step = pl.program_id(0)
    width = n_pairs * LANES

    @pl.when(step == 0)
    def _():
        g_acc[...] = jnp.zeros_like(g_acc)
        f_acc[...] = jnp.zeros_like(f_acc)
        suf_acc[...] = jnp.zeros_like(suf_acc)
        spread[...] = spread_matrix(spread.shape, first_head, LANES // 2)

    def terms_of(c, p):
        rows = slice(c * CHUNK, (c + 1) * CHUNK)
        wide = slice(p * LANES, min(p + 2, n_pairs) * LANES)
        return [jnp.dot(r[rows, :], spread[:, wide], preferred_element_type=F32) for r in (cum_ref, nexc_ref, dt_ref)]

    def finish(c, total):
        rows = slice(c * CHUNK, (c + 1) * CHUNK)
        suffix = suf_acc[...]
        suf_ref[c, 0:1, :] = suffix[0:1, :]
        suf_ref[c, 1:2, :] = total
        sums = lax.dot_general(bc_ref[rows, :LANES], v_buf[rows, :], (((0,), (0,)), ((), ())), preferred_element_type=F32)
        back = g_acc[...]
        gloc_ref[c] = back
        g_acc[...] = back * jnp.exp(total) + sums[:, :width]
        f_acc[...] += sums[:, width:] * jnp.exp(suffix[0:1, :])
        suf_acc[...] = suffix + total

    order = [(c, p) for c in reversed(range(STATE_CHUNKS)) for p in range(0, n_pairs, 2)]
    ahead = terms_of(*order[0])
    for i, (c, p0) in enumerate(order):
        terms = ahead
        if i + 1 < len(order):
            ahead = terms_of(*order[i + 1])
        rows = slice(c * CHUNK, (c + 1) * CHUNK)
        if p0 == 0:
            totals = []
        for p in range(p0, min(p0 + 2, n_pairs)):
            part = slice(p * LANES, (p + 1) * LANES)
            half = slice((p - p0) * LANES, (p - p0 + 1) * LANES)
            cum, nexc, dt_val = [t[:, half] for t in terms]
            scaled = u_ref[rows, part].astype(F32) * dt_val
            total = cum[CHUNK - 1:CHUNK, :]
            totals.append(total)
            ut_ref[rows, part] = scaled.astype(BF16)
            v_buf[rows, part] = (scaled * jnp.exp(-nexc)).astype(BF16)
            end = (scaled * jnp.exp(total - cum)).astype(BF16)
            vf_ref[rows, part] = end
            v_buf[rows, slice(width + p * LANES, width + (p + 1) * LANES)] = end
        if p0 + 2 >= n_pairs:
            finish(c, jnp.concatenate(totals, axis=1))

    @pl.when(step == pl.num_programs(0) - 1)
    def _():
        sf_ref[...] = f_acc[...].astype(BF16)
        sb_ref[...] = g_acc[...].astype(BF16)


def peer_weights(sp_index, logs):
    fwd, bwd = [], []
    for s in (1, 2, 3):
        peer = sp_index ^ s
        between = jnp.zeros_like(logs[0])
        for o in (1, 2, 3):
            other = sp_index ^ o
            inside = (other > jnp.minimum(peer, sp_index)) & (other < jnp.maximum(peer, sp_index))
            between = between + jnp.where(inside, logs[o - 1], 0.0)
        decay = jnp.exp(between)
        fwd.append(jnp.where(peer < sp_index, decay, 0.0))
        bwd.append(jnp.where(peer > sp_index, decay, 0.0))
    return fwd, bwd


def out_kernel(first_head, n_pairs, who_ref, u_ref, z_ref, ut_ref, vf_ref, bc_ref, cum_ref, nexc_ref, tail1_ref, tail2_ref, gloc_ref, suf_ref, r1_ref, r2_ref, r3_ref, l1_ref, l2_ref, l3_ref, skip_ref, after_ref, o0_ref, o1_ref, o2_ref, o3_ref, f_acc, hb_acc, skip_buf, g_buf, spread, pick, fwd_buf, bwd_buf):
    step = pl.program_id(0)

    @pl.when(step == 0)
    def _():
        low8 = lax.broadcasted_iota(jnp.int32, (8, LANES), 1) < LANES // 2
        fwd, bwd = peer_weights(who_ref[1], [r[...] for r in (l1_ref, l2_ref, l3_ref)])
        got = (r1_ref, r2_ref, r3_ref)
        spread[...] = spread_matrix(spread.shape, first_head, LANES // 2)
        pick[...] = spread_matrix(pick.shape, first_head, LANES)
        for p in range(n_pairs):
            part = slice(p * LANES, (p + 1) * LANES)
            over = lambda v: pair_cols(v, first_head + 2 * p, low8)
            skip_buf[:, part] = 2.0 * over(jnp.broadcast_to(skip_ref[...], (8, skip_ref.shape[1])))
            f_acc[:, part] = sum(got[s][:, part].astype(F32) * over(fwd[s])[0:1, :] for s in range(3))
            hb_acc[:, part] = sum(got[s][:, part].astype(F32) * over(bwd[s])[0:1, :] for s in range(3))

    row = lax.broadcasted_iota(jnp.int32, (CHUNK, LANES), 0)
    lane = lax.broadcasted_iota(jnp.int32, (CHUNK, LANES), 1)
    low = lane < LANES // 2
    zeros = jnp.zeros((16, 2 * LANES), BF16)
    grams = []
    for c in range(OUT_CHUNKS):
        rows = slice(c * CHUNK, (c + 1) * CHUNK)
        b_val = bc_ref[rows, :LANES]
        gram = lax.dot_general(bc_ref[rows, LANES:], b_val, (((1,), (1,)), ((), ())), preferred_element_type=F32)
        grams.append(jnp.where(row == lane, 2.0 * gram, gram))
        sums = lax.dot_general(b_val, vf_ref[rows, :], (((0,), (0,)), ((), ())), preferred_element_type=F32)
        state = f_acc[...]
        fwd_buf[c] = state.astype(BF16)
        bwd_buf[c] = (gloc_ref[c] + hb_acc[...] * jnp.exp(suf_ref[c, 0:1, :])).astype(BF16)
        f_acc[...] = state * jnp.exp(suf_ref[c, 1:2, :]) + sums

    def weights(c, p):
        rows = slice(c * CHUNK, (c + 1) * CHUNK)
        head = first_head + 2 * p

        def differences(terms_ref, tail_ref):
            tails = jnp.concatenate([tail_ref[16 * h:16 * h + 16, rows] for h in (head, head + 1)], axis=1)
            chosen = pick[0:3 * SLOT, slice(2 * p * LANES, 2 * (p + 1) * LANES)]
            return jnp.dot(terms_ref[rows, :], jnp.concatenate([chosen, tails, zeros], axis=0), preferred_element_type=F32)

        decay = jnp.exp(jnp.minimum(differences(cum_ref, tail1_ref), differences(nexc_ref, tail2_ref)))
        return jnp.concatenate([(decay[:, :LANES] * grams[c]).astype(BF16), (decay[:, LANES:] * grams[c]).astype(BF16)], axis=1)

    def passed(c, p):
        rows = slice(c * CHUNK, (c + 1) * CHUNK)
        part = slice(p * LANES, (p + 1) * LANES)
        c_val = bc_ref[rows, LANES:]
        cum = jnp.dot(cum_ref[rows, :], spread[:, part], preferred_element_type=F32)
        nexc = jnp.dot(nexc_ref[rows, :], spread[:, part], preferred_element_type=F32)
        y_fwd = jnp.dot(c_val, fwd_buf[c, :, part], preferred_element_type=F32)
        y_bwd = jnp.dot(c_val, bwd_buf[c, :, part], preferred_element_type=F32)
        y_val = jnp.exp(cum) * y_fwd + jnp.exp(suf_ref[c, 1:2, part] + nexc) * y_bwd
        return y_val + skip_buf[0:1, part] * u_ref[rows, part].astype(F32)

    order = [(c, p) for c in range(OUT_CHUNKS) for p in range(n_pairs)]
    ahead = [weights(*order[i]) for i in range(OUT_AHEAD)]
    for i, (c, p) in enumerate(order):
        mix = ahead.pop(0)
        if i + OUT_AHEAD < len(order):
            ahead.append(weights(*order[i + OUT_AHEAD]))
        y_val = passed(c, p)
        rows = slice(c * CHUNK, (c + 1) * CHUNK)
        part = slice(p * LANES, (p + 1) * LANES)
        scaled = ut_ref[rows, part]
        none = jnp.zeros_like(scaled)
        rhs = jnp.concatenate([jnp.where(low, scaled, none), jnp.where(low, none, scaled)], axis=0)
        y_val = jnp.dot(mix, rhs, preferred_element_type=F32) + y_val
        z_val = z_ref[rows, part].astype(F32)
        g_buf[rows, part] = (y_val * (z_val * jax.nn.sigmoid(z_val))).astype(BF16)

    steps = pl.num_programs(0) // 4
    slot = (step // steps) ^ who_ref[0]
    length = OUT_CHUNKS * CHUNK
    for s, o_ref in enumerate((o0_ref, o1_ref, o2_ref, o3_ref)):
        @pl.when(slot == s)
        def _():
            o_ref[pl.ds(pl.multiple_of((step % steps) * length, length), length), :] = g_buf[...]


def params(mib=62):
    return pltpu.CompilerParams(dimension_semantics=("arbitrary",), vmem_limit_bytes=mib << 20)


def cost(flops, moved):
    return pl.CostEstimate(flops=int(flops), bytes_accessed=int(moved), transcendentals=0)


ANY = pl.BlockSpec(memory_space=pl.ANY)


def w_specs(w, first_tile, n_tiles):
    return [pl.BlockSpec((w.shape[0], 256), functools.partial(lambda t, i: (0, t), first_tile + t), pipeline_mode=pl.Buffered(1)) for t in range(n_tiles)]


def prep(x_blk, w_bc, w_dt_rows, bias, a_neg, w_x, n_tiles):
    tokens, d_model = x_blk.shape
    tile = min(512, tokens)
    width = 256 * n_tiles
    whole = lambda a: pl.BlockSpec(a.shape, lambda i: (0, 0), pipeline_mode=pl.Buffered(1))
    tok = lambda w: pl.BlockSpec((tile, w), lambda i: (i, 0))
    heads = bias.shape[1]
    tail = pl.BlockSpec((16 * heads, tile), lambda i: (0, i))
    return pl.pallas_call(
        functools.partial(prep_kernel, n_tiles),
        grid=(tokens // tile,),
        in_specs=[tok(d_model), whole(w_bc), whole(w_dt_rows), whole(bias), whole(a_neg)] + w_specs(w_x, 0, n_tiles),
        out_specs=[tok(2 * LANES), tok(LANES), tok(LANES), tok(LANES), tail, tail, pl.BlockSpec((8, LANES), lambda i: (0, 0)), tok(width)],
        out_shape=[jax.ShapeDtypeStruct((tokens, 2 * LANES), BF16)] + [jax.ShapeDtypeStruct((tokens, LANES), BF16)] * 3 + [jax.ShapeDtypeStruct((16 * heads, tokens), BF16)] * 2 + [jax.ShapeDtypeStruct((8, LANES), F32), jax.ShapeDtypeStruct((tokens, width), BF16)],
        scratch_shapes=[pltpu.VMEM((LANES, d_model), BF16), pltpu.VMEM((8, LANES), F32), pltpu.VMEM((16 * heads, LANES), BF16)],
        compiler_params=params(),
        cost_estimate=cost(2 * tokens * d_model * (512 + width), 2 * tokens * d_model),
        name="prep",
    )(x_blk, w_bc, w_dt_rows, bias, a_neg, *([w_x] * n_tiles))


def project(x_blk, parts, after):
    tokens, d_model = x_blk.shape
    tile = min(512, tokens)
    counts = [n for _, _, n in parts]
    specs = [spec for w, t, n in parts for spec in w_specs(w, t, n)]
    return pl.pallas_call(
        functools.partial(proj_kernel, counts),
        grid=(tokens // tile,),
        in_specs=[pl.BlockSpec((tile, d_model), lambda i: (i, 0))] + specs + [ANY],
        out_specs=[pl.BlockSpec((tile, 256 * n), lambda i: (i, 0)) for n in counts],
        out_shape=[jax.ShapeDtypeStruct((tokens, 256 * n), BF16) for n in counts],
        compiler_params=params(),
        cost_estimate=cost(512 * tokens * d_model * sum(counts), 2 * tokens * d_model),
        name="project",
    )(x_blk, *[w for w, _, n in parts for _ in range(n)], after)


def add_products(who, acc, pieces, out_dtype):
    rows, d_model = pieces[0][0].shape[0], acc.shape[1]
    tile = min(512, d_model)
    n_tiles = [g.shape[1] // 256 for g, _, _ in pieces]
    mine = acc.shape[0] > rows
    specs, args = [pl.BlockSpec((rows, tile), lambda i, who: (who[0] if mine else 0, i))], [acc]
    for (g, w, tile0), count in zip(pieces, n_tiles):
        specs.append(pl.BlockSpec(g.shape, lambda i, who: (0, 0)))
        specs += [pl.BlockSpec((256, tile), functools.partial(lambda t, i, who: (t, i), tile0 + t)) for t in range(count)]
        args += [g] + [w] * count

    def body(who_ref, *refs):
        sum_kernel(n_tiles, len(pieces), *refs)

    return pl.pallas_call(
        body,
        grid_spec=pltpu.PrefetchScalarGridSpec(num_scalar_prefetch=1, grid=(d_model // tile,), in_specs=specs, out_specs=pl.BlockSpec((rows, tile), lambda i, who: (0, i))),
        out_shape=jax.ShapeDtypeStruct((rows, d_model), out_dtype),
        compiler_params=params(SUM_MIB),
        cost_estimate=cost(2 * rows * d_model * 256 * sum(n_tiles), 2 * rows * d_model),
        name="add_products",
    )(who, *args)


def chunk_states(u, bc, sums, after, first_head, n_pairs):
    tokens, width = u.shape
    n_chunks = tokens // CHUNK
    last = n_chunks // STATE_CHUNKS - 1
    tok = lambda w: pl.BlockSpec((STATE_CHUNKS * CHUNK, w), lambda i: (last - i, 0))
    whole = pl.BlockSpec((LANES, width), lambda i: (0, 0))

    def body(u_ref, bc_ref, cum_ref, nexc_ref, dt_ref, after_ref, *refs):
        state_kernel(first_head, n_pairs, u_ref, bc_ref, cum_ref, nexc_ref, dt_ref, *refs)

    return pl.pallas_call(
        body,
        grid=(last + 1,),
        in_specs=[tok(width), tok(2 * LANES)] + [tok(LANES)] * 3 + [ANY],
        out_specs=[pl.BlockSpec((STATE_CHUNKS, LANES, width), lambda i: (last - i, 0, 0)), pl.BlockSpec((STATE_CHUNKS, 8, width), lambda i: (last - i, 0, 0)), whole, whole, tok(width), tok(width)],
        out_shape=[jax.ShapeDtypeStruct((n_chunks, LANES, width), F32), jax.ShapeDtypeStruct((n_chunks, 8, width), F32)] + [jax.ShapeDtypeStruct((LANES, width), BF16)] * 2 + [jax.ShapeDtypeStruct((tokens, width), BF16)] * 2,
        scratch_shapes=[pltpu.VMEM((LANES, width), F32), pltpu.VMEM((LANES, width), F32), pltpu.VMEM((8, width), F32), pltpu.VMEM((STATE_CHUNKS * CHUNK, 2 * width), BF16), pltpu.VMEM((LANES, width), BF16)],
        compiler_params=params(),
        cost_estimate=cost(16 * tokens * width * 256, 8 * tokens * width),
        name="states",
    )(u, bc, *sums, after)


def chunk_outputs(who, u, z, bc, sums, tails, local, got, logs, skip, after, first_head, n_pairs):
    tokens, width = u.shape
    n_steps = tokens // (OUT_CHUNKS * CHUNK)
    gloc, suf, scaled, ends = local
    tail = pl.BlockSpec((tails[0].shape[0], OUT_CHUNKS * CHUNK), lambda i, who: (0, i))
    tok = lambda w: pl.BlockSpec((OUT_CHUNKS * CHUNK, w), lambda i, who: (i, 0))
    state = pl.BlockSpec((LANES, width), lambda i, who: (0, 0))
    small = lambda a: pl.BlockSpec(a.shape, lambda i, who: (0, 0))
    rows_out = tokens // 4
    return pl.pallas_call(
        functools.partial(out_kernel, first_head, n_pairs),
        grid_spec=pltpu.PrefetchScalarGridSpec(
            num_scalar_prefetch=1,
            grid=(n_steps,),
            in_specs=[tok(width)] * 4 + [tok(2 * LANES), tok(LANES), tok(LANES), tail, tail, pl.BlockSpec((OUT_CHUNKS, LANES, width), lambda i, who: (i, 0, 0)), pl.BlockSpec((OUT_CHUNKS, 8, width), lambda i, who: (i, 0, 0)), state, state, state] + [small(v) for v in logs] + [small(skip), ANY],
            out_specs=[pl.BlockSpec((rows_out, width), lambda i, who: (0, 0))] * 4,
            scratch_shapes=[pltpu.VMEM((LANES, width), F32), pltpu.VMEM((LANES, width), F32), pltpu.VMEM((8, width), F32), pltpu.VMEM((OUT_CHUNKS * CHUNK, width), BF16), pltpu.VMEM((LANES, width), BF16), pltpu.VMEM((LANES, 2 * width), BF16)] + [pltpu.VMEM((OUT_CHUNKS, LANES, width), BF16)] * 2,
        ),
        out_shape=[jax.ShapeDtypeStruct((rows_out, width), BF16)] * 4,
        compiler_params=params(),
        cost_estimate=cost(24 * tokens * width * 256, 8 * tokens * width),
        name="outputs",
    )(who, u, z, scaled, ends, bc, sums[0], sums[1], *tails, gloc, suf, *got, *logs, skip, after)


def solution(mesh):
    n_sp, n_dp = mesh.shape['sp'], mesh.shape['dp']

    def swap(val, axis, slot):
        return lax.ppermute(val, axis, [(i, i ^ slot) for i in range(4)])

    def later(vals, after):
        return list(lax.optimization_barrier((*vals, after)))[:-1]

    def device_fn(x_blk, w_z, w_x, w_bc, w_dt, a_neg, dt_bias, d_skip, w_out):
        heads = a_neg.shape[0]
        head_dim = w_x.shape[1] // heads
        tp_index = lax.axis_index('tp')
        sp_index = lax.axis_index('sp')

        piece_rows = w_out.shape[0] // (n_dp * n_sp)
        mine = (sp_index % 2) * (n_dp * n_sp // 2) + lax.axis_index('dp') * (n_sp // 2) + sp_index // 2
        piece = lax.dynamic_slice_in_dim(w_out, mine * piece_rows, piece_rows, axis=0)
        one = swap(piece, 'tp', 1)
        two = swap(piece, 'tp', 2)
        core = sp_index % 2

        def plane(v):
            return lax.all_gather(v, ('dp', 'sp'), tiled=True, axis_index_groups=[[0, 2, 4, 6], [1, 3, 5, 7]])

        def whole(half):
            other = swap(half, 'sp', 1)
            return jnp.where(core == 0, jnp.concatenate([half, other]), jnp.concatenate([other, half]))

        n_tiles = w_x.shape[1] // 256
        first = n_tiles * 2 // 5
        (t_a, n_a), (t_b, n_b) = (0, first), (first, n_tiles - first)
        head_b = first * 256 // head_dim
        who = jnp.stack([tp_index, sp_index])
        skip = d_skip[None, :]

        def exchange(s_fwd, s_bwd):
            return [swap(jnp.where(sp_index < (sp_index ^ s), s_fwd, s_bwd), 'sp', s) for s in (1, 2, 3)]

        def send(pieces):
            return [pieces[0]] + [swap(pieces[s], 'tp', s) for s in (1, 2, 3)]

        bc, cum3, nexc3, dt3, tail1, tail2, block_log, u_a = prep(x_blk, w_bc, w_dt.T, dt_bias[None, :], a_neg[None, :], w_x, n_a)
        logs = [swap(block_log, 'sp', s) for s in (1, 2, 3)]
        one, = later((one,), block_log)
        w_one = plane(one)
        gloc_a, suf_a, s_fwd, s_bwd, ut_a, vf_a = chunk_states(u_a, bc, (cum3, nexc3, dt3), one, 0, 2 * n_a)
        got_a = exchange(s_fwd, s_bwd)
        two, = later((two,), s_fwd)
        three = swap(two, 'tp', 1)
        w_two = plane(two)
        z_a, u_b = project(x_blk, [(w_z, t_a, n_a), (w_x, t_b, n_b)], two)
        g_a = chunk_outputs(who, u_a, z_a, bc, (cum3, nexc3), (tail1, tail2), (gloc_a, suf_a, ut_a, vf_a), got_a, logs, skip, three, 0, 2 * n_a)
        got_g_a = send(g_a)
        w_three = plane(three)
        gloc_b, suf_b, s_fwd, s_bwd, ut_b, vf_b = chunk_states(u_b, bc, (cum3, nexc3, dt3), g_a[0], head_b, 2 * n_b)
        got_b = exchange(s_fwd, s_bwd)
        z_b, = project(x_blk, [(w_z, t_b, n_b)], s_fwd)
        g_b = chunk_outputs(who, u_b, z_b, bc, (cum3, nexc3), (tail1, tail2), (gloc_b, suf_b, ut_b, vf_b), got_b, logs, skip, z_b, head_b, 2 * n_b)
        got_g_b = send(g_b)

        w_one, w_two, w_three = [whole(half) for half in later((w_one, w_two, w_three), g_b[0])]
        total = add_products(who, x_blk, [(got_g_a[0], w_out, t_a), (got_g_b[0], w_out, t_b)], F32)
        total = add_products(who, total, [(got_g_a[1], w_one, t_a), (got_g_a[2], w_two, t_a), (got_g_a[3], w_three, t_a)], F32)
        total = add_products(who, total, [(got_g_b[1], w_one, t_b), (got_g_b[2], w_two, t_b)], F32)
        return add_products(who, total, [(got_g_b[3], w_three, t_b)], BF16)

    in_specs = (P(('dp', 'sp'), None), P(None, 'tp'), P(None, 'tp'), P(None, None), P(None, 'tp'), P('tp'), P('tp'), P('tp'), P('tp', None))
    out_specs = P(('dp', 'sp', 'tp'), None)
    return jax.shard_map(device_fn, mesh=mesh, in_specs=in_specs, out_specs=out_specs, check_vma=False)
```

```python
import functools

import jax
import jax.numpy as jnp
from jax import lax
from jax.experimental import pallas as pl
from jax.experimental.pallas import tpu as pltpu
from jax.sharding import PartitionSpec as P


CHUNK = 128
LANES = 128
SLOT = 32
STATE_CHUNKS = 4
OUT_CHUNKS = 2
OUT_AHEAD = 2
SUM_MIB = 24
F32 = jnp.float32
BF16 = jnp.bfloat16


def split3(val, lane, last):
    first = val.astype(BF16).astype(F32)
    rest = val - first
    second = rest.astype(BF16).astype(F32)
    third = rest - second
    return jnp.where(lane < SLOT, first, jnp.where(lane < 2 * SLOT, second, jnp.where(lane < 3 * SLOT, third, last))).astype(BF16)


def prep_kernel(n_tiles, x_ref, wbc_ref, wdt_ref, bias_ref, a_ref, *refs):
    bc_ref, cum_ref, nexc_ref, dt_ref, tail1_ref, tail2_ref, log_ref, u_ref = refs[n_tiles:n_tiles + 8]
    w_buf, par, pick = refs[-8:-5]
    heads = bias_ref.shape[1]
    row = lax.broadcasted_iota(jnp.int32, (CHUNK, LANES), 0)
    lane = lax.broadcasted_iota(jnp.int32, (CHUNK, LANES), 1)

    @pl.when(pl.program_id(0) == 0)
    def _():
        log_ref[...] = jnp.zeros_like(log_ref)
        w_buf[...] = jnp.zeros_like(w_buf)
        par[...] = jnp.zeros_like(par)
        for k in range(3):
            w_buf[k * SLOT:k * SLOT + heads, :] = wdt_ref[...]
            par[0:1, k * SLOT:k * SLOT + heads] = bias_ref[...]
            par[1:2, k * SLOT:k * SLOT + heads] = a_ref[...]
        out_row = lax.broadcasted_iota(jnp.int32, pick.shape, 0)
        term = lax.broadcasted_iota(jnp.int32, pick.shape, 1)
        head, which = out_row // 16, out_row % 16
        pick[...] = jnp.where((which < 3) & (term == which * SLOT + head), -1.0, 0.0).astype(BF16)

    x_val = x_ref[...]
    raw = lax.dot_general(x_val, w_buf[...], (((1,), (1,)), ((), ())), preferred_element_type=F32) + par[0:1, :]

    def u_tile(i):
        u_ref[:, i * 256:(i + 1) * 256] = jnp.dot(x_val, refs[i][...], preferred_element_type=F32).astype(BF16)

    u_tile(0)
    dt_val = jnp.maximum(raw, 0.0) + jnp.log1p(jnp.exp(-jnp.abs(raw)))
    la_val = jnp.maximum(dt_val * par[1:2, :], -1000.0)
    tri = jnp.where(row >= lane, 1.0, 0.0).astype(BF16)
    parts = [slice(c * CHUNK, (c + 1) * CHUNK) for c in range(x_val.shape[0] // CHUNK)]
    sums = []
    for part in parts:
        la_c = la_val[part, :]
        first = la_c.astype(BF16)
        rest = la_c - first.astype(F32)
        second = rest.astype(BF16)
        third = (rest - second.astype(F32)).astype(BF16)
        sums.append(sum(jnp.dot(tri, t, preferred_element_type=F32) for t in (first, second, third)))
    for i in range(1, n_tiles):
        u_tile(i)
    one = jnp.where(lane < 3 * SLOT + 3, 1.0, 0.0)
    for part, cum in zip(parts, sums):
        cum_ref[part, :] = split3(cum, lane, one)
        nexc_ref[part, :] = split3(la_val[part, :] - cum, lane, one)
        dt_ref[part, :] = split3(dt_val[part, :], lane, 0.0)
        log_ref[...] += cum[CHUNK - 1:CHUNK, :]
    bc_ref[...] = jnp.dot(x_val, wbc_ref[...], preferred_element_type=F32).astype(BF16)
    across = (((1,), (1,)), ((), ()))
    tail1_ref[...] = lax.dot_general(pick[...], cum_ref[...], across, preferred_element_type=F32).astype(BF16)
    tail2_ref[...] = lax.dot_general(pick[...], nexc_ref[...], across, preferred_element_type=F32).astype(BF16)


def first_kernel(n_tiles, *refs):
    prep_kernel(n_tiles, *refs)
    bc_ref, cum_ref, nexc_ref, dt_ref, _, _, _, u_ref = refs[5 + n_tiles:13 + n_tiles]
    state_kernel(0, 2 * n_tiles, u_ref, bc_ref, cum_ref, nexc_ref, dt_ref, *refs[13 + n_tiles:-8], *refs[-5:])


def next_kernel(first_head, n_tiles, x_ref, bc_ref, cum_ref, nexc_ref, dt_ref, *refs):
    u_ref = refs[n_tiles + 1]
    project_into(u_ref, x_ref[...], refs[:n_tiles])
    state_kernel(first_head, 2 * n_tiles, u_ref, bc_ref, cum_ref, nexc_ref, dt_ref, *refs[n_tiles + 2:])


def project_into(o_ref, x_val, w_refs):
    for i, w_ref in enumerate(w_refs):
        o_ref[:, i * 256:(i + 1) * 256] = jnp.dot(x_val, w_ref[...], preferred_element_type=F32).astype(BF16)


def sum_kernel(n_tiles, n_pieces, acc_ref, *refs):
    o_ref = refs[-1]
    total = acc_ref[...].astype(F32)
    for i in range(n_pieces):
        g_ref, w_refs = refs[sum(n_tiles[:i]) + i], refs[sum(n_tiles[:i]) + i + 1:sum(n_tiles[:i + 1]) + i + 1]
        for t in range(n_tiles[i]):
            total = total + jnp.dot(g_ref[:, t * 256:(t + 1) * 256], w_refs[t][...], preferred_element_type=F32)
    o_ref[...] = total.astype(o_ref.dtype)


def spread_matrix(shape, first_head, lanes_per_head):
    term = lax.broadcasted_iota(jnp.int32, shape, 0)
    lane = lax.broadcasted_iota(jnp.int32, shape, 1)
    return jnp.where((term % SLOT == first_head + lane // lanes_per_head) & (term < 3 * SLOT), 1.0, 0.0).astype(BF16)


def pair_cols(cols, head, low):
    return jnp.where(low, jnp.broadcast_to(cols[:, head:head + 1], low.shape), jnp.broadcast_to(cols[:, head + 1:head + 2], low.shape))


def state_kernel(first_head, n_pairs, u_ref, bc_ref, cum_ref, nexc_ref, dt_ref, gloc_ref, suf_ref, sf_ref, sb_ref, ut_ref, vf_ref, g_acc, f_acc, suf_acc, v_buf, spread):
    step = pl.program_id(0)
    width = n_pairs * LANES

    @pl.when(step == 0)
    def _():
        g_acc[...] = jnp.zeros_like(g_acc)
        f_acc[...] = jnp.zeros_like(f_acc)
        suf_acc[...] = jnp.zeros_like(suf_acc)
        spread[...] = spread_matrix(spread.shape, first_head, LANES // 2)

    def terms_of(c, p):
        rows = slice(c * CHUNK, (c + 1) * CHUNK)
        wide = slice(p * LANES, min(p + 2, n_pairs) * LANES)
        return [jnp.dot(r[rows, :], spread[:, wide], preferred_element_type=F32) for r in (cum_ref, nexc_ref, dt_ref)]

    def finish(c, total):
        rows = slice(c * CHUNK, (c + 1) * CHUNK)
        suffix = suf_acc[...]
        suf_ref[c, 0:1, :] = suffix[0:1, :]
        suf_ref[c, 1:2, :] = total
        sums = lax.dot_general(bc_ref[rows, :LANES], v_buf[rows, :], (((0,), (0,)), ((), ())), preferred_element_type=F32)
        back = g_acc[...]
        gloc_ref[c] = back
        g_acc[...] = back * jnp.exp(total) + sums[:, :width]
        f_acc[...] += sums[:, width:] * jnp.exp(suffix[0:1, :])
        suf_acc[...] = suffix + total

    order = [(c, p) for c in reversed(range(STATE_CHUNKS)) for p in range(0, n_pairs, 2)]
    ahead = terms_of(*order[0])
    for i, (c, p0) in enumerate(order):
        terms = ahead
        if i + 1 < len(order):
            ahead = terms_of(*order[i + 1])
        rows = slice(c * CHUNK, (c + 1) * CHUNK)
        if p0 == 0:
            totals = []
        for p in range(p0, min(p0 + 2, n_pairs)):
            part = slice(p * LANES, (p + 1) * LANES)
            half = slice((p - p0) * LANES, (p - p0 + 1) * LANES)
            cum, nexc, dt_val = [t[:, half] for t in terms]
            scaled = u_ref[rows, part].astype(F32) * dt_val
            total = cum[CHUNK - 1:CHUNK, :]
            totals.append(total)
            ut_ref[rows, part] = scaled.astype(BF16)
            v_buf[rows, part] = (scaled * jnp.exp(-nexc)).astype(BF16)
            end = (scaled * jnp.exp(total - cum)).astype(BF16)
            vf_ref[rows, part] = end
            v_buf[rows, slice(width + p * LANES, width + (p + 1) * LANES)] = end
        if p0 + 2 >= n_pairs:
            finish(c, jnp.concatenate(totals, axis=1))

    @pl.when(step == pl.num_programs(0) - 1)
    def _():
        sf_ref[...] = f_acc[...].astype(BF16)
        sb_ref[...] = g_acc[...].astype(BF16)


def peer_weights(sp_index, logs):
    fwd, bwd = [], []
    for s in (1, 2, 3):
        peer = sp_index ^ s
        between = jnp.zeros_like(logs[0])
        for o in (1, 2, 3):
            other = sp_index ^ o
            inside = (other > jnp.minimum(peer, sp_index)) & (other < jnp.maximum(peer, sp_index))
            between = between + jnp.where(inside, logs[o - 1], 0.0)
        decay = jnp.exp(between)
        fwd.append(jnp.where(peer < sp_index, decay, 0.0))
        bwd.append(jnp.where(peer > sp_index, decay, 0.0))
    return fwd, bwd


def out_kernel(first_head, n_pairs, who_ref, u_ref, x_ref, ut_ref, vf_ref, bc_ref, cum_ref, nexc_ref, tail1_ref, tail2_ref, gloc_ref, suf_ref, r1_ref, r2_ref, r3_ref, l1_ref, l2_ref, l3_ref, skip_ref, after_ref, *refs):
    w_refs, (o0_ref, o1_ref, o2_ref, o3_ref, f_acc, hb_acc, skip_buf, g_buf, spread, pick, fwd_buf, bwd_buf, z_ref) = refs[:n_pairs // 2], refs[n_pairs // 2:]
    step = pl.program_id(0)
    project_into(z_ref, x_ref[...], w_refs)

    @pl.when(step == 0)
    def _():
        low8 = lax.broadcasted_iota(jnp.int32, (8, LANES), 1) < LANES // 2
        fwd, bwd = peer_weights(who_ref[1], [r[...] for r in (l1_ref, l2_ref, l3_ref)])
        got = (r1_ref, r2_ref, r3_ref)
        spread[...] = spread_matrix(spread.shape, first_head, LANES // 2)
        pick[...] = spread_matrix(pick.shape, first_head, LANES)
        for p in range(n_pairs):
            part = slice(p * LANES, (p + 1) * LANES)
            over = lambda v: pair_cols(v, first_head + 2 * p, low8)
            skip_buf[:, part] = 2.0 * over(jnp.broadcast_to(skip_ref[...], (8, skip_ref.shape[1])))
            f_acc[:, part] = sum(got[s][:, part].astype(F32) * over(fwd[s])[0:1, :] for s in range(3))
            hb_acc[:, part] = sum(got[s][:, part].astype(F32) * over(bwd[s])[0:1, :] for s in range(3))

    row = lax.broadcasted_iota(jnp.int32, (CHUNK, LANES), 0)
    lane = lax.broadcasted_iota(jnp.int32, (CHUNK, LANES), 1)
    low = lane < LANES // 2
    zeros = jnp.zeros((16, 2 * LANES), BF16)
    grams = []
    for c in range(OUT_CHUNKS):
        rows = slice(c * CHUNK, (c + 1) * CHUNK)
        b_val = bc_ref[rows, :LANES]
        gram = lax.dot_general(bc_ref[rows, LANES:], b_val, (((1,), (1,)), ((), ())), preferred_element_type=F32)
        grams.append(jnp.where(row == lane, 2.0 * gram, gram))
        sums = lax.dot_general(b_val, vf_ref[rows, :], (((0,), (0,)), ((), ())), preferred_element_type=F32)
        state = f_acc[...]
        fwd_buf[c] = state.astype(BF16)
        bwd_buf[c] = (gloc_ref[c] + hb_acc[...] * jnp.exp(suf_ref[c, 0:1, :])).astype(BF16)
        f_acc[...] = state * jnp.exp(suf_ref[c, 1:2, :]) + sums

    def weights(c, p):
        rows = slice(c * CHUNK, (c + 1) * CHUNK)
        head = first_head + 2 * p

        def differences(terms_ref, tail_ref):
            tails = jnp.concatenate([tail_ref[16 * h:16 * h + 16, rows] for h in (head, head + 1)], axis=1)
            chosen = pick[0:3 * SLOT, slice(2 * p * LANES, 2 * (p + 1) * LANES)]
            return jnp.dot(terms_ref[rows, :], jnp.concatenate([chosen, tails, zeros], axis=0), preferred_element_type=F32)

        decay = jnp.exp(jnp.minimum(differences(cum_ref, tail1_ref), differences(nexc_ref, tail2_ref)))
        return jnp.concatenate([(decay[:, :LANES] * grams[c]).astype(BF16), (decay[:, LANES:] * grams[c]).astype(BF16)], axis=1)

    def passed(c, p):
        rows = slice(c * CHUNK, (c + 1) * CHUNK)
        part = slice(p * LANES, (p + 1) * LANES)
        c_val = bc_ref[rows, LANES:]
        cum = jnp.dot(cum_ref[rows, :], spread[:, part], preferred_element_type=F32)
        nexc = jnp.dot(nexc_ref[rows, :], spread[:, part], preferred_element_type=F32)
        y_fwd = jnp.dot(c_val, fwd_buf[c, :, part], preferred_element_type=F32)
        y_bwd = jnp.dot(c_val, bwd_buf[c, :, part], preferred_element_type=F32)
        y_val = jnp.exp(cum) * y_fwd + jnp.exp(suf_ref[c, 1:2, part] + nexc) * y_bwd
        return y_val + skip_buf[0:1, part] * u_ref[rows, part].astype(F32)

    order = [(c, p) for c in range(OUT_CHUNKS) for p in range(n_pairs)]
    ahead = [weights(*order[i]) for i in range(OUT_AHEAD)]
    for i, (c, p) in enumerate(order):
        mix = ahead.pop(0)
        if i + OUT_AHEAD < len(order):
            ahead.append(weights(*order[i + OUT_AHEAD]))
        y_val = passed(c, p)
        rows = slice(c * CHUNK, (c + 1) * CHUNK)
        part = slice(p * LANES, (p + 1) * LANES)
        scaled = ut_ref[rows, part]
        none = jnp.zeros_like(scaled)
        rhs = jnp.concatenate([jnp.where(low, scaled, none), jnp.where(low, none, scaled)], axis=0)
        y_val = jnp.dot(mix, rhs, preferred_element_type=F32) + y_val
        z_val = z_ref[rows, part].astype(F32)
        g_buf[rows, part] = (y_val * (z_val * jax.nn.sigmoid(z_val))).astype(BF16)

    steps = pl.num_programs(0) // 4
    slot = (step // steps) ^ who_ref[0]
    length = OUT_CHUNKS * CHUNK
    for s, o_ref in enumerate((o0_ref, o1_ref, o2_ref, o3_ref)):
        @pl.when(slot == s)
        def _():
            o_ref[pl.ds(pl.multiple_of((step % steps) * length, length), length), :] = g_buf[...]


def params(mib=62):
    return pltpu.CompilerParams(dimension_semantics=("arbitrary",), vmem_limit_bytes=mib << 20)


def cost(flops, moved):
    return pl.CostEstimate(flops=int(flops), bytes_accessed=int(moved), transcendentals=0)


ANY = pl.BlockSpec(memory_space=pl.ANY)


def w_specs(w, first_tile, n_tiles):
    return [pl.BlockSpec((w.shape[0], 256), functools.partial(lambda t, i: (0, t), first_tile + t), pipeline_mode=pl.Buffered(1)) for t in range(n_tiles)]


def state_parts(tokens, width, tok, at):
    n_chunks = tokens // CHUNK
    whole = pl.BlockSpec((LANES, width), lambda i: (0, 0))
    specs = [tok(width), pl.BlockSpec((STATE_CHUNKS, LANES, width), lambda i: (at(i), 0, 0)), pl.BlockSpec((STATE_CHUNKS, 8, width), lambda i: (at(i), 0, 0)), whole, whole, tok(width), tok(width)]
    shapes = [jax.ShapeDtypeStruct((tokens, width), BF16), jax.ShapeDtypeStruct((n_chunks, LANES, width), F32), jax.ShapeDtypeStruct((n_chunks, 8, width), F32)] + [jax.ShapeDtypeStruct((LANES, width), BF16)] * 2 + [jax.ShapeDtypeStruct((tokens, width), BF16)] * 2
    scratch = [pltpu.VMEM((LANES, width), F32), pltpu.VMEM((LANES, width), F32), pltpu.VMEM((8, width), F32), pltpu.VMEM((STATE_CHUNKS * CHUNK, 2 * width), BF16), pltpu.VMEM((LANES, width), BF16)]
    return specs, shapes, scratch


def first_group(x_blk, w_bc, w_dt_rows, bias, a_neg, w_x, n_tiles):
    tokens, d_model = x_blk.shape
    tile = STATE_CHUNKS * CHUNK
    width = 256 * n_tiles
    at = lambda i: tokens // tile - 1 - i
    whole = lambda a: pl.BlockSpec(a.shape, lambda i: (0, 0), pipeline_mode=pl.Buffered(1))
    tok = lambda w: pl.BlockSpec((tile, w), lambda i: (at(i), 0))
    heads = bias.shape[1]
    tail = pl.BlockSpec((16 * heads, tile), lambda i: (0, at(i)))
    specs, shapes, scratch = state_parts(tokens, width, tok, at)
    return pl.pallas_call(
        functools.partial(first_kernel, n_tiles),
        grid=(tokens // tile,),
        in_specs=[tok(d_model), whole(w_bc), whole(w_dt_rows), whole(bias), whole(a_neg)] + w_specs(w_x, 0, n_tiles),
        out_specs=[tok(2 * LANES), tok(LANES), tok(LANES), tok(LANES), tail, tail, pl.BlockSpec((8, LANES), lambda i: (0, 0))] + specs,
        out_shape=[jax.ShapeDtypeStruct((tokens, 2 * LANES), BF16)] + [jax.ShapeDtypeStruct((tokens, LANES), BF16)] * 3 + [jax.ShapeDtypeStruct((16 * heads, tokens), BF16)] * 2 + [jax.ShapeDtypeStruct((8, LANES), F32)] + shapes,
        scratch_shapes=[pltpu.VMEM((LANES, d_model), BF16), pltpu.VMEM((8, LANES), F32), pltpu.VMEM((16 * heads, LANES), BF16)] + scratch,
        compiler_params=params(),
        cost_estimate=cost(2 * tokens * d_model * (1024 + width), 2 * tokens * d_model),
        name="first_group",
    )(x_blk, w_bc, w_dt_rows, bias, a_neg, *([w_x] * n_tiles))


def next_group(x_blk, w_x, first_tile, n_tiles, bc, sums, after, first_head):
    tokens, d_model = x_blk.shape
    tile = STATE_CHUNKS * CHUNK
    at = lambda i: tokens // tile - 1 - i
    tok = lambda w: pl.BlockSpec((tile, w), lambda i: (at(i), 0))
    specs, shapes, scratch = state_parts(tokens, 256 * n_tiles, tok, at)
    return pl.pallas_call(
        functools.partial(next_kernel, first_head, n_tiles),
        grid=(tokens // tile,),
        in_specs=[tok(d_model), tok(2 * LANES), tok(LANES), tok(LANES), tok(LANES)] + w_specs(w_x, first_tile, n_tiles) + [ANY],
        out_specs=specs,
        out_shape=shapes,
        scratch_shapes=scratch,
        compiler_params=params(),
        cost_estimate=cost(2 * tokens * d_model * (512 + 256 * n_tiles), 2 * tokens * d_model),
        name="next_group",
    )(x_blk, bc, *sums, *([w_x] * n_tiles), after)


def add_products(who, acc, pieces, out_dtype):
    rows, d_model = pieces[0][0].shape[0], acc.shape[1]
    tile = min(512, d_model)
    n_tiles = [g.shape[1] // 256 for g, _, _ in pieces]
    mine = acc.shape[0] > rows
    specs, args = [pl.BlockSpec((rows, tile), lambda i, who: (who[0] if mine else 0, i))], [acc]
    for (g, w, tile0), count in zip(pieces, n_tiles):
        specs.append(pl.BlockSpec(g.shape, lambda i, who: (0, 0)))
        specs += [pl.BlockSpec((256, tile), functools.partial(lambda t, i, who: (t, i), tile0 + t)) for t in range(count)]
        args += [g] + [w] * count

    def body(who_ref, *refs):
        sum_kernel(n_tiles, len(pieces), *refs)

    return pl.pallas_call(
        body,
        grid_spec=pltpu.PrefetchScalarGridSpec(num_scalar_prefetch=1, grid=(d_model // tile,), in_specs=specs, out_specs=pl.BlockSpec((rows, tile), lambda i, who: (0, i))),
        out_shape=jax.ShapeDtypeStruct((rows, d_model), out_dtype),
        compiler_params=params(SUM_MIB),
        cost_estimate=cost(2 * rows * d_model * 256 * sum(n_tiles), 2 * rows * d_model),
        name="add_products",
    )(who, *args)


def chunk_outputs(who, u, x_blk, w_z, first_tile, bc, sums, tails, local, got, logs, skip, after, first_head, n_pairs):
    tokens, width = u.shape
    n_steps = tokens // (OUT_CHUNKS * CHUNK)
    gloc, suf, scaled, ends = local
    tail = pl.BlockSpec((tails[0].shape[0], OUT_CHUNKS * CHUNK), lambda i, who: (0, i))
    tok = lambda w: pl.BlockSpec((OUT_CHUNKS * CHUNK, w), lambda i, who: (i, 0))
    state = pl.BlockSpec((LANES, width), lambda i, who: (0, 0))
    small = lambda a: pl.BlockSpec(a.shape, lambda i, who: (0, 0))
    rows_out = tokens // 4
    return pl.pallas_call(
        functools.partial(out_kernel, first_head, n_pairs),
        grid_spec=pltpu.PrefetchScalarGridSpec(
            num_scalar_prefetch=1,
            grid=(n_steps,),
            in_specs=[tok(width), tok(x_blk.shape[1]), tok(width), tok(width)] + [tok(2 * LANES), tok(LANES), tok(LANES), tail, tail, pl.BlockSpec((OUT_CHUNKS, LANES, width), lambda i, who: (i, 0, 0)), pl.BlockSpec((OUT_CHUNKS, 8, width), lambda i, who: (i, 0, 0)), state, state, state] + [small(v) for v in logs] + [small(skip), ANY] + [pl.BlockSpec((w_z.shape[0], 256), functools.partial(lambda t, i, who: (0, t), first_tile + t), pipeline_mode=pl.Buffered(1)) for t in range(n_pairs // 2)],
            out_specs=[pl.BlockSpec((rows_out, width), lambda i, who: (0, 0))] * 4,
            scratch_shapes=[pltpu.VMEM((LANES, width), F32), pltpu.VMEM((LANES, width), F32), pltpu.VMEM((8, width), F32), pltpu.VMEM((OUT_CHUNKS * CHUNK, width), BF16), pltpu.VMEM((LANES, width), BF16), pltpu.VMEM((LANES, 2 * width), BF16)] + [pltpu.VMEM((OUT_CHUNKS, LANES, width), BF16)] * 2 + [pltpu.VMEM((OUT_CHUNKS * CHUNK, width), BF16)],
        ),
        out_shape=[jax.ShapeDtypeStruct((rows_out, width), BF16)] * 4,
        compiler_params=params(),
        cost_estimate=cost(24 * tokens * width * 256, 8 * tokens * width),
        name="outputs",
    )(who, u, x_blk, scaled, ends, bc, sums[0], sums[1], *tails, gloc, suf, *got, *logs, skip, after, *([w_z] * (n_pairs // 2)))


def solution(mesh):
    n_sp, n_dp = mesh.shape['sp'], mesh.shape['dp']

    def swap(val, axis, slot):
        return lax.ppermute(val, axis, [(i, i ^ slot) for i in range(4)])

    def later(vals, after):
        return list(lax.optimization_barrier((*vals, after)))[:-1]

    def device_fn(x_blk, w_z, w_x, w_bc, w_dt, a_neg, dt_bias, d_skip, w_out):
        heads = a_neg.shape[0]
        head_dim = w_x.shape[1] // heads
        tp_index = lax.axis_index('tp')
        sp_index = lax.axis_index('sp')

        piece_rows = w_out.shape[0] // (n_dp * n_sp)
        mine = lax.axis_index('dp') * n_sp + sp_index
        piece = lax.dynamic_slice_in_dim(w_out, mine * piece_rows, piece_rows, axis=0)
        one = swap(piece, 'tp', 1)
        two = swap(piece, 'tp', 2)
        plane = lambda v: lax.all_gather(v, ('dp', 'sp'), tiled=True)

        n_tiles = w_x.shape[1] // 256
        first = n_tiles * 2 // 5
        (t_a, n_a), (t_b, n_b) = (0, first), (first, n_tiles - first)
        head_b = first * 256 // head_dim
        who = jnp.stack([tp_index, sp_index])
        skip = d_skip[None, :]

        def exchange(s_fwd, s_bwd):
            return [swap(jnp.where(sp_index < (sp_index ^ s), s_fwd, s_bwd), 'sp', s) for s in (1, 2, 3)]

        def send(pieces):
            return [pieces[0]] + [swap(pieces[s], 'tp', s) for s in (1, 2, 3)]

        bc, cum3, nexc3, dt3, tail1, tail2, block_log, u_a, gloc, suf, s_fwd, s_bwd, ut, vf = first_group(x_blk, w_bc, w_dt.T, dt_bias[None, :], a_neg[None, :], w_x, n_a)
        local_a = (gloc, suf, ut, vf)
        logs = [swap(block_log, 'sp', s) for s in (1, 2, 3)]
        got_a = exchange(s_fwd, s_bwd)
        one, = later((one,), block_log)
        w_one = plane(one)
        u_b, gloc, suf, s_fwd, s_bwd, ut, vf = next_group(x_blk, w_x, t_b, n_b, bc, (cum3, nexc3, dt3), one, head_b)
        local_b = (gloc, suf, ut, vf)
        got_b = exchange(s_fwd, s_bwd)
        g_a = chunk_outputs(who, u_a, x_blk, w_z, t_a, bc, (cum3, nexc3), (tail1, tail2), local_a, got_a, logs, skip, u_b, 0, 2 * n_a)
        got_g_a = send(g_a)
        two, = later((two,), g_a[0])
        three = swap(two, 'tp', 1)
        w_two = plane(two)
        g_b = chunk_outputs(who, u_b, x_blk, w_z, t_b, bc, (cum3, nexc3), (tail1, tail2), local_b, got_b, logs, skip, two, head_b, 2 * n_b)
        got_g_b = send(g_b)
        w_three = plane(three)

        total = add_products(who, x_blk, [(got_g_a[0], w_out, t_a), (got_g_b[0], w_out, t_b)], F32)
        total = add_products(who, total, [(got_g_a[1], w_one, t_a), (got_g_b[1], w_one, t_b)], F32)
        total = add_products(who, total, [(got_g_a[2], w_two, t_a), (got_g_b[2], w_two, t_b)], F32)
        return add_products(who, total, [(got_g_a[3], w_three, t_a), (got_g_b[3], w_three, t_b)], BF16)

    in_specs = (P(('dp', 'sp'), None), P(None, 'tp'), P(None, 'tp'), P(None, None), P(None, 'tp'), P('tp'), P('tp'), P('tp'), P('tp', None))
    out_specs = P(('dp', 'sp', 'tp'), None)
    return jax.shard_map(device_fn, mesh=mesh, in_specs=in_specs, out_specs=out_specs, check_vma=False)
```

```python
import functools

import jax
import jax.numpy as jnp
from jax import lax
from jax.experimental import pallas as pl
from jax.experimental.pallas import tpu as pltpu
from jax.sharding import PartitionSpec as P


CHUNK = 128
LANES = 128
SLOT = 32
STATE_CHUNKS = 4
OUT_CHUNKS = 2
OUT_AHEAD = 2
SUM_MIB = 62
F32 = jnp.float32
BF16 = jnp.bfloat16


def split3(val, lane, last):
    first = val.astype(BF16).astype(F32)
    rest = val - first
    second = rest.astype(BF16).astype(F32)
    third = rest - second
    return jnp.where(lane < SLOT, first, jnp.where(lane < 2 * SLOT, second, jnp.where(lane < 3 * SLOT, third, last))).astype(BF16)


def prep_kernel(n_tiles, x_ref, wbc_ref, wdt_ref, bias_ref, a_ref, *refs):
    bc_ref, cum_ref, nexc_ref, dt_ref, tail1_ref, tail2_ref, u_ref = refs[n_tiles:n_tiles + 7]
    w_buf, par, pick = refs[-8:-5]
    heads = bias_ref.shape[1]
    row = lax.broadcasted_iota(jnp.int32, (CHUNK, LANES), 0)
    lane = lax.broadcasted_iota(jnp.int32, (CHUNK, LANES), 1)

    @pl.when(pl.program_id(0) == 0)
    def _():
        w_buf[...] = jnp.zeros_like(w_buf)
        par[...] = jnp.zeros_like(par)
        for k in range(3):
            w_buf[k * SLOT:k * SLOT + heads, :] = wdt_ref[...]
            par[0:1, k * SLOT:k * SLOT + heads] = bias_ref[...]
            par[1:2, k * SLOT:k * SLOT + heads] = a_ref[...]
        out_row = lax.broadcasted_iota(jnp.int32, pick.shape, 0)
        term = lax.broadcasted_iota(jnp.int32, pick.shape, 1)
        head, which = out_row // 16, out_row % 16
        pick[...] = jnp.where((which < 3) & (term == which * SLOT + head), -1.0, 0.0).astype(BF16)

    x_val = x_ref[...]
    raw = lax.dot_general(x_val, w_buf[...], (((1,), (1,)), ((), ())), preferred_element_type=F32) + par[0:1, :]

    project_tile(u_ref, x_ref, refs[0], 0)
    dt_val = jnp.maximum(raw, 0.0) + jnp.log1p(jnp.exp(-jnp.abs(raw)))
    la_val = jnp.maximum(dt_val * par[1:2, :], -1000.0)
    tri = jnp.where(row >= lane, 1.0, 0.0).astype(BF16)
    parts = [slice(c * CHUNK, (c + 1) * CHUNK) for c in range(x_val.shape[0] // CHUNK)]
    sums = []
    for part in parts:
        la_c = la_val[part, :]
        first = la_c.astype(BF16)
        rest = la_c - first.astype(F32)
        second = rest.astype(BF16)
        third = (rest - second.astype(F32)).astype(BF16)
        sums.append(sum(jnp.dot(tri, t, preferred_element_type=F32) for t in (first, second, third)))
    one = jnp.where(lane < 3 * SLOT + 3, 1.0, 0.0)
    for part, cum in zip(parts, sums):
        cum_ref[part, :] = split3(cum, lane, one)
        nexc_ref[part, :] = split3(la_val[part, :] - cum, lane, one)
        dt_ref[part, :] = split3(dt_val[part, :], lane, 0.0)
    bc_ref[...] = jnp.dot(x_val, wbc_ref[...], preferred_element_type=F32).astype(BF16)
    across = (((1,), (1,)), ((), ()))
    tail1_ref[...] = lax.dot_general(pick[...], cum_ref[...], across, preferred_element_type=F32).astype(BF16)
    tail2_ref[...] = lax.dot_general(pick[...], nexc_ref[...], across, preferred_element_type=F32).astype(BF16)


def first_kernel(n_tiles, who_ref, *refs):
    prep_kernel(n_tiles, *refs)
    bc_ref, cum_ref, nexc_ref, dt_ref, _, _, u_ref = refs[5 + n_tiles:12 + n_tiles]
    project = lambda t: project_tile(u_ref, refs[0], refs[5 + t], t) if t else None
    state_kernel(0, 2 * n_tiles, project, u_ref, bc_ref, cum_ref, nexc_ref, dt_ref, *refs[12 + n_tiles:-8], who_ref, *refs[-5:])


def next_kernel(first_head, n_tiles, who_ref, x_ref, bc_ref, cum_ref, nexc_ref, dt_ref, *refs):
    u_ref = refs[n_tiles + 1]
    project = lambda t: project_tile(u_ref, x_ref, refs[t], t)
    state_kernel(first_head, 2 * n_tiles, project, u_ref, bc_ref, cum_ref, nexc_ref, dt_ref, *refs[n_tiles + 2:-5], who_ref, *refs[-5:])


def project_tile(o_ref, x_ref, w_ref, t):
    o_ref[:, t * 256:(t + 1) * 256] = jnp.dot(x_ref[...], w_ref[...], preferred_element_type=F32).astype(BF16)


def sum_kernel(n_tiles, n_pieces, acc_ref, *refs):
    o_ref = refs[-1]
    total = acc_ref[...].astype(F32)
    for i in range(n_pieces):
        g_ref, w_refs = refs[sum(n_tiles[:i]) + i], refs[sum(n_tiles[:i]) + i + 1:sum(n_tiles[:i + 1]) + i + 1]
        for t in range(n_tiles[i]):
            total = total + jnp.dot(g_ref[:, t * 256:(t + 1) * 256], w_refs[t][...], preferred_element_type=F32)
    o_ref[...] = total.astype(o_ref.dtype)


def spread_matrix(shape, first_head, lanes_per_head):
    term = lax.broadcasted_iota(jnp.int32, shape, 0)
    lane = lax.broadcasted_iota(jnp.int32, shape, 1)
    return jnp.where((term % SLOT == first_head + lane // lanes_per_head) & (term < 3 * SLOT), 1.0, 0.0).astype(BF16)


def pair_cols(cols, head, low):
    return jnp.where(low, jnp.broadcast_to(cols[:, head:head + 1], low.shape), jnp.broadcast_to(cols[:, head + 1:head + 2], low.shape))


def state_kernel(first_head, n_pairs, project, u_ref, bc_ref, cum_ref, nexc_ref, dt_ref, gloc_ref, suf_ref, s1_ref, s2_ref, s3_ref, ut_ref, vf_ref, who_ref, g_acc, f_acc, suf_acc, v_buf, spread):
    step = pl.program_id(0)
    width = n_pairs * LANES

    @pl.when(step == 0)
    def _():
        g_acc[...] = jnp.zeros_like(g_acc)
        f_acc[...] = jnp.zeros_like(f_acc)
        suf_acc[...] = jnp.zeros_like(suf_acc)
        spread[...] = spread_matrix(spread.shape, first_head, LANES // 2)

    def terms_of(c, t):
        rows = slice(c * CHUNK, (c + 1) * CHUNK)
        return [jnp.dot(r[rows, :], spread[:, t * 256:(t + 1) * 256], preferred_element_type=F32) for r in (cum_ref, nexc_ref, dt_ref)]

    project(0)
    order = [(c, t) for t in range(n_pairs // 2) for c in reversed(range(STATE_CHUNKS))]
    ahead = terms_of(*order[0])
    for i, (c, t) in enumerate(order):
        terms = ahead
        if i + 1 < len(order):
            ahead = terms_of(*order[i + 1])
        if c == STATE_CHUNKS - 1 and t + 1 < n_pairs // 2:
            project(t + 1)
        rows = slice(c * CHUNK, (c + 1) * CHUNK)
        wide = slice(t * 256, (t + 1) * 256)
        cum, nexc, dt_val = terms
        scaled = u_ref[rows, wide].astype(F32) * dt_val
        total = cum[CHUNK - 1:CHUNK, :]
        suffix = suf_acc[:, wide]
        ut_ref[rows, wide] = scaled.astype(BF16)
        v_buf[c, :, t * 512:t * 512 + 256] = (scaled * jnp.exp(-nexc)).astype(BF16)
        end = (scaled * jnp.exp(total - cum)).astype(BF16)
        vf_ref[rows, wide] = end
        v_buf[c, :, t * 512 + 256:(t + 1) * 512] = end
        suf_ref[c, 0:1, wide] = suffix[0:1, :]
        suf_ref[c, 1:2, wide] = total
        suf_acc[:, wide] = suffix + total
        sums = lax.dot_general(bc_ref[rows, :LANES], v_buf[c, :, t * 512:(t + 1) * 512], (((0,), (0,)), ((), ())), preferred_element_type=F32)
        back = g_acc[:, wide]
        gloc_ref[c, :, wide] = back
        g_acc[:, wide] = back * jnp.exp(total) + sums[:, :256]
        f_acc[:, wide] += sums[:, 256:] * jnp.exp(suffix[0:1, :])

    @pl.when(step == pl.num_programs(0) - 1)
    def _():
        row = lax.broadcasted_iota(jnp.int32, (16, width), 0)
        log = jnp.broadcast_to(suf_acc[0:1, :], (16, width))
        first = log.astype(BF16).astype(F32)
        second = (log - first).astype(BF16).astype(F32)
        third = log - first - second
        terms = jnp.where(row == 0, first, jnp.where(row == 1, second, jnp.where(row == 2, third, 0.0))).astype(BF16)
        me = who_ref[1]
        for s, s_ref in ((1, s1_ref), (2, s2_ref), (3, s3_ref)):
            s_ref[LANES:LANES + 16, :] = terms
            s_ref[0:LANES, :] = jnp.where(me < (me ^ s), f_acc[...], g_acc[...]).astype(BF16)


def peer_weights(sp_index, logs):
    fwd, bwd = [], []
    for s in (1, 2, 3):
        peer = sp_index ^ s
        between = jnp.zeros_like(logs[0])
        for o in (1, 2, 3):
            other = sp_index ^ o
            inside = (other > jnp.minimum(peer, sp_index)) & (other < jnp.maximum(peer, sp_index))
            between = between + jnp.where(inside, logs[o - 1], 0.0)
        decay = jnp.exp(between)
        fwd.append(jnp.where(peer < sp_index, decay, 0.0))
        bwd.append(jnp.where(peer > sp_index, decay, 0.0))
    return fwd, bwd


def out_kernel(first_head, n_pairs, who_ref, u_ref, x_ref, ut_ref, vf_ref, bc_ref, cum_ref, nexc_ref, tail1_ref, tail2_ref, gloc_ref, suf_ref, r1_ref, r2_ref, r3_ref, skip_ref, after_ref, *refs):
    w_refs, (o0_ref, o1_ref, o2_ref, o3_ref, f_acc, hb_acc, skip_buf, g_buf, spread, pick, fwd_buf, bwd_buf, z_ref) = refs[:n_pairs // 2], refs[n_pairs // 2:]
    step = pl.program_id(0)

    @pl.when(step == 0)
    def _():
        low8 = lax.broadcasted_iota(jnp.int32, (8, LANES), 1) < LANES // 2
        got = (r1_ref, r2_ref, r3_ref)
        logs = [r[LANES:LANES + 16, :].astype(F32) for r in got]
        fwd, bwd = peer_weights(who_ref[1], [v[0:1, :] + v[1:2, :] + v[2:3, :] for v in logs])
        spread[...] = spread_matrix(spread.shape, first_head, LANES // 2)
        pick[...] = spread_matrix(pick.shape, first_head, LANES)
        for p in range(n_pairs):
            part = slice(p * LANES, (p + 1) * LANES)
            skip_buf[:, part] = 2.0 * pair_cols(jnp.broadcast_to(skip_ref[...], (8, skip_ref.shape[1])), first_head + 2 * p, low8)
        f_acc[...] = sum(got[s][0:LANES, :].astype(F32) * fwd[s] for s in range(3))
        hb_acc[...] = sum(got[s][0:LANES, :].astype(F32) * bwd[s] for s in range(3))

    row = lax.broadcasted_iota(jnp.int32, (CHUNK, LANES), 0)
    lane = lax.broadcasted_iota(jnp.int32, (CHUNK, LANES), 1)
    low = lane < LANES // 2
    zeros = jnp.zeros((16, 2 * LANES), BF16)
    grams = []
    for c in range(OUT_CHUNKS):
        rows = slice(c * CHUNK, (c + 1) * CHUNK)
        b_val = bc_ref[rows, :LANES]
        gram = lax.dot_general(bc_ref[rows, LANES:], b_val, (((1,), (1,)), ((), ())), preferred_element_type=F32)
        grams.append(jnp.where(row == lane, 2.0 * gram, gram))
        sums = lax.dot_general(b_val, vf_ref[rows, :], (((0,), (0,)), ((), ())), preferred_element_type=F32)
        state = f_acc[...]
        fwd_buf[c] = state.astype(BF16)
        bwd_buf[c] = (gloc_ref[c] + hb_acc[...] * jnp.exp(suf_ref[c, 0:1, :])).astype(BF16)
        f_acc[...] = state * jnp.exp(suf_ref[c, 1:2, :]) + sums

    def weights(c, p):
        rows = slice(c * CHUNK, (c + 1) * CHUNK)
        head = first_head + 2 * p

        def differences(terms_ref, tail_ref):
            tails = jnp.concatenate([tail_ref[16 * h:16 * h + 16, rows] for h in (head, head + 1)], axis=1)
            chosen = pick[0:3 * SLOT, slice(2 * p * LANES, 2 * (p + 1) * LANES)]
            return jnp.dot(terms_ref[rows, :], jnp.concatenate([chosen, tails, zeros], axis=0), preferred_element_type=F32)

        decay = jnp.exp(jnp.minimum(differences(cum_ref, tail1_ref), differences(nexc_ref, tail2_ref)))
        return jnp.concatenate([(decay[:, :LANES] * grams[c]).astype(BF16), (decay[:, LANES:] * grams[c]).astype(BF16)], axis=1)

    def passed(c, p):
        rows = slice(c * CHUNK, (c + 1) * CHUNK)
        part = slice(p * LANES, (p + 1) * LANES)
        c_val = bc_ref[rows, LANES:]
        cum = jnp.dot(cum_ref[rows, :], spread[:, part], preferred_element_type=F32)
        nexc = jnp.dot(nexc_ref[rows, :], spread[:, part], preferred_element_type=F32)
        y_fwd = jnp.dot(c_val, fwd_buf[c, :, part], preferred_element_type=F32)
        y_bwd = jnp.dot(c_val, bwd_buf[c, :, part], preferred_element_type=F32)
        y_val = jnp.exp(cum) * y_fwd + jnp.exp(suf_ref[c, 1:2, part] + nexc) * y_bwd
        return y_val + skip_buf[0:1, part] * u_ref[rows, part].astype(F32)

    order = [(c, 2 * t + h) for t in range(n_pairs // 2) for c in range(OUT_CHUNKS) for h in range(2)]
    ahead = [weights(*order[i]) for i in range(OUT_AHEAD)]
    project_tile(z_ref, x_ref, w_refs[0], 0)
    for i, (c, p) in enumerate(order):
        mix = ahead.pop(0)
        if i + OUT_AHEAD < len(order):
            ahead.append(weights(*order[i + OUT_AHEAD]))
        if c == 0 and p % 2 == 0 and p // 2 + 1 < n_pairs // 2:
            project_tile(z_ref, x_ref, w_refs[p // 2 + 1], p // 2 + 1)
        y_val = passed(c, p)
        rows = slice(c * CHUNK, (c + 1) * CHUNK)
        part = slice(p * LANES, (p + 1) * LANES)
        scaled = ut_ref[rows, part]
        none = jnp.zeros_like(scaled)
        rhs = jnp.concatenate([jnp.where(low, scaled, none), jnp.where(low, none, scaled)], axis=0)
        y_val = jnp.dot(mix, rhs, preferred_element_type=F32) + y_val
        z_val = z_ref[rows, part].astype(F32)
        g_buf[rows, part] = (y_val * (z_val * jax.nn.sigmoid(z_val))).astype(BF16)

    steps = pl.num_programs(0) // 4
    slot = (step // steps) ^ who_ref[0]
    length = OUT_CHUNKS * CHUNK
    for s, o_ref in enumerate((o0_ref, o1_ref, o2_ref, o3_ref)):
        @pl.when(slot == s)
        def _():
            o_ref[pl.ds(pl.multiple_of((step % steps) * length, length), length), :] = g_buf[...]


def params(mib=62):
    return pltpu.CompilerParams(dimension_semantics=("arbitrary",), vmem_limit_bytes=mib << 20)


def cost(flops, moved):
    return pl.CostEstimate(flops=int(flops), bytes_accessed=int(moved), transcendentals=0)


ANY = pl.BlockSpec(memory_space=pl.ANY)
SMEM = pl.BlockSpec(memory_space=pltpu.SMEM)


def w_specs(w, first_tile, n_tiles):
    return [pl.BlockSpec((w.shape[0], 256), functools.partial(lambda t, i: (0, t), first_tile + t), pipeline_mode=pl.Buffered(1)) for t in range(n_tiles)]


def state_parts(tokens, width, tok, at):
    n_chunks = tokens // CHUNK
    whole = pl.BlockSpec((LANES + 16, width), lambda i: (0, 0))
    specs = [tok(width), pl.BlockSpec((STATE_CHUNKS, LANES, width), lambda i: (at(i), 0, 0)), pl.BlockSpec((STATE_CHUNKS, 8, width), lambda i: (at(i), 0, 0)), whole, whole, whole, tok(width), tok(width)]
    shapes = [jax.ShapeDtypeStruct((tokens, width), BF16), jax.ShapeDtypeStruct((n_chunks, LANES, width), F32), jax.ShapeDtypeStruct((n_chunks, 8, width), F32)] + [jax.ShapeDtypeStruct((LANES + 16, width), BF16)] * 3 + [jax.ShapeDtypeStruct((tokens, width), BF16)] * 2
    scratch = [pltpu.VMEM((LANES, width), F32), pltpu.VMEM((LANES, width), F32), pltpu.VMEM((8, width), F32), pltpu.VMEM((STATE_CHUNKS, CHUNK, 2 * width), BF16), pltpu.VMEM((LANES, width), BF16)]
    return specs, shapes, scratch


def first_group(who, x_blk, w_bc, w_dt_rows, bias, a_neg, w_x, n_tiles):
    tokens, d_model = x_blk.shape
    tile = STATE_CHUNKS * CHUNK
    width = 256 * n_tiles
    at = lambda i: tokens // tile - 1 - i
    whole = lambda a: pl.BlockSpec(a.shape, lambda i: (0, 0), pipeline_mode=pl.Buffered(1))
    tok = lambda w: pl.BlockSpec((tile, w), lambda i: (at(i), 0))
    heads = bias.shape[1]
    tail = pl.BlockSpec((16 * heads, tile), lambda i: (0, at(i)))
    specs, shapes, scratch = state_parts(tokens, width, tok, at)
    return pl.pallas_call(
        functools.partial(first_kernel, n_tiles),
        grid=(tokens // tile,),
        in_specs=[SMEM, tok(d_model), whole(w_bc), whole(w_dt_rows), whole(bias), whole(a_neg)] + w_specs(w_x, 0, n_tiles),
        out_specs=[tok(2 * LANES), tok(LANES), tok(LANES), tok(LANES), tail, tail] + specs,
        out_shape=[jax.ShapeDtypeStruct((tokens, 2 * LANES), BF16)] + [jax.ShapeDtypeStruct((tokens, LANES), BF16)] * 3 + [jax.ShapeDtypeStruct((16 * heads, tokens), BF16)] * 2 + shapes,
        scratch_shapes=[pltpu.VMEM((LANES, d_model), BF16), pltpu.VMEM((8, LANES), F32), pltpu.VMEM((16 * heads, LANES), BF16)] + scratch,
        compiler_params=params(),
        cost_estimate=cost(2 * tokens * d_model * (1024 + width), 2 * tokens * d_model),
        name="first_group",
    )(who, x_blk, w_bc, w_dt_rows, bias, a_neg, *([w_x] * n_tiles))


def next_group(who, x_blk, w_x, first_tile, n_tiles, bc, sums, after, first_head):
    tokens, d_model = x_blk.shape
    tile = STATE_CHUNKS * CHUNK
    at = lambda i: tokens // tile - 1 - i
    tok = lambda w: pl.BlockSpec((tile, w), lambda i: (at(i), 0))
    specs, shapes, scratch = state_parts(tokens, 256 * n_tiles, tok, at)
    return pl.pallas_call(
        functools.partial(next_kernel, first_head, n_tiles),
        grid=(tokens // tile,),
        in_specs=[SMEM, tok(d_model), tok(2 * LANES), tok(LANES), tok(LANES), tok(LANES)] + w_specs(w_x, first_tile, n_tiles) + [ANY],
        out_specs=specs,
        out_shape=shapes,
        scratch_shapes=scratch,
        compiler_params=params(),
        cost_estimate=cost(2 * tokens * d_model * (512 + 256 * n_tiles), 2 * tokens * d_model),
        name="next_group",
    )(who, x_blk, bc, *sums, *([w_x] * n_tiles), after)


def add_products(who, acc, pieces, out_dtype):
    rows, d_model = pieces[0][0].shape[0], acc.shape[1]
    tile = min(512, d_model)
    n_tiles = [g.shape[1] // 256 for g, _, _ in pieces]
    mine = acc.shape[0] > rows
    specs, args = [pl.BlockSpec((rows, tile), lambda i, who: (who[0] if mine else 0, i))], [acc]
    for (g, w, tile0), count in zip(pieces, n_tiles):
        specs.append(pl.BlockSpec(g.shape, lambda i, who: (0, 0)))
        specs += [pl.BlockSpec((256, tile), functools.partial(lambda t, i, who: (t, i), tile0 + t)) for t in range(count)]
        args += [g] + [w] * count

    def body(who_ref, *refs):
        sum_kernel(n_tiles, len(pieces), *refs)

    return pl.pallas_call(
        body,
        grid_spec=pltpu.PrefetchScalarGridSpec(num_scalar_prefetch=1, grid=(d_model // tile,), in_specs=specs, out_specs=pl.BlockSpec((rows, tile), lambda i, who: (0, i))),
        out_shape=jax.ShapeDtypeStruct((rows, d_model), out_dtype),
        compiler_params=params(SUM_MIB),
        cost_estimate=cost(2 * rows * d_model * 256 * sum(n_tiles), 2 * rows * d_model),
        name="add_products",
    )(who, *args)


def chunk_outputs(who, u, x_blk, w_z, first_tile, bc, sums, tails, local, got, skip, after, first_head, n_pairs):
    tokens, width = u.shape
    n_steps = tokens // (OUT_CHUNKS * CHUNK)
    gloc, suf, scaled, ends = local
    tail = pl.BlockSpec((tails[0].shape[0], OUT_CHUNKS * CHUNK), lambda i, who: (0, i))
    tok = lambda w: pl.BlockSpec((OUT_CHUNKS * CHUNK, w), lambda i, who: (i, 0))
    state = pl.BlockSpec((LANES + 16, width), lambda i, who: (0, 0))
    small = lambda a: pl.BlockSpec(a.shape, lambda i, who: (0, 0))
    rows_out = tokens // 4
    return pl.pallas_call(
        functools.partial(out_kernel, first_head, n_pairs),
        grid_spec=pltpu.PrefetchScalarGridSpec(
            num_scalar_prefetch=1,
            grid=(n_steps,),
            in_specs=[tok(width), tok(x_blk.shape[1]), tok(width), tok(width)] + [tok(2 * LANES), tok(LANES), tok(LANES), tail, tail, pl.BlockSpec((OUT_CHUNKS, LANES, width), lambda i, who: (i, 0, 0)), pl.BlockSpec((OUT_CHUNKS, 8, width), lambda i, who: (i, 0, 0)), state, state, state] + [small(skip), ANY] + [pl.BlockSpec((w_z.shape[0], 256), functools.partial(lambda t, i, who: (0, t), first_tile + t), pipeline_mode=pl.Buffered(1)) for t in range(n_pairs // 2)],
            out_specs=[pl.BlockSpec((rows_out, width), lambda i, who: (0, 0))] * 4,
            scratch_shapes=[pltpu.VMEM((LANES, width), F32), pltpu.VMEM((LANES, width), F32), pltpu.VMEM((8, width), F32), pltpu.VMEM((OUT_CHUNKS * CHUNK, width), BF16), pltpu.VMEM((LANES, width), BF16), pltpu.VMEM((LANES, 2 * width), BF16)] + [pltpu.VMEM((OUT_CHUNKS, LANES, width), BF16)] * 2 + [pltpu.VMEM((OUT_CHUNKS * CHUNK, width), BF16)],
        ),
        out_shape=[jax.ShapeDtypeStruct((rows_out, width), BF16)] * 4,
        compiler_params=params(),
        cost_estimate=cost(24 * tokens * width * 256, 8 * tokens * width),
        name="outputs",
    )(who, u, x_blk, scaled, ends, bc, sums[0], sums[1], *tails, gloc, suf, *got, skip, after, *([w_z] * (n_pairs // 2)))


def solution(mesh):
    n_sp, n_dp = mesh.shape['sp'], mesh.shape['dp']

    def swap(val, axis, slot):
        return lax.ppermute(val, axis, [(i, i ^ slot) for i in range(4)])

    def later(vals, after):
        return list(lax.optimization_barrier((*vals, after)))[:-1]

    def device_fn(x_blk, w_z, w_x, w_bc, w_dt, a_neg, dt_bias, d_skip, w_out):
        heads = a_neg.shape[0]
        head_dim = w_x.shape[1] // heads
        tp_index = lax.axis_index('tp')
        sp_index = lax.axis_index('sp')

        piece_rows = w_out.shape[0] // (n_dp * n_sp)
        mine = lax.axis_index('dp') * n_sp + sp_index
        piece = lax.dynamic_slice_in_dim(w_out, mine * piece_rows, piece_rows, axis=0)
        one = swap(piece, 'tp', 1)
        two = swap(piece, 'tp', 2)
        plane = lambda v: lax.all_gather(v, ('dp', 'sp'), tiled=True)

        n_tiles = w_x.shape[1] // 256
        first = n_tiles * 2 // 5
        (t_a, n_a), (t_b, n_b) = (0, first), (first, n_tiles - first)
        head_b = first * 256 // head_dim
        who = jnp.stack([tp_index, sp_index])
        skip = d_skip[None, :]

        def exchange(states):
            return [swap(states[s - 1], 'sp', s) for s in (1, 2, 3)]

        def send(pieces):
            return [pieces[0]] + [swap(pieces[s], 'tp', s) for s in (1, 2, 3)]

        bc, cum3, nexc3, dt3, tail1, tail2, u_a, gloc, suf, *states, ut, vf = first_group(who, x_blk, w_bc, w_dt.T, dt_bias[None, :], a_neg[None, :], w_x, n_a)
        local_a = (gloc, suf, ut, vf)
        got_a = exchange(states)
        one, = later((one,), bc)
        w_one = plane(one)
        u_b, gloc, suf, *states, ut, vf = next_group(who, x_blk, w_x, t_b, n_b, bc, (cum3, nexc3, dt3), one, head_b)
        local_b = (gloc, suf, ut, vf)
        got_b = exchange(states)
        g_a = chunk_outputs(who, u_a, x_blk, w_z, t_a, bc, (cum3, nexc3), (tail1, tail2), local_a, got_a, skip, u_b, 0, 2 * n_a)
        got_g_a = send(g_a)
        two, = later((two,), g_a[0])
        three = swap(two, 'tp', 1)
        w_two = plane(two)
        g_b = chunk_outputs(who, u_b, x_blk, w_z, t_b, bc, (cum3, nexc3), (tail1, tail2), local_b, got_b, skip, two, head_b, 2 * n_b)
        got_g_b = send(g_b)
        w_three = plane(three)

        total = add_products(who, x_blk, [(got_g_a[0], w_out, t_a), (got_g_b[0], w_out, t_b), (got_g_a[1], w_one, t_a)], F32)
        total = add_products(who, total, [(got_g_a[2], w_two, t_a), (got_g_b[1], w_one, t_b)], F32)
        total = add_products(who, total, [(got_g_b[2], w_two, t_b), (got_g_a[3], w_three, t_a)], F32)
        return add_products(who, total, [(got_g_b[3], w_three, t_b)], BF16)

    in_specs = (P(('dp', 'sp'), None), P(None, 'tp'), P(None, 'tp'), P(None, None), P(None, 'tp'), P('tp'), P('tp'), P('tp'), P('tp', None))
    out_specs = P(('dp', 'sp', 'tp'), None)
    return jax.shard_map(device_fn, mesh=mesh, in_specs=in_specs, out_specs=out_specs, check_vma=False)
```

```python
import functools

import jax
import jax.numpy as jnp
from jax import lax
from jax.experimental import pallas as pl
from jax.experimental.pallas import tpu as pltpu
from jax.sharding import PartitionSpec as P


CHUNK = 128
LANES = 128
SLOT = 32
STATE_CHUNKS = 4
OUT_CHUNKS = 2
OUT_AHEAD = 2
SUM_MIB = 56
F32 = jnp.float32
BF16 = jnp.bfloat16


def split3(val, lane, last):
    first = val.astype(BF16).astype(F32)
    rest = val - first
    second = rest.astype(BF16).astype(F32)
    third = rest - second
    return jnp.where(lane < SLOT, first, jnp.where(lane < 2 * SLOT, second, jnp.where(lane < 3 * SLOT, third, last))).astype(BF16)


def prep_kernel(n_tiles, x_ref, wbc_ref, wdt_ref, bias_ref, a_ref, *refs):
    bc_ref, cum_ref, nexc_ref, dt_ref, tail1_ref, tail2_ref, u_ref = refs[n_tiles:n_tiles + 7]
    w_buf, par, pick = refs[-8:-5]
    heads = bias_ref.shape[1]
    row = lax.broadcasted_iota(jnp.int32, (CHUNK, LANES), 0)
    lane = lax.broadcasted_iota(jnp.int32, (CHUNK, LANES), 1)

    @pl.when(pl.program_id(0) == 0)
    def _():
        w_buf[...] = jnp.zeros_like(w_buf)
        par[...] = jnp.zeros_like(par)
        for k in range(3):
            w_buf[k * SLOT:k * SLOT + heads, :] = wdt_ref[...]
            par[0:1, k * SLOT:k * SLOT + heads] = bias_ref[...]
            par[1:2, k * SLOT:k * SLOT + heads] = a_ref[...]
        out_row = lax.broadcasted_iota(jnp.int32, pick.shape, 0)
        term = lax.broadcasted_iota(jnp.int32, pick.shape, 1)
        head, which = out_row // 16, out_row % 16
        pick[...] = jnp.where((which < 3) & (term == which * SLOT + head), -1.0, 0.0).astype(BF16)

    x_val = x_ref[...]
    raw = lax.dot_general(x_val, w_buf[...], (((1,), (1,)), ((), ())), preferred_element_type=F32) + par[0:1, :]

    project_tile(u_ref, x_ref, refs[0], 0)
    dt_val = jnp.maximum(raw, 0.0) + jnp.log1p(jnp.exp(-jnp.abs(raw)))
    la_val = jnp.maximum(dt_val * par[1:2, :], -1000.0)
    tri = jnp.where(row >= lane, 1.0, 0.0).astype(BF16)
    parts = [slice(c * CHUNK, (c + 1) * CHUNK) for c in range(x_val.shape[0] // CHUNK)]
    sums = []
    for part in parts:
        la_c = la_val[part, :]
        first = la_c.astype(BF16)
        rest = la_c - first.astype(F32)
        second = rest.astype(BF16)
        third = (rest - second.astype(F32)).astype(BF16)
        sums.append(sum(jnp.dot(tri, t, preferred_element_type=F32) for t in (first, second, third)))
    for t in range(1, n_tiles):
        project_tile(u_ref, x_ref, refs[t], t)
    one = jnp.where(lane < 3 * SLOT + 3, 1.0, 0.0)
    for part, cum in zip(parts, sums):
        cum_ref[part, :] = split3(cum, lane, one)
        nexc_ref[part, :] = split3(la_val[part, :] - cum, lane, one)
        dt_ref[part, :] = split3(dt_val[part, :], lane, 0.0)
    bc_ref[...] = jnp.dot(x_val, wbc_ref[...], preferred_element_type=F32).astype(BF16)
    across = (((1,), (1,)), ((), ()))
    tail1_ref[...] = lax.dot_general(pick[...], cum_ref[...], across, preferred_element_type=F32).astype(BF16)
    tail2_ref[...] = lax.dot_general(pick[...], nexc_ref[...], across, preferred_element_type=F32).astype(BF16)


def first_kernel(n_tiles, who_ref, *refs):
    prep_kernel(n_tiles, *refs)
    bc_ref, cum_ref, nexc_ref, dt_ref, _, _, u_ref = refs[5 + n_tiles:12 + n_tiles]
    state_kernel(0, 2 * n_tiles, lambda t: None, u_ref, bc_ref, cum_ref, nexc_ref, dt_ref, *refs[12 + n_tiles:-8], who_ref, *refs[-5:])


def next_kernel(first_head, n_tiles, who_ref, x_ref, bc_ref, cum_ref, nexc_ref, dt_ref, *refs):
    u_ref = refs[n_tiles + 1]
    project = lambda t: project_tile(u_ref, x_ref, refs[t], t)
    state_kernel(first_head, 2 * n_tiles, project, u_ref, bc_ref, cum_ref, nexc_ref, dt_ref, *refs[n_tiles + 2:-5], who_ref, *refs[-5:])


def project_tile(o_ref, x_ref, w_ref, t):
    o_ref[:, t * 256:(t + 1) * 256] = jnp.dot(x_ref[...], w_ref[...], preferred_element_type=F32).astype(BF16)


def sum_kernel(n_tiles, n_pieces, acc_ref, *refs):
    o_ref = refs[-1]
    total = acc_ref[...].astype(F32)
    for i in range(n_pieces):
        g_ref, w_refs = refs[sum(n_tiles[:i]) + i], refs[sum(n_tiles[:i]) + i + 1:sum(n_tiles[:i + 1]) + i + 1]
        for t in range(n_tiles[i]):
            total = total + jnp.dot(g_ref[:, t * 256:(t + 1) * 256], w_refs[t][...], preferred_element_type=F32)
    o_ref[...] = total.astype(o_ref.dtype)


def spread_matrix(shape, first_head, lanes_per_head):
    term = lax.broadcasted_iota(jnp.int32, shape, 0)
    lane = lax.broadcasted_iota(jnp.int32, shape, 1)
    return jnp.where((term % SLOT == first_head + lane // lanes_per_head) & (term < 3 * SLOT), 1.0, 0.0).astype(BF16)


def pair_cols(cols, head, low):
    return jnp.where(low, jnp.broadcast_to(cols[:, head:head + 1], low.shape), jnp.broadcast_to(cols[:, head + 1:head + 2], low.shape))


def state_kernel(first_head, n_pairs, project, u_ref, bc_ref, cum_ref, nexc_ref, dt_ref, gloc_ref, suf_ref, s1_ref, s2_ref, s3_ref, ut_ref, vf_ref, who_ref, g_acc, f_acc, suf_acc, v_buf, spread):
    step = pl.program_id(0)
    width = n_pairs * LANES

    @pl.when(step == 0)
    def _():
        g_acc[...] = jnp.zeros_like(g_acc)
        f_acc[...] = jnp.zeros_like(f_acc)
        suf_acc[...] = jnp.zeros_like(suf_acc)
        spread[...] = spread_matrix(spread.shape, first_head, LANES // 2)

    def terms_of(c, t):
        rows = slice(c * CHUNK, (c + 1) * CHUNK)
        return [jnp.dot(r[rows, :], spread[:, t * 256:(t + 1) * 256], preferred_element_type=F32) for r in (cum_ref, nexc_ref, dt_ref)]

    project(0)
    order = [(c, t) for t in range(n_pairs // 2) for c in reversed(range(STATE_CHUNKS))]
    ahead = terms_of(*order[0])
    for i, (c, t) in enumerate(order):
        terms = ahead
        if i + 1 < len(order):
            ahead = terms_of(*order[i + 1])
        if c == STATE_CHUNKS - 1 and t + 1 < n_pairs // 2:
            project(t + 1)
        rows = slice(c * CHUNK, (c + 1) * CHUNK)
        wide = slice(t * 256, (t + 1) * 256)
        cum, nexc, dt_val = terms
        scaled = u_ref[rows, wide].astype(F32) * dt_val
        total = cum[CHUNK - 1:CHUNK, :]
        suffix = suf_acc[:, wide]
        ut_ref[rows, wide] = scaled.astype(BF16)
        v_buf[c, :, t * 512:t * 512 + 256] = (scaled * jnp.exp(-nexc)).astype(BF16)
        end = (scaled * jnp.exp(total - cum)).astype(BF16)
        vf_ref[rows, wide] = end
        v_buf[c, :, t * 512 + 256:(t + 1) * 512] = end
        suf_ref[c, 0:1, wide] = suffix[0:1, :]
        suf_ref[c, 1:2, wide] = total
        suf_acc[:, wide] = suffix + total
        sums = lax.dot_general(bc_ref[rows, :LANES], v_buf[c, :, t * 512:(t + 1) * 512], (((0,), (0,)), ((), ())), preferred_element_type=F32)
        back = g_acc[:, wide]
        gloc_ref[c, :, wide] = back
        g_acc[:, wide] = back * jnp.exp(total) + sums[:, :256]
        f_acc[:, wide] += sums[:, 256:] * jnp.exp(suffix[0:1, :])

    @pl.when(step == pl.num_programs(0) - 1)
    def _():
        row = lax.broadcasted_iota(jnp.int32, (16, width), 0)
        log = jnp.broadcast_to(suf_acc[0:1, :], (16, width))
        first = log.astype(BF16).astype(F32)
        second = (log - first).astype(BF16).astype(F32)
        third = log - first - second
        terms = jnp.where(row == 0, first, jnp.where(row == 1, second, jnp.where(row == 2, third, 0.0))).astype(BF16)
        me = who_ref[1]
        for s, s_ref in ((1, s1_ref), (2, s2_ref), (3, s3_ref)):
            s_ref[LANES:LANES + 16, :] = terms
            s_ref[0:LANES, :] = jnp.where(me < (me ^ s), f_acc[...], g_acc[...]).astype(BF16)


def peer_weights(sp_index, logs):
    fwd, bwd = [], []
    for s in (1, 2, 3):
        peer = sp_index ^ s
        between = jnp.zeros_like(logs[0])
        for o in (1, 2, 3):
            other = sp_index ^ o
            inside = (other > jnp.minimum(peer, sp_index)) & (other < jnp.maximum(peer, sp_index))
            between = between + jnp.where(inside, logs[o - 1], 0.0)
        decay = jnp.exp(between)
        fwd.append(jnp.where(peer < sp_index, decay, 0.0))
        bwd.append(jnp.where(peer > sp_index, decay, 0.0))
    return fwd, bwd


def out_kernel(first_head, n_pairs, who_ref, u_ref, x_ref, ut_ref, vf_ref, bc_ref, cum_ref, nexc_ref, tail1_ref, tail2_ref, gloc_ref, suf_ref, r1_ref, r2_ref, r3_ref, skip_ref, after_ref, *refs):
    w_refs, (o0_ref, o1_ref, o2_ref, o3_ref, f_acc, hb_acc, skip_buf, g_buf, spread, pick, fwd_buf, bwd_buf, z_ref) = refs[:n_pairs // 2], refs[n_pairs // 2:]
    step = pl.program_id(0)

    @pl.when(step == 0)
    def _():
        low8 = lax.broadcasted_iota(jnp.int32, (8, LANES), 1) < LANES // 2
        got = (r1_ref, r2_ref, r3_ref)
        logs = [r[LANES:LANES + 16, :].astype(F32) for r in got]
        fwd, bwd = peer_weights(who_ref[1], [v[0:1, :] + v[1:2, :] + v[2:3, :] for v in logs])
        spread[...] = spread_matrix(spread.shape, first_head, LANES // 2)
        pick[...] = spread_matrix(pick.shape, first_head, LANES)
        for p in range(n_pairs):
            part = slice(p * LANES, (p + 1) * LANES)
            skip_buf[:, part] = 2.0 * pair_cols(jnp.broadcast_to(skip_ref[...], (8, skip_ref.shape[1])), first_head + 2 * p, low8)
        f_acc[...] = sum(got[s][0:LANES, :].astype(F32) * fwd[s] for s in range(3))
        hb_acc[...] = sum(got[s][0:LANES, :].astype(F32) * bwd[s] for s in range(3))

    row = lax.broadcasted_iota(jnp.int32, (CHUNK, LANES), 0)
    lane = lax.broadcasted_iota(jnp.int32, (CHUNK, LANES), 1)
    low = lane < LANES // 2
    zeros = jnp.zeros((16, 2 * LANES), BF16)
    grams = []
    for c in range(OUT_CHUNKS):
        rows = slice(c * CHUNK, (c + 1) * CHUNK)
        b_val = bc_ref[rows, :LANES]
        gram = lax.dot_general(bc_ref[rows, LANES:], b_val, (((1,), (1,)), ((), ())), preferred_element_type=F32)
        grams.append(jnp.where(row == lane, 2.0 * gram, gram))
        sums = lax.dot_general(b_val, vf_ref[rows, :], (((0,), (0,)), ((), ())), preferred_element_type=F32)
        state = f_acc[...]
        fwd_buf[c] = state.astype(BF16)
        bwd_buf[c] = (gloc_ref[c] + hb_acc[...] * jnp.exp(suf_ref[c, 0:1, :])).astype(BF16)
        f_acc[...] = state * jnp.exp(suf_ref[c, 1:2, :]) + sums

    def weights(c, p):
        rows = slice(c * CHUNK, (c + 1) * CHUNK)
        head = first_head + 2 * p

        def differences(terms_ref, tail_ref):
            tails = jnp.concatenate([tail_ref[16 * h:16 * h + 16, rows] for h in (head, head + 1)], axis=1)
            chosen = pick[0:3 * SLOT, slice(2 * p * LANES, 2 * (p + 1) * LANES)]
            return jnp.dot(terms_ref[rows, :], jnp.concatenate([chosen, tails, zeros], axis=0), preferred_element_type=F32)

        decay = jnp.exp(jnp.minimum(differences(cum_ref, tail1_ref), differences(nexc_ref, tail2_ref)))
        return jnp.concatenate([(decay[:, :LANES] * grams[c]).astype(BF16), (decay[:, LANES:] * grams[c]).astype(BF16)], axis=1)

    def passed(c, p):
        rows = slice(c * CHUNK, (c + 1) * CHUNK)
        part = slice(p * LANES, (p + 1) * LANES)
        c_val = bc_ref[rows, LANES:]
        cum = jnp.dot(cum_ref[rows, :], spread[:, part], preferred_element_type=F32)
        nexc = jnp.dot(nexc_ref[rows, :], spread[:, part], preferred_element_type=F32)
        y_fwd = jnp.dot(c_val, fwd_buf[c, :, part], preferred_element_type=F32)
        y_bwd = jnp.dot(c_val, bwd_buf[c, :, part], preferred_element_type=F32)
        y_val = jnp.exp(cum) * y_fwd + jnp.exp(suf_ref[c, 1:2, part] + nexc) * y_bwd
        return y_val + skip_buf[0:1, part] * u_ref[rows, part].astype(F32)

    order = [(c, 2 * t + h) for t in range(n_pairs // 2) for c in range(OUT_CHUNKS) for h in range(2)]
    ahead = [weights(*order[i]) for i in range(OUT_AHEAD)]
    project_tile(z_ref, x_ref, w_refs[0], 0)
    for i, (c, p) in enumerate(order):
        mix = ahead.pop(0)
        if i + OUT_AHEAD < len(order):
            ahead.append(weights(*order[i + OUT_AHEAD]))
        if c == 0 and p % 2 == 0 and p // 2 + 1 < n_pairs // 2:
            project_tile(z_ref, x_ref, w_refs[p // 2 + 1], p // 2 + 1)
        y_val = passed(c, p)
        rows = slice(c * CHUNK, (c + 1) * CHUNK)
        part = slice(p * LANES, (p + 1) * LANES)
        scaled = ut_ref[rows, part]
        none = jnp.zeros_like(scaled)
        rhs = jnp.concatenate([jnp.where(low, scaled, none), jnp.where(low, none, scaled)], axis=0)
        y_val = jnp.dot(mix, rhs, preferred_element_type=F32) + y_val
        z_val = z_ref[rows, part].astype(F32)
        g_buf[rows, part] = (y_val * (z_val * jax.nn.sigmoid(z_val))).astype(BF16)

    steps = pl.num_programs(0) // 4
    slot = (step // steps) ^ who_ref[0]
    length = OUT_CHUNKS * CHUNK
    for s, o_ref in enumerate((o0_ref, o1_ref, o2_ref, o3_ref)):
        @pl.when(slot == s)
        def _():
            o_ref[pl.ds(pl.multiple_of((step % steps) * length, length), length), :] = g_buf[...]


def params(mib=62):
    return pltpu.CompilerParams(dimension_semantics=("arbitrary",), vmem_limit_bytes=mib << 20)


def cost(flops, moved):
    return pl.CostEstimate(flops=int(flops), bytes_accessed=int(moved), transcendentals=0)


ANY = pl.BlockSpec(memory_space=pl.ANY)
SMEM = pl.BlockSpec(memory_space=pltpu.SMEM)


def w_specs(w, first_tile, n_tiles):
    return [pl.BlockSpec((w.shape[0], 256), functools.partial(lambda t, i: (0, t), first_tile + t), pipeline_mode=pl.Buffered(1)) for t in range(n_tiles)]


def state_parts(tokens, width, tok, at):
    n_chunks = tokens // CHUNK
    whole = pl.BlockSpec((LANES + 16, width), lambda i: (0, 0))
    specs = [tok(width), pl.BlockSpec((STATE_CHUNKS, LANES, width), lambda i: (at(i), 0, 0)), pl.BlockSpec((STATE_CHUNKS, 8, width), lambda i: (at(i), 0, 0)), whole, whole, whole, tok(width), tok(width)]
    shapes = [jax.ShapeDtypeStruct((tokens, width), BF16), jax.ShapeDtypeStruct((n_chunks, LANES, width), F32), jax.ShapeDtypeStruct((n_chunks, 8, width), F32)] + [jax.ShapeDtypeStruct((LANES + 16, width), BF16)] * 3 + [jax.ShapeDtypeStruct((tokens, width), BF16)] * 2
    scratch = [pltpu.VMEM((LANES, width), F32), pltpu.VMEM((LANES, width), F32), pltpu.VMEM((8, width), F32), pltpu.VMEM((STATE_CHUNKS, CHUNK, 2 * width), BF16), pltpu.VMEM((LANES, width), BF16)]
    return specs, shapes, scratch


def first_group(who, x_blk, w_bc, w_dt_rows, bias, a_neg, w_x, n_tiles):
    tokens, d_model = x_blk.shape
    tile = STATE_CHUNKS * CHUNK
    width = 256 * n_tiles
    at = lambda i: tokens // tile - 1 - i
    whole = lambda a: pl.BlockSpec(a.shape, lambda i: (0, 0), pipeline_mode=pl.Buffered(1))
    tok = lambda w: pl.BlockSpec((tile, w), lambda i: (at(i), 0))
    heads = bias.shape[1]
    tail = pl.BlockSpec((16 * heads, tile), lambda i: (0, at(i)))
    specs, shapes, scratch = state_parts(tokens, width, tok, at)
    return pl.pallas_call(
        functools.partial(first_kernel, n_tiles),
        grid=(tokens // tile,),
        in_specs=[SMEM, tok(d_model), whole(w_bc), whole(w_dt_rows), whole(bias), whole(a_neg)] + w_specs(w_x, 0, n_tiles),
        out_specs=[tok(2 * LANES), tok(LANES), tok(LANES), tok(LANES), tail, tail] + specs,
        out_shape=[jax.ShapeDtypeStruct((tokens, 2 * LANES), BF16)] + [jax.ShapeDtypeStruct((tokens, LANES), BF16)] * 3 + [jax.ShapeDtypeStruct((16 * heads, tokens), BF16)] * 2 + shapes,
        scratch_shapes=[pltpu.VMEM((LANES, d_model), BF16), pltpu.VMEM((8, LANES), F32), pltpu.VMEM((16 * heads, LANES), BF16)] + scratch,
        compiler_params=params(),
        cost_estimate=cost(2 * tokens * d_model * (1024 + width), 2 * tokens * d_model),
        name="first_group",
    )(who, x_blk, w_bc, w_dt_rows, bias, a_neg, *([w_x] * n_tiles))


def next_group(who, x_blk, w_x, first_tile, n_tiles, bc, sums, after, first_head):
    tokens, d_model = x_blk.shape
    tile = STATE_CHUNKS * CHUNK
    at = lambda i: tokens // tile - 1 - i
    tok = lambda w: pl.BlockSpec((tile, w), lambda i: (at(i), 0))
    specs, shapes, scratch = state_parts(tokens, 256 * n_tiles, tok, at)
    return pl.pallas_call(
        functools.partial(next_kernel, first_head, n_tiles),
        grid=(tokens // tile,),
        in_specs=[SMEM, tok(d_model), tok(2 * LANES), tok(LANES), tok(LANES), tok(LANES)] + w_specs(w_x, first_tile, n_tiles) + [ANY],
        out_specs=specs,
        out_shape=shapes,
        scratch_shapes=scratch,
        compiler_params=params(),
        cost_estimate=cost(2 * tokens * d_model * (512 + 256 * n_tiles), 2 * tokens * d_model),
        name="next_group",
    )(who, x_blk, bc, *sums, *([w_x] * n_tiles), after)


def add_products(who, acc, pieces, out_dtype):
    rows, d_model = pieces[0][0].shape[0], acc.shape[1]
    tile = min(512, d_model)
    n_tiles = [g.shape[1] // 256 for g, _, _ in pieces]
    mine = acc.shape[0] > rows
    specs, args = [pl.BlockSpec((rows, tile), lambda i, who: (who[0] if mine else 0, i))], [acc]
    for (g, w, tile0), count in zip(pieces, n_tiles):
        specs.append(pl.BlockSpec(g.shape, lambda i, who: (0, 0)))
        specs += [pl.BlockSpec((256, tile), functools.partial(lambda t, i, who: (t, i), tile0 + t)) for t in range(count)]
        args += [g] + [w] * count

    def body(who_ref, *refs):
        sum_kernel(n_tiles, len(pieces), *refs)

    return pl.pallas_call(
        body,
        grid_spec=pltpu.PrefetchScalarGridSpec(num_scalar_prefetch=1, grid=(d_model // tile,), in_specs=specs, out_specs=pl.BlockSpec((rows, tile), lambda i, who: (0, i))),
        out_shape=jax.ShapeDtypeStruct((rows, d_model), out_dtype),
        compiler_params=params(SUM_MIB),
        cost_estimate=cost(2 * rows * d_model * 256 * sum(n_tiles), 2 * rows * d_model),
        name="add_products",
    )(who, *args)


def chunk_outputs(who, u, x_blk, w_z, first_tile, bc, sums, tails, local, got, skip, after, first_head, n_pairs):
    tokens, width = u.shape
    n_steps = tokens // (OUT_CHUNKS * CHUNK)
    gloc, suf, scaled, ends = local
    tail = pl.BlockSpec((tails[0].shape[0], OUT_CHUNKS * CHUNK), lambda i, who: (0, i))
    tok = lambda w: pl.BlockSpec((OUT_CHUNKS * CHUNK, w), lambda i, who: (i, 0))
    state = pl.BlockSpec((LANES + 16, width), lambda i, who: (0, 0))
    small = lambda a: pl.BlockSpec(a.shape, lambda i, who: (0, 0))
    rows_out = tokens // 4
    return pl.pallas_call(
        functools.partial(out_kernel, first_head, n_pairs),
        grid_spec=pltpu.PrefetchScalarGridSpec(
            num_scalar_prefetch=1,
            grid=(n_steps,),
            in_specs=[tok(width), tok(x_blk.shape[1]), tok(width), tok(width)] + [tok(2 * LANES), tok(LANES), tok(LANES), tail, tail, pl.BlockSpec((OUT_CHUNKS, LANES, width), lambda i, who: (i, 0, 0)), pl.BlockSpec((OUT_CHUNKS, 8, width), lambda i, who: (i, 0, 0)), state, state, state] + [small(skip), ANY] + [pl.BlockSpec((w_z.shape[0], 256), functools.partial(lambda t, i, who: (0, t), first_tile + t), pipeline_mode=pl.Buffered(1)) for t in range(n_pairs // 2)],
            out_specs=[pl.BlockSpec((rows_out, width), lambda i, who: (0, 0))] * 4,
            scratch_shapes=[pltpu.VMEM((LANES, width), F32), pltpu.VMEM((LANES, width), F32), pltpu.VMEM((8, width), F32), pltpu.VMEM((OUT_CHUNKS * CHUNK, width), BF16), pltpu.VMEM((LANES, width), BF16), pltpu.VMEM((LANES, 2 * width), BF16)] + [pltpu.VMEM((OUT_CHUNKS, LANES, width), BF16)] * 2 + [pltpu.VMEM((OUT_CHUNKS * CHUNK, width), BF16)],
        ),
        out_shape=[jax.ShapeDtypeStruct((rows_out, width), BF16)] * 4,
        compiler_params=params(),
        cost_estimate=cost(24 * tokens * width * 256, 8 * tokens * width),
        name="outputs",
    )(who, u, x_blk, scaled, ends, bc, sums[0], sums[1], *tails, gloc, suf, *got, skip, after, *([w_z] * (n_pairs // 2)))


def solution(mesh):
    n_sp, n_dp = mesh.shape['sp'], mesh.shape['dp']

    def swap(val, axis, slot):
        return lax.ppermute(val, axis, [(i, i ^ slot) for i in range(4)])

    def later(vals, after):
        return list(lax.optimization_barrier((*vals, after)))[:-1]

    def device_fn(x_blk, w_z, w_x, w_bc, w_dt, a_neg, dt_bias, d_skip, w_out):
        heads = a_neg.shape[0]
        head_dim = w_x.shape[1] // heads
        tp_index = lax.axis_index('tp')
        sp_index = lax.axis_index('sp')

        piece_rows = w_out.shape[0] // (n_dp * n_sp)
        mine = lax.axis_index('dp') * n_sp + sp_index
        piece = lax.dynamic_slice_in_dim(w_out, mine * piece_rows, piece_rows, axis=0)
        one = swap(piece, 'tp', 1)
        two = swap(piece, 'tp', 2)
        plane = lambda v: lax.all_gather(v, ('dp', 'sp'), tiled=True)

        n_tiles = w_x.shape[1] // 256
        first = n_tiles * 2 // 5
        (t_a, n_a), (t_b, n_b) = (0, first), (first, n_tiles - first)
        head_b = first * 256 // head_dim
        who = jnp.stack([tp_index, sp_index])
        skip = d_skip[None, :]

        def exchange(states):
            return [swap(states[s - 1], 'sp', s) for s in (1, 2, 3)]

        def send(pieces):
            return [pieces[0]] + [swap(pieces[s], 'tp', s) for s in (1, 2, 3)]

        bc, cum3, nexc3, dt3, tail1, tail2, u_a, gloc, suf, *states, ut, vf = first_group(who, x_blk, w_bc, w_dt.T, dt_bias[None, :], a_neg[None, :], w_x, n_a)
        local_a = (gloc, suf, ut, vf)
        got_a = exchange(states)
        one, = later((one,), bc)
        w_one = plane(one)
        u_b, gloc, suf, *states, ut, vf = next_group(who, x_blk, w_x, t_b, n_b, bc, (cum3, nexc3, dt3), one, head_b)
        local_b = (gloc, suf, ut, vf)
        got_b = exchange(states)
        g_a = chunk_outputs(who, u_a, x_blk, w_z, t_a, bc, (cum3, nexc3), (tail1, tail2), local_a, got_a, skip, u_b, 0, 2 * n_a)
        got_g_a = send(g_a)
        two, = later((two,), g_a[0])
        three = swap(two, 'tp', 1)
        w_two = plane(two)
        g_b = chunk_outputs(who, u_b, x_blk, w_z, t_b, bc, (cum3, nexc3), (tail1, tail2), local_b, got_b, skip, two, head_b, 2 * n_b)
        got_g_b = send(g_b)
        w_three = plane(three)

        total = add_products(who, x_blk, [(got_g_a[0], w_out, t_a), (got_g_b[0], w_out, t_b), (got_g_a[1], w_one, t_a)], F32)
        total = add_products(who, total, [(got_g_a[2], w_two, t_a), (got_g_b[1], w_one, t_b)], F32)
        total = add_products(who, total, [(got_g_b[2], w_two, t_b)], F32)
        return add_products(who, total, [(got_g_a[3], w_three, t_a), (got_g_b[3], w_three, t_b)], BF16)

    in_specs = (P(('dp', 'sp'), None), P(None, 'tp'), P(None, 'tp'), P(None, None), P(None, 'tp'), P('tp'), P('tp'), P('tp'), P('tp', None))
    out_specs = P(('dp', 'sp', 'tp'), None)
    return jax.shard_map(device_fn, mesh=mesh, in_specs=in_specs, out_specs=out_specs, check_vma=False)
```

```python
import functools

import jax
import jax.numpy as jnp
from jax import lax
from jax.experimental import pallas as pl
from jax.experimental.pallas import tpu as pltpu
from jax.sharding import PartitionSpec as P


CHUNK = 128
LANES = 128
SLOT = 32
STATE_CHUNKS = 4
OUT_CHUNKS = 2
OUT_AHEAD = 2
SUM_MIB = 56
F32 = jnp.float32
BF16 = jnp.bfloat16


def split3(val, lane, last):
    first = val.astype(BF16).astype(F32)
    rest = val - first
    second = rest.astype(BF16).astype(F32)
    third = rest - second
    return jnp.where(lane < SLOT, first, jnp.where(lane < 2 * SLOT, second, jnp.where(lane < 3 * SLOT, third, last))).astype(BF16)


def prep_kernel(n_tiles, x_ref, wbc_ref, wdt_ref, bias_ref, a_ref, *refs):
    bc_ref, cum_ref, nexc_ref, dt_ref, tail1_ref, tail2_ref, u_ref = refs[n_tiles:n_tiles + 7]
    w_buf, par, pick = refs[-8:-5]
    heads = bias_ref.shape[1]
    row = lax.broadcasted_iota(jnp.int32, (CHUNK, LANES), 0)
    lane = lax.broadcasted_iota(jnp.int32, (CHUNK, LANES), 1)

    @pl.when(pl.program_id(0) == 0)
    def _():
        w_buf[...] = jnp.zeros_like(w_buf)
        par[...] = jnp.zeros_like(par)
        for k in range(3):
            w_buf[k * SLOT:k * SLOT + heads, :] = wdt_ref[...]
            par[0:1, k * SLOT:k * SLOT + heads] = bias_ref[...]
            par[1:2, k * SLOT:k * SLOT + heads] = a_ref[...]
        out_row = lax.broadcasted_iota(jnp.int32, pick.shape, 0)
        term = lax.broadcasted_iota(jnp.int32, pick.shape, 1)
        head, which = out_row // 16, out_row % 16
        pick[...] = jnp.where((which < 3) & (term == which * SLOT + head), -1.0, 0.0).astype(BF16)

    x_val = x_ref[...]
    raw = lax.dot_general(x_val, w_buf[...], (((1,), (1,)), ((), ())), preferred_element_type=F32) + par[0:1, :]

    project_tile(u_ref, x_ref, refs[0], 0)
    dt_val = jnp.maximum(raw, 0.0) + jnp.log1p(jnp.exp(-jnp.abs(raw)))
    la_val = jnp.maximum(dt_val * par[1:2, :], -1000.0)
    tri = jnp.where(row >= lane, 1.0, 0.0).astype(BF16)
    parts = [slice(c * CHUNK, (c + 1) * CHUNK) for c in range(x_val.shape[0] // CHUNK)]
    sums = []
    for part in parts:
        la_c = la_val[part, :]
        first = la_c.astype(BF16)
        rest = la_c - first.astype(F32)
        second = rest.astype(BF16)
        third = (rest - second.astype(F32)).astype(BF16)
        sums.append(sum(jnp.dot(tri, t, preferred_element_type=F32) for t in (first, second, third)))
    for t in range(1, n_tiles):
        project_tile(u_ref, x_ref, refs[t], t)
    one = jnp.where(lane < 3 * SLOT + 3, 1.0, 0.0)
    for part, cum in zip(parts, sums):
        cum_ref[part, :] = split3(cum, lane, one)
        nexc_ref[part, :] = split3(la_val[part, :] - cum, lane, one)
        dt_ref[part, :] = split3(dt_val[part, :], lane, 0.0)
    bc_ref[...] = jnp.dot(x_val, wbc_ref[...], preferred_element_type=F32).astype(BF16)
    across = (((1,), (1,)), ((), ()))
    tail1_ref[...] = lax.dot_general(pick[...], cum_ref[...], across, preferred_element_type=F32).astype(BF16)
    tail2_ref[...] = lax.dot_general(pick[...], nexc_ref[...], across, preferred_element_type=F32).astype(BF16)


def first_kernel(n_tiles, who_ref, *refs):
    prep_kernel(n_tiles, *refs)
    bc_ref, cum_ref, nexc_ref, dt_ref, _, _, u_ref = refs[5 + n_tiles:12 + n_tiles]
    state_kernel(0, 2 * n_tiles, lambda t: None, u_ref, bc_ref, cum_ref, nexc_ref, dt_ref, *refs[12 + n_tiles:-8], who_ref, *refs[-5:])


def next_kernel(first_head, n_tiles, who_ref, x_ref, bc_ref, cum_ref, nexc_ref, dt_ref, *refs):
    u_ref = refs[n_tiles + 1]
    project = lambda t: project_tile(u_ref, x_ref, refs[t], t)
    state_kernel(first_head, 2 * n_tiles, project, u_ref, bc_ref, cum_ref, nexc_ref, dt_ref, *refs[n_tiles + 2:-5], who_ref, *refs[-5:])


def project_tile(o_ref, x_ref, w_ref, t):
    o_ref[:, t * 256:(t + 1) * 256] = jnp.dot(x_ref[...], w_ref[...], preferred_element_type=F32).astype(BF16)


def sum_kernel(n_tiles, n_pieces, acc_ref, *refs):
    o_ref = refs[-1]
    total = acc_ref[...].astype(F32)
    for i in range(n_pieces):
        g_ref, w_refs = refs[sum(n_tiles[:i]) + i], refs[sum(n_tiles[:i]) + i + 1:sum(n_tiles[:i + 1]) + i + 1]
        for t in range(n_tiles[i]):
            total = total + jnp.dot(g_ref[:, t * 256:(t + 1) * 256], w_refs[t][...], preferred_element_type=F32)
    o_ref[...] = total.astype(o_ref.dtype)


def spread_matrix(shape, first_head, lanes_per_head):
    term = lax.broadcasted_iota(jnp.int32, shape, 0)
    lane = lax.broadcasted_iota(jnp.int32, shape, 1)
    return jnp.where((term % SLOT == first_head + lane // lanes_per_head) & (term < 3 * SLOT), 1.0, 0.0).astype(BF16)


def pair_cols(cols, head, low):
    return jnp.where(low, jnp.broadcast_to(cols[:, head:head + 1], low.shape), jnp.broadcast_to(cols[:, head + 1:head + 2], low.shape))


def state_kernel(first_head, n_pairs, project, u_ref, bc_ref, cum_ref, nexc_ref, dt_ref, gloc_ref, suf_ref, s1_ref, s2_ref, s3_ref, ut_ref, vf_ref, who_ref, g_acc, f_acc, suf_acc, v_buf, spread):
    step = pl.program_id(0)
    width = n_pairs * LANES

    @pl.when(step == 0)
    def _():
        g_acc[...] = jnp.zeros_like(g_acc)
        f_acc[...] = jnp.zeros_like(f_acc)
        suf_acc[...] = jnp.zeros_like(suf_acc)
        spread[...] = spread_matrix(spread.shape, first_head, LANES // 2)

    def terms_of(c, t):
        rows = slice(c * CHUNK, (c + 1) * CHUNK)
        return [jnp.dot(r[rows, :], spread[:, t * 256:(t + 1) * 256], preferred_element_type=F32) for r in (cum_ref, nexc_ref, dt_ref)]

    project(0)
    order = [(c, t) for t in range(n_pairs // 2) for c in reversed(range(STATE_CHUNKS))]
    ahead = terms_of(*order[0])
    for i, (c, t) in enumerate(order):
        terms = ahead
        if i + 1 < len(order):
            ahead = terms_of(*order[i + 1])
        if c == STATE_CHUNKS - 1 and t + 1 < n_pairs // 2:
            project(t + 1)
        rows = slice(c * CHUNK, (c + 1) * CHUNK)
        wide = slice(t * 256, (t + 1) * 256)
        cum, nexc, dt_val = terms
        scaled = u_ref[rows, wide].astype(F32) * dt_val
        total = cum[CHUNK - 1:CHUNK, :]
        suffix = suf_acc[:, wide]
        ut_ref[rows, wide] = scaled.astype(BF16)
        v_buf[c, :, t * 512:t * 512 + 256] = (scaled * jnp.exp(-nexc)).astype(BF16)
        end = (scaled * jnp.exp(total - cum)).astype(BF16)
        vf_ref[rows, wide] = end
        v_buf[c, :, t * 512 + 256:(t + 1) * 512] = end
        suf_ref[c, 0:1, wide] = suffix[0:1, :]
        suf_ref[c, 1:2, wide] = total
        suf_acc[:, wide] = suffix + total
        sums = lax.dot_general(bc_ref[rows, :LANES], v_buf[c, :, t * 512:(t + 1) * 512], (((0,), (0,)), ((), ())), preferred_element_type=F32)
        back = g_acc[:, wide]
        gloc_ref[c, :, wide] = back
        g_acc[:, wide] = back * jnp.exp(total) + sums[:, :256]
        f_acc[:, wide] += sums[:, 256:] * jnp.exp(suffix[0:1, :])

    @pl.when(step == pl.num_programs(0) - 1)
    def _():
        row = lax.broadcasted_iota(jnp.int32, (16, width), 0)
        log = jnp.broadcast_to(suf_acc[0:1, :], (16, width))
        first = log.astype(BF16).astype(F32)
        second = (log - first).astype(BF16).astype(F32)
        third = log - first - second
        terms = jnp.where(row == 0, first, jnp.where(row == 1, second, jnp.where(row == 2, third, 0.0))).astype(BF16)
        me = who_ref[1]
        for s, s_ref in ((1, s1_ref), (2, s2_ref), (3, s3_ref)):
            s_ref[LANES:LANES + 16, :] = terms
            s_ref[0:LANES, :] = jnp.where(me < (me ^ s), f_acc[...], g_acc[...]).astype(BF16)


def peer_weights(sp_index, logs):
    fwd, bwd = [], []
    for s in (1, 2, 3):
        peer = sp_index ^ s
        between = jnp.zeros_like(logs[0])
        for o in (1, 2, 3):
            other = sp_index ^ o
            inside = (other > jnp.minimum(peer, sp_index)) & (other < jnp.maximum(peer, sp_index))
            between = between + jnp.where(inside, logs[o - 1], 0.0)
        decay = jnp.exp(between)
        fwd.append(jnp.where(peer < sp_index, decay, 0.0))
        bwd.append(jnp.where(peer > sp_index, decay, 0.0))
    return fwd, bwd


def out_kernel(first_head, n_pairs, who_ref, u_ref, x_ref, ut_ref, vf_ref, bc_ref, cum_ref, nexc_ref, tail1_ref, tail2_ref, gloc_ref, suf_ref, r1_ref, r2_ref, r3_ref, skip_ref, after_ref, *refs):
    w_refs, (o0_ref, o1_ref, o2_ref, o3_ref, f_acc, hb_acc, skip_buf, g_buf, spread, pick, fwd_buf, bwd_buf, z_ref) = refs[:n_pairs // 2], refs[n_pairs // 2:]
    step = pl.program_id(0)

    @pl.when(step == 0)
    def _():
        low8 = lax.broadcasted_iota(jnp.int32, (8, LANES), 1) < LANES // 2
        got = (r1_ref, r2_ref, r3_ref)
        logs = [r[LANES:LANES + 16, :].astype(F32) for r in got]
        fwd, bwd = peer_weights(who_ref[1], [v[0:1, :] + v[1:2, :] + v[2:3, :] for v in logs])
        spread[...] = spread_matrix(spread.shape, first_head, LANES // 2)
        pick[...] = spread_matrix(pick.shape, first_head, LANES)
        for p in range(n_pairs):
            part = slice(p * LANES, (p + 1) * LANES)
            skip_buf[:, part] = 2.0 * pair_cols(jnp.broadcast_to(skip_ref[...], (8, skip_ref.shape[1])), first_head + 2 * p, low8)
        f_acc[...] = sum(got[s][0:LANES, :].astype(F32) * fwd[s] for s in range(3))
        hb_acc[...] = sum(got[s][0:LANES, :].astype(F32) * bwd[s] for s in range(3))

    row = lax.broadcasted_iota(jnp.int32, (CHUNK, LANES), 0)
    lane = lax.broadcasted_iota(jnp.int32, (CHUNK, LANES), 1)
    low = lane < LANES // 2
    zeros = jnp.zeros((16, 2 * LANES), BF16)
    grams = []
    for c in range(OUT_CHUNKS):
        rows = slice(c * CHUNK, (c + 1) * CHUNK)
        b_val = bc_ref[rows, :LANES]
        gram = lax.dot_general(bc_ref[rows, LANES:], b_val, (((1,), (1,)), ((), ())), preferred_element_type=F32)
        grams.append(jnp.where(row == lane, 2.0 * gram, gram))
        sums = lax.dot_general(b_val, vf_ref[rows, :], (((0,), (0,)), ((), ())), preferred_element_type=F32)
        state = f_acc[...]
        fwd_buf[c] = state.astype(BF16)
        bwd_buf[c] = (gloc_ref[c] + hb_acc[...] * jnp.exp(suf_ref[c, 0:1, :])).astype(BF16)
        f_acc[...] = state * jnp.exp(suf_ref[c, 1:2, :]) + sums

    def weights(c, p):
        rows = slice(c * CHUNK, (c + 1) * CHUNK)
        head = first_head + 2 * p

        def differences(terms_ref, tail_ref):
            tails = jnp.concatenate([tail_ref[16 * h:16 * h + 16, rows] for h in (head, head + 1)], axis=1)
            chosen = pick[0:3 * SLOT, slice(2 * p * LANES, 2 * (p + 1) * LANES)]
            return jnp.dot(terms_ref[rows, :], jnp.concatenate([chosen, tails, zeros], axis=0), preferred_element_type=F32)

        decay = jnp.exp(jnp.minimum(differences(cum_ref, tail1_ref), differences(nexc_ref, tail2_ref)))
        return jnp.concatenate([(decay[:, :LANES] * grams[c]).astype(BF16), (decay[:, LANES:] * grams[c]).astype(BF16)], axis=1)

    def passed(c, p):
        rows = slice(c * CHUNK, (c + 1) * CHUNK)
        part = slice(p * LANES, (p + 1) * LANES)
        c_val = bc_ref[rows, LANES:]
        cum = jnp.dot(cum_ref[rows, :], spread[:, part], preferred_element_type=F32)
        nexc = jnp.dot(nexc_ref[rows, :], spread[:, part], preferred_element_type=F32)
        y_fwd = jnp.dot(c_val, fwd_buf[c, :, part], preferred_element_type=F32)
        y_bwd = jnp.dot(c_val, bwd_buf[c, :, part], preferred_element_type=F32)
        y_val = jnp.exp(cum) * y_fwd + jnp.exp(suf_ref[c, 1:2, part] + nexc) * y_bwd
        return y_val + skip_buf[0:1, part] * u_ref[rows, part].astype(F32)

    order = [(c, 2 * t + h) for t in range(n_pairs // 2) for c in range(OUT_CHUNKS) for h in range(2)]
    ahead = [weights(*order[i]) for i in range(OUT_AHEAD)]
    project_tile(z_ref, x_ref, w_refs[0], 0)
    for i, (c, p) in enumerate(order):
        mix = ahead.pop(0)
        if i + OUT_AHEAD < len(order):
            ahead.append(weights(*order[i + OUT_AHEAD]))
        if c == 0 and p % 2 == 0 and p // 2 + 1 < n_pairs // 2:
            project_tile(z_ref, x_ref, w_refs[p // 2 + 1], p // 2 + 1)
        y_val = passed(c, p)
        rows = slice(c * CHUNK, (c + 1) * CHUNK)
        part = slice(p * LANES, (p + 1) * LANES)
        scaled = ut_ref[rows, part]
        none = jnp.zeros_like(scaled)
        rhs = jnp.concatenate([jnp.where(low, scaled, none), jnp.where(low, none, scaled)], axis=0)
        y_val = jnp.dot(mix, rhs, preferred_element_type=F32) + y_val
        z_val = z_ref[rows, part].astype(F32)
        g_buf[rows, part] = (y_val * (z_val * jax.nn.sigmoid(z_val))).astype(BF16)

    steps = pl.num_programs(0) // 4
    slot = (step // steps) ^ who_ref[0]
    length = OUT_CHUNKS * CHUNK
    for s, o_ref in enumerate((o0_ref, o1_ref, o2_ref, o3_ref)):
        @pl.when(slot == s)
        def _():
            o_ref[pl.ds(pl.multiple_of((step % steps) * length, length), length), :] = g_buf[...]


def params(mib=62):
    return pltpu.CompilerParams(dimension_semantics=("arbitrary",), vmem_limit_bytes=mib << 20)


def cost(flops, moved):
    return pl.CostEstimate(flops=int(flops), bytes_accessed=int(moved), transcendentals=0)


ANY = pl.BlockSpec(memory_space=pl.ANY)
SMEM = pl.BlockSpec(memory_space=pltpu.SMEM)


def w_specs(w, first_tile, n_tiles):
    return [pl.BlockSpec((w.shape[0], 256), functools.partial(lambda t, i: (0, t), first_tile + t), pipeline_mode=pl.Buffered(1)) for t in range(n_tiles)]


def state_parts(tokens, width, tok, at):
    n_chunks = tokens // CHUNK
    whole = pl.BlockSpec((LANES + 16, width), lambda i: (0, 0))
    specs = [tok(width), pl.BlockSpec((STATE_CHUNKS, LANES, width), lambda i: (at(i), 0, 0)), pl.BlockSpec((STATE_CHUNKS, 8, width), lambda i: (at(i), 0, 0)), whole, whole, whole, tok(width), tok(width)]
    shapes = [jax.ShapeDtypeStruct((tokens, width), BF16), jax.ShapeDtypeStruct((n_chunks, LANES, width), F32), jax.ShapeDtypeStruct((n_chunks, 8, width), F32)] + [jax.ShapeDtypeStruct((LANES + 16, width), BF16)] * 3 + [jax.ShapeDtypeStruct((tokens, width), BF16)] * 2
    scratch = [pltpu.VMEM((LANES, width), F32), pltpu.VMEM((LANES, width), F32), pltpu.VMEM((8, width), F32), pltpu.VMEM((STATE_CHUNKS, CHUNK, 2 * width), BF16), pltpu.VMEM((LANES, width), BF16)]
    return specs, shapes, scratch


def first_group(who, x_blk, w_bc, w_dt_rows, bias, a_neg, w_x, n_tiles):
    tokens, d_model = x_blk.shape
    tile = STATE_CHUNKS * CHUNK
    width = 256 * n_tiles
    at = lambda i: tokens // tile - 1 - i
    whole = lambda a: pl.BlockSpec(a.shape, lambda i: (0, 0), pipeline_mode=pl.Buffered(1))
    tok = lambda w: pl.BlockSpec((tile, w), lambda i: (at(i), 0))
    heads = bias.shape[1]
    tail = pl.BlockSpec((16 * heads, tile), lambda i: (0, at(i)))
    specs, shapes, scratch = state_parts(tokens, width, tok, at)
    return pl.pallas_call(
        functools.partial(first_kernel, n_tiles),
        grid=(tokens // tile,),
        in_specs=[SMEM, tok(d_model), whole(w_bc), whole(w_dt_rows), whole(bias), whole(a_neg)] + w_specs(w_x, 0, n_tiles),
        out_specs=[tok(2 * LANES), tok(LANES), tok(LANES), tok(LANES), tail, tail] + specs,
        out_shape=[jax.ShapeDtypeStruct((tokens, 2 * LANES), BF16)] + [jax.ShapeDtypeStruct((tokens, LANES), BF16)] * 3 + [jax.ShapeDtypeStruct((16 * heads, tokens), BF16)] * 2 + shapes,
        scratch_shapes=[pltpu.VMEM((LANES, d_model), BF16), pltpu.VMEM((8, LANES), F32), pltpu.VMEM((16 * heads, LANES), BF16)] + scratch,
        compiler_params=params(),
        cost_estimate=cost(2 * tokens * d_model * (1024 + width), 2 * tokens * d_model),
        name="first_group",
    )(who, x_blk, w_bc, w_dt_rows, bias, a_neg, *([w_x] * n_tiles))


def next_group(who, x_blk, w_x, first_tile, n_tiles, bc, sums, after, first_head):
    tokens, d_model = x_blk.shape
    tile = STATE_CHUNKS * CHUNK
    at = lambda i: tokens // tile - 1 - i
    tok = lambda w: pl.BlockSpec((tile, w), lambda i: (at(i), 0))
    specs, shapes, scratch = state_parts(tokens, 256 * n_tiles, tok, at)
    return pl.pallas_call(
        functools.partial(next_kernel, first_head, n_tiles),
        grid=(tokens // tile,),
        in_specs=[SMEM, tok(d_model), tok(2 * LANES), tok(LANES), tok(LANES), tok(LANES)] + w_specs(w_x, first_tile, n_tiles) + [ANY],
        out_specs=specs,
        out_shape=shapes,
        scratch_shapes=scratch,
        compiler_params=params(),
        cost_estimate=cost(2 * tokens * d_model * (512 + 256 * n_tiles), 2 * tokens * d_model),
        name="next_group",
    )(who, x_blk, bc, *sums, *([w_x] * n_tiles), after)


def add_products(who, acc, pieces, out_dtype):
    rows, d_model = pieces[0][0].shape[0], acc.shape[1]
    tile = min(512, d_model)
    n_tiles = [g.shape[1] // 256 for g, _, _ in pieces]
    mine = acc.shape[0] > rows
    specs, args = [pl.BlockSpec((rows, tile), lambda i, who: (who[0] if mine else 0, i))], [acc]
    for (g, w, tile0), count in zip(pieces, n_tiles):
        specs.append(pl.BlockSpec(g.shape, lambda i, who: (0, 0)))
        specs += [pl.BlockSpec((256, tile), functools.partial(lambda t, i, who: (t, i), tile0 + t)) for t in range(count)]
        args += [g] + [w] * count

    def body(who_ref, *refs):
        sum_kernel(n_tiles, len(pieces), *refs)

    return pl.pallas_call(
        body,
        grid_spec=pltpu.PrefetchScalarGridSpec(num_scalar_prefetch=1, grid=(d_model // tile,), in_specs=specs, out_specs=pl.BlockSpec((rows, tile), lambda i, who: (0, i))),
        out_shape=jax.ShapeDtypeStruct((rows, d_model), out_dtype),
        compiler_params=params(SUM_MIB),
        cost_estimate=cost(2 * rows * d_model * 256 * sum(n_tiles), 2 * rows * d_model),
        name="add_products",
    )(who, *args)


def chunk_outputs(who, u, x_blk, w_z, first_tile, bc, sums, tails, local, got, skip, after, first_head, n_pairs):
    tokens, width = u.shape
    n_steps = tokens // (OUT_CHUNKS * CHUNK)
    gloc, suf, scaled, ends = local
    tail = pl.BlockSpec((tails[0].shape[0], OUT_CHUNKS * CHUNK), lambda i, who: (0, i))
    tok = lambda w: pl.BlockSpec((OUT_CHUNKS * CHUNK, w), lambda i, who: (i, 0))
    state = pl.BlockSpec((LANES + 16, width), lambda i, who: (0, 0))
    small = lambda a: pl.BlockSpec(a.shape, lambda i, who: (0, 0))
    rows_out = tokens // 4
    return pl.pallas_call(
        functools.partial(out_kernel, first_head, n_pairs),
        grid_spec=pltpu.PrefetchScalarGridSpec(
            num_scalar_prefetch=1,
            grid=(n_steps,),
            in_specs=[tok(width), tok(x_blk.shape[1]), tok(width), tok(width)] + [tok(2 * LANES), tok(LANES), tok(LANES), tail, tail, pl.BlockSpec((OUT_CHUNKS, LANES, width), lambda i, who: (i, 0, 0)), pl.BlockSpec((OUT_CHUNKS, 8, width), lambda i, who: (i, 0, 0)), state, state, state] + [small(skip), ANY] + [pl.BlockSpec((w_z.shape[0], 256), functools.partial(lambda t, i, who: (0, t), first_tile + t), pipeline_mode=pl.Buffered(1)) for t in range(n_pairs // 2)],
            out_specs=[pl.BlockSpec((rows_out, width), lambda i, who: (0, 0))] * 4,
            scratch_shapes=[pltpu.VMEM((LANES, width), F32), pltpu.VMEM((LANES, width), F32), pltpu.VMEM((8, width), F32), pltpu.VMEM((OUT_CHUNKS * CHUNK, width), BF16), pltpu.VMEM((LANES, width), BF16), pltpu.VMEM((LANES, 2 * width), BF16)] + [pltpu.VMEM((OUT_CHUNKS, LANES, width), BF16)] * 2 + [pltpu.VMEM((OUT_CHUNKS * CHUNK, width), BF16)],
        ),
        out_shape=[jax.ShapeDtypeStruct((rows_out, width), BF16)] * 4,
        compiler_params=params(),
        cost_estimate=cost(24 * tokens * width * 256, 8 * tokens * width),
        name="outputs",
    )(who, u, x_blk, scaled, ends, bc, sums[0], sums[1], *tails, gloc, suf, *got, skip, after, *([w_z] * (n_pairs // 2)))


def solution(mesh):
    n_sp, n_dp = mesh.shape['sp'], mesh.shape['dp']

    def swap(val, axis, slot):
        return lax.ppermute(val, axis, [(i, i ^ slot) for i in range(4)])

    def later(vals, after):
        return list(lax.optimization_barrier((*vals, after)))[:-1]

    def device_fn(x_blk, w_z, w_x, w_bc, w_dt, a_neg, dt_bias, d_skip, w_out):
        heads = a_neg.shape[0]
        head_dim = w_x.shape[1] // heads
        tp_index = lax.axis_index('tp')
        sp_index = lax.axis_index('sp')

        piece_rows = w_out.shape[0] // (n_dp * n_sp)
        mine = lax.axis_index('dp') * n_sp + sp_index
        piece = lax.dynamic_slice_in_dim(w_out, mine * piece_rows, piece_rows, axis=0)
        one = swap(piece, 'tp', 1)
        two = swap(piece, 'tp', 2)
        plane = lambda v: lax.all_gather(v, ('dp', 'sp'), tiled=True)

        n_tiles = w_x.shape[1] // 256
        first = n_tiles * 2 // 5
        t_a, t_b, t_c = 0, first, first + 1
        n_a, n_b, n_c = first, 1, n_tiles - first - 1
        heads_tile = 256 // head_dim
        who = jnp.stack([tp_index, sp_index])
        skip = d_skip[None, :]

        def exchange(states):
            return [swap(states[s - 1], 'sp', s) for s in (1, 2, 3)]

        def send(pieces):
            return [pieces[0]] + [swap(pieces[s], 'tp', s) for s in (1, 2, 3)]

        def outputs(u, tile0, tiles, local, got, after):
            return chunk_outputs(who, u, x_blk, w_z, tile0, bc, (cum3, nexc3), (tail1, tail2), local, got, skip, after, tile0 * heads_tile, 2 * tiles)

        bc, cum3, nexc3, dt3, tail1, tail2, u_a, gloc, suf, *states, ut, vf = first_group(who, x_blk, w_bc, w_dt.T, dt_bias[None, :], a_neg[None, :], w_x, n_a)
        local_a = (gloc, suf, ut, vf)
        got_a = exchange(states)
        one, = later((one,), bc)
        w_one = plane(one)
        u_b, gloc, suf, *states, ut, vf = next_group(who, x_blk, w_x, t_b, n_b, bc, (cum3, nexc3, dt3), one, t_b * heads_tile)
        local_b = (gloc, suf, ut, vf)
        got_b = exchange(states)
        g_a = outputs(u_a, t_a, n_a, local_a, got_a, u_b)
        got_g_a = send(g_a)
        u_c, gloc, suf, *states, ut, vf = next_group(who, x_blk, w_x, t_c, n_c, bc, (cum3, nexc3, dt3), g_a[0], t_c * heads_tile)
        local_c = (gloc, suf, ut, vf)
        got_c = exchange(states)
        two, = later((two,), u_c)
        three = swap(two, 'tp', 1)
        w_two = plane(two)
        g_b = outputs(u_b, t_b, n_b, local_b, got_b, two)
        got_g_b = send(g_b)
        g_c = outputs(u_c, t_c, n_c, local_c, got_c, g_b[0])
        got_g_c = send(g_c)
        three, = later((three,), g_c[0])
        w_three = plane(three)

        def pieces(slot, w, which):
            groups = {"a": (got_g_a, t_a), "b": (got_g_b, t_b), "c": (got_g_c, t_c)}
            return [(groups[k][0][slot], w, groups[k][1]) for k in which]

        total = add_products(who, x_blk, pieces(0, w_out, "abc") + pieces(1, w_one, "a"), F32)
        total = add_products(who, total, pieces(2, w_two, "ab") + pieces(1, w_one, "b"), F32)
        total = add_products(who, total, pieces(1, w_one, "c") + pieces(2, w_two, "c"), F32)
        return add_products(who, total, pieces(3, w_three, "abc"), BF16)

    in_specs = (P(('dp', 'sp'), None), P(None, 'tp'), P(None, 'tp'), P(None, None), P(None, 'tp'), P('tp'), P('tp'), P('tp'), P('tp', None))
    out_specs = P(('dp', 'sp', 'tp'), None)
    return jax.shard_map(device_fn, mesh=mesh, in_specs=in_specs, out_specs=out_specs, check_vma=False)
```

```python
import functools

import jax
import jax.numpy as jnp
from jax import lax
from jax.experimental import pallas as pl
from jax.experimental.pallas import tpu as pltpu
from jax.sharding import PartitionSpec as P


CHUNK = 128
LANES = 128
SLOT = 32
STATE_CHUNKS = 4
OUT_CHUNKS = 2
OUT_AHEAD = 2
SUM_MIB = 56
F32 = jnp.float32
BF16 = jnp.bfloat16


def split3(val, lane, last):
    first = val.astype(BF16).astype(F32)
    rest = val - first
    second = rest.astype(BF16).astype(F32)
    third = rest - second
    return jnp.where(lane < SLOT, first, jnp.where(lane < 2 * SLOT, second, jnp.where(lane < 3 * SLOT, third, last))).astype(BF16)


def prep_kernel(n_tiles, x_ref, wbc_ref, wdt_ref, bias_ref, a_ref, *refs):
    bc_ref, cum_ref, nexc_ref, dt_ref, tail1_ref, tail2_ref, u_ref = refs[n_tiles:n_tiles + 7]
    w_buf, par, pick = refs[-8:-5]
    heads = bias_ref.shape[1]
    row = lax.broadcasted_iota(jnp.int32, (CHUNK, LANES), 0)
    lane = lax.broadcasted_iota(jnp.int32, (CHUNK, LANES), 1)

    @pl.when(pl.program_id(0) == 0)
    def _():
        w_buf[...] = jnp.zeros_like(w_buf)
        par[...] = jnp.zeros_like(par)
        for k in range(3):
            w_buf[k * SLOT:k * SLOT + heads, :] = wdt_ref[...]
            par[0:1, k * SLOT:k * SLOT + heads] = bias_ref[...]
            par[1:2, k * SLOT:k * SLOT + heads] = a_ref[...]
        out_row = lax.broadcasted_iota(jnp.int32, pick.shape, 0)
        term = lax.broadcasted_iota(jnp.int32, pick.shape, 1)
        head, which = out_row // 16, out_row % 16
        pick[...] = jnp.where((which < 3) & (term == which * SLOT + head), -1.0, 0.0).astype(BF16)

    x_val = x_ref[...]
    raw = lax.dot_general(x_val, w_buf[...], (((1,), (1,)), ((), ())), preferred_element_type=F32) + par[0:1, :]

    project_tile(u_ref, x_ref, refs[0], 0)
    dt_val = jnp.maximum(raw, 0.0) + jnp.log1p(jnp.exp(-jnp.abs(raw)))
    la_val = jnp.maximum(dt_val * par[1:2, :], -1000.0)
    tri = jnp.where(row >= lane, 1.0, 0.0).astype(BF16)
    parts = [slice(c * CHUNK, (c + 1) * CHUNK) for c in range(x_val.shape[0] // CHUNK)]
    sums = []
    for part in parts:
        la_c = la_val[part, :]
        first = la_c.astype(BF16)
        rest = la_c - first.astype(F32)
        second = rest.astype(BF16)
        third = (rest - second.astype(F32)).astype(BF16)
        sums.append(sum(jnp.dot(tri, t, preferred_element_type=F32) for t in (first, second, third)))
    for t in range(1, n_tiles):
        project_tile(u_ref, x_ref, refs[t], t)
    one = jnp.where(lane < 3 * SLOT + 3, 1.0, 0.0)
    for part, cum in zip(parts, sums):
        cum_ref[part, :] = split3(cum, lane, one)
        nexc_ref[part, :] = split3(la_val[part, :] - cum, lane, one)
        dt_ref[part, :] = split3(dt_val[part, :], lane, 0.0)
    bc_ref[...] = jnp.dot(x_val, wbc_ref[...], preferred_element_type=F32).astype(BF16)
    across = (((1,), (1,)), ((), ()))
    tail1_ref[...] = lax.dot_general(pick[...], cum_ref[...], across, preferred_element_type=F32).astype(BF16)
    tail2_ref[...] = lax.dot_general(pick[...], nexc_ref[...], across, preferred_element_type=F32).astype(BF16)


def first_kernel(n_tiles, who_ref, *refs):
    prep_kernel(n_tiles, *refs)
    bc_ref, cum_ref, nexc_ref, dt_ref, _, _, u_ref = refs[5 + n_tiles:12 + n_tiles]
    state_kernel(0, 2 * n_tiles, lambda t: None, u_ref, bc_ref, cum_ref, nexc_ref, dt_ref, *refs[12 + n_tiles:-8], who_ref, *refs[-5:])


def next_kernel(first_head, n_tiles, who_ref, x_ref, bc_ref, cum_ref, nexc_ref, dt_ref, *refs):
    u_ref = refs[n_tiles + 1]
    project = lambda t: project_tile(u_ref, x_ref, refs[t], t)
    state_kernel(first_head, 2 * n_tiles, project, u_ref, bc_ref, cum_ref, nexc_ref, dt_ref, *refs[n_tiles + 2:-5], who_ref, *refs[-5:])


def project_tile(o_ref, x_ref, w_ref, t):
    o_ref[:, t * 256:(t + 1) * 256] = jnp.dot(x_ref[...], w_ref[...], preferred_element_type=F32).astype(BF16)


def sum_kernel(n_tiles, n_pieces, acc_ref, *refs):
    o_ref = refs[-1]
    total = acc_ref[...].astype(F32)
    for i in range(n_pieces):
        g_ref, w_refs = refs[sum(n_tiles[:i]) + i], refs[sum(n_tiles[:i]) + i + 1:sum(n_tiles[:i + 1]) + i + 1]
        for t in range(n_tiles[i]):
            total = total + jnp.dot(g_ref[:, t * 256:(t + 1) * 256], w_refs[t][...], preferred_element_type=F32)
    o_ref[...] = total.astype(o_ref.dtype)


def spread_matrix(shape, first_head, lanes_per_head):
    term = lax.broadcasted_iota(jnp.int32, shape, 0)
    lane = lax.broadcasted_iota(jnp.int32, shape, 1)
    return jnp.where((term % SLOT == first_head + lane // lanes_per_head) & (term < 3 * SLOT), 1.0, 0.0).astype(BF16)


def pair_cols(cols, head, low):
    return jnp.where(low, jnp.broadcast_to(cols[:, head:head + 1], low.shape), jnp.broadcast_to(cols[:, head + 1:head + 2], low.shape))


def state_kernel(first_head, n_pairs, project, u_ref, bc_ref, cum_ref, nexc_ref, dt_ref, gloc_ref, suf_ref, s1_ref, s2_ref, s3_ref, ut_ref, vf_ref, who_ref, g_acc, f_acc, suf_acc, v_buf, spread):
    step = pl.program_id(0)
    width = n_pairs * LANES

    @pl.when(step == 0)
    def _():
        g_acc[...] = jnp.zeros_like(g_acc)
        f_acc[...] = jnp.zeros_like(f_acc)
        suf_acc[...] = jnp.zeros_like(suf_acc)
        spread[...] = spread_matrix(spread.shape, first_head, LANES // 2)

    def terms_of(c, t):
        rows = slice(c * CHUNK, (c + 1) * CHUNK)
        return [jnp.dot(r[rows, :], spread[:, t * 256:(t + 1) * 256], preferred_element_type=F32) for r in (cum_ref, nexc_ref, dt_ref)]

    project(0)
    order = [(c, t) for t in range(n_pairs // 2) for c in reversed(range(STATE_CHUNKS))]
    ahead = terms_of(*order[0])
    for i, (c, t) in enumerate(order):
        terms = ahead
        if i + 1 < len(order):
            ahead = terms_of(*order[i + 1])
        if c == STATE_CHUNKS - 1 and t + 1 < n_pairs // 2:
            project(t + 1)
        rows = slice(c * CHUNK, (c + 1) * CHUNK)
        wide = slice(t * 256, (t + 1) * 256)
        cum, nexc, dt_val = terms
        scaled = u_ref[rows, wide].astype(F32) * dt_val
        total = cum[CHUNK - 1:CHUNK, :]
        suffix = suf_acc[:, wide]
        ut_ref[rows, wide] = scaled.astype(BF16)
        v_buf[c, :, t * 512:t * 512 + 256] = (scaled * jnp.exp(-nexc)).astype(BF16)
        end = (scaled * jnp.exp(total - cum)).astype(BF16)
        vf_ref[rows, wide] = end
        v_buf[c, :, t * 512 + 256:(t + 1) * 512] = end
        suf_ref[c, 0:1, wide] = suffix[0:1, :]
        suf_ref[c, 1:2, wide] = total
        suf_acc[:, wide] = suffix + total
        sums = lax.dot_general(bc_ref[rows, :LANES], v_buf[c, :, t * 512:(t + 1) * 512], (((0,), (0,)), ((), ())), preferred_element_type=F32)
        back = g_acc[:, wide]
        gloc_ref[c, :, wide] = back
        g_acc[:, wide] = back * jnp.exp(total) + sums[:, :256]
        f_acc[:, wide] += sums[:, 256:] * jnp.exp(suffix[0:1, :])

    @pl.when(step == pl.num_programs(0) - 1)
    def _():
        row = lax.broadcasted_iota(jnp.int32, (16, width), 0)
        log = jnp.broadcast_to(suf_acc[0:1, :], (16, width))
        first = log.astype(BF16).astype(F32)
        second = (log - first).astype(BF16).astype(F32)
        third = log - first - second
        terms = jnp.where(row == 0, first, jnp.where(row == 1, second, jnp.where(row == 2, third, 0.0))).astype(BF16)
        me = who_ref[1]
        for s, s_ref in ((1, s1_ref), (2, s2_ref), (3, s3_ref)):
            s_ref[LANES:LANES + 16, :] = terms
            s_ref[0:LANES, :] = jnp.where(me < (me ^ s), f_acc[...], g_acc[...]).astype(BF16)


def peer_weights(sp_index, logs):
    fwd, bwd = [], []
    for s in (1, 2, 3):
        peer = sp_index ^ s
        between = jnp.zeros_like(logs[0])
        for o in (1, 2, 3):
            other = sp_index ^ o
            inside = (other > jnp.minimum(peer, sp_index)) & (other < jnp.maximum(peer, sp_index))
            between = between + jnp.where(inside, logs[o - 1], 0.0)
        decay = jnp.exp(between)
        fwd.append(jnp.where(peer < sp_index, decay, 0.0))
        bwd.append(jnp.where(peer > sp_index, decay, 0.0))
    return fwd, bwd


def out_kernel(first_head, n_pairs, who_ref, u_ref, x_ref, ut_ref, vf_ref, bc_ref, cum_ref, nexc_ref, tail1_ref, tail2_ref, gloc_ref, suf_ref, r1_ref, r2_ref, r3_ref, skip_ref, after_ref, *refs):
    w_refs, (o0_ref, o1_ref, o2_ref, o3_ref, f_acc, hb_acc, skip_buf, g_buf, spread, pick, fwd_buf, bwd_buf, z_ref) = refs[:n_pairs // 2], refs[n_pairs // 2:]
    step = pl.program_id(0)

    @pl.when(step == 0)
    def _():
        low8 = lax.broadcasted_iota(jnp.int32, (8, LANES), 1) < LANES // 2
        got = (r1_ref, r2_ref, r3_ref)
        logs = [r[LANES:LANES + 16, :].astype(F32) for r in got]
        fwd, bwd = peer_weights(who_ref[1], [v[0:1, :] + v[1:2, :] + v[2:3, :] for v in logs])
        spread[...] = spread_matrix(spread.shape, first_head, LANES // 2)
        pick[...] = spread_matrix(pick.shape, first_head, LANES)
        for p in range(n_pairs):
            part = slice(p * LANES, (p + 1) * LANES)
            skip_buf[:, part] = 2.0 * pair_cols(jnp.broadcast_to(skip_ref[...], (8, skip_ref.shape[1])), first_head + 2 * p, low8)
        f_acc[...] = sum(got[s][0:LANES, :].astype(F32) * fwd[s] for s in range(3))
        hb_acc[...] = sum(got[s][0:LANES, :].astype(F32) * bwd[s] for s in range(3))

    row = lax.broadcasted_iota(jnp.int32, (CHUNK, LANES), 0)
    lane = lax.broadcasted_iota(jnp.int32, (CHUNK, LANES), 1)
    low = lane < LANES // 2
    zeros = jnp.zeros((16, 2 * LANES), BF16)
    grams = []
    for c in range(OUT_CHUNKS):
        rows = slice(c * CHUNK, (c + 1) * CHUNK)
        b_val = bc_ref[rows, :LANES]
        gram = lax.dot_general(bc_ref[rows, LANES:], b_val, (((1,), (1,)), ((), ())), preferred_element_type=F32)
        grams.append(jnp.where(row == lane, 2.0 * gram, gram))
        sums = lax.dot_general(b_val, vf_ref[rows, :], (((0,), (0,)), ((), ())), preferred_element_type=F32)
        state = f_acc[...]
        fwd_buf[c] = state.astype(BF16)
        bwd_buf[c] = (gloc_ref[c] + hb_acc[...] * jnp.exp(suf_ref[c, 0:1, :])).astype(BF16)
        f_acc[...] = state * jnp.exp(suf_ref[c, 1:2, :]) + sums

    def weights(c, p):
        rows = slice(c * CHUNK, (c + 1) * CHUNK)
        head = first_head + 2 * p

        def differences(terms_ref, tail_ref):
            tails = jnp.concatenate([tail_ref[16 * h:16 * h + 16, rows] for h in (head, head + 1)], axis=1)
            chosen = pick[0:3 * SLOT, slice(2 * p * LANES, 2 * (p + 1) * LANES)]
            return jnp.dot(terms_ref[rows, :], jnp.concatenate([chosen, tails, zeros], axis=0), preferred_element_type=F32)

        decay = jnp.exp(jnp.minimum(differences(cum_ref, tail1_ref), differences(nexc_ref, tail2_ref)))
        return jnp.concatenate([(decay[:, :LANES] * grams[c]).astype(BF16), (decay[:, LANES:] * grams[c]).astype(BF16)], axis=1)

    def passed(c, p):
        rows = slice(c * CHUNK, (c + 1) * CHUNK)
        part = slice(p * LANES, (p + 1) * LANES)
        c_val = bc_ref[rows, LANES:]
        cum = jnp.dot(cum_ref[rows, :], spread[:, part], preferred_element_type=F32)
        nexc = jnp.dot(nexc_ref[rows, :], spread[:, part], preferred_element_type=F32)
        y_fwd = jnp.dot(c_val, fwd_buf[c, :, part], preferred_element_type=F32)
        y_bwd = jnp.dot(c_val, bwd_buf[c, :, part], preferred_element_type=F32)
        y_val = jnp.exp(cum) * y_fwd + jnp.exp(suf_ref[c, 1:2, part] + nexc) * y_bwd
        return y_val + skip_buf[0:1, part] * u_ref[rows, part].astype(F32)

    order = [(c, 2 * t + h) for t in range(n_pairs // 2) for c in range(OUT_CHUNKS) for h in range(2)]
    ahead = [weights(*order[i]) for i in range(OUT_AHEAD)]
    project_tile(z_ref, x_ref, w_refs[0], 0)
    for i, (c, p) in enumerate(order):
        mix = ahead.pop(0)
        if i + OUT_AHEAD < len(order):
            ahead.append(weights(*order[i + OUT_AHEAD]))
        if c == 0 and p % 2 == 0 and p // 2 + 1 < n_pairs // 2:
            project_tile(z_ref, x_ref, w_refs[p // 2 + 1], p // 2 + 1)
        y_val = passed(c, p)
        rows = slice(c * CHUNK, (c + 1) * CHUNK)
        part = slice(p * LANES, (p + 1) * LANES)
        scaled = ut_ref[rows, part]
        none = jnp.zeros_like(scaled)
        rhs = jnp.concatenate([jnp.where(low, scaled, none), jnp.where(low, none, scaled)], axis=0)
        y_val = jnp.dot(mix, rhs, preferred_element_type=F32) + y_val
        z_val = z_ref[rows, part].astype(F32)
        g_buf[rows, part] = (y_val * (z_val * jax.nn.sigmoid(z_val))).astype(BF16)

    steps = pl.num_programs(0) // 4
    slot = (step // steps) ^ who_ref[0]
    length = OUT_CHUNKS * CHUNK
    for s, o_ref in enumerate((o0_ref, o1_ref, o2_ref, o3_ref)):
        @pl.when(slot == s)
        def _():
            o_ref[pl.ds(pl.multiple_of((step % steps) * length, length), length), :] = g_buf[...]


def params(mib=62):
    return pltpu.CompilerParams(dimension_semantics=("arbitrary",), vmem_limit_bytes=mib << 20)


def cost(flops, moved):
    return pl.CostEstimate(flops=int(flops), bytes_accessed=int(moved), transcendentals=0)


ANY = pl.BlockSpec(memory_space=pl.ANY)
SMEM = pl.BlockSpec(memory_space=pltpu.SMEM)


def w_specs(w, first_tile, n_tiles):
    return [pl.BlockSpec((w.shape[0], 256), functools.partial(lambda t, i: (0, t), first_tile + t), pipeline_mode=pl.Buffered(1)) for t in range(n_tiles)]


def state_parts(tokens, width, tok, at):
    n_chunks = tokens // CHUNK
    whole = pl.BlockSpec((LANES + 16, width), lambda i: (0, 0))
    specs = [tok(width), pl.BlockSpec((STATE_CHUNKS, LANES, width), lambda i: (at(i), 0, 0)), pl.BlockSpec((STATE_CHUNKS, 8, width), lambda i: (at(i), 0, 0)), whole, whole, whole, tok(width), tok(width)]
    shapes = [jax.ShapeDtypeStruct((tokens, width), BF16), jax.ShapeDtypeStruct((n_chunks, LANES, width), F32), jax.ShapeDtypeStruct((n_chunks, 8, width), F32)] + [jax.ShapeDtypeStruct((LANES + 16, width), BF16)] * 3 + [jax.ShapeDtypeStruct((tokens, width), BF16)] * 2
    scratch = [pltpu.VMEM((LANES, width), F32), pltpu.VMEM((LANES, width), F32), pltpu.VMEM((8, width), F32), pltpu.VMEM((STATE_CHUNKS, CHUNK, 2 * width), BF16), pltpu.VMEM((LANES, width), BF16)]
    return specs, shapes, scratch


def first_group(who, x_blk, w_bc, w_dt_rows, bias, a_neg, w_x, n_tiles):
    tokens, d_model = x_blk.shape
    tile = STATE_CHUNKS * CHUNK
    width = 256 * n_tiles
    at = lambda i: tokens // tile - 1 - i
    whole = lambda a: pl.BlockSpec(a.shape, lambda i: (0, 0), pipeline_mode=pl.Buffered(1))
    tok = lambda w: pl.BlockSpec((tile, w), lambda i: (at(i), 0))
    heads = bias.shape[1]
    tail = pl.BlockSpec((16 * heads, tile), lambda i: (0, at(i)))
    specs, shapes, scratch = state_parts(tokens, width, tok, at)
    return pl.pallas_call(
        functools.partial(first_kernel, n_tiles),
        grid=(tokens // tile,),
        in_specs=[SMEM, tok(d_model), whole(w_bc), whole(w_dt_rows), whole(bias), whole(a_neg)] + w_specs(w_x, 0, n_tiles),
        out_specs=[tok(2 * LANES), tok(LANES), tok(LANES), tok(LANES), tail, tail] + specs,
        out_shape=[jax.ShapeDtypeStruct((tokens, 2 * LANES), BF16)] + [jax.ShapeDtypeStruct((tokens, LANES), BF16)] * 3 + [jax.ShapeDtypeStruct((16 * heads, tokens), BF16)] * 2 + shapes,
        scratch_shapes=[pltpu.VMEM((LANES, d_model), BF16), pltpu.VMEM((8, LANES), F32), pltpu.VMEM((16 * heads, LANES), BF16)] + scratch,
        compiler_params=params(),
        cost_estimate=cost(2 * tokens * d_model * (1024 + width), 2 * tokens * d_model),
        name="first_group",
    )(who, x_blk, w_bc, w_dt_rows, bias, a_neg, *([w_x] * n_tiles))


def next_group(who, x_blk, w_x, first_tile, n_tiles, bc, sums, after, first_head):
    tokens, d_model = x_blk.shape
    tile = STATE_CHUNKS * CHUNK
    at = lambda i: tokens // tile - 1 - i
    tok = lambda w: pl.BlockSpec((tile, w), lambda i: (at(i), 0))
    specs, shapes, scratch = state_parts(tokens, 256 * n_tiles, tok, at)
    return pl.pallas_call(
        functools.partial(next_kernel, first_head, n_tiles),
        grid=(tokens // tile,),
        in_specs=[SMEM, tok(d_model), tok(2 * LANES), tok(LANES), tok(LANES), tok(LANES)] + w_specs(w_x, first_tile, n_tiles) + [ANY],
        out_specs=specs,
        out_shape=shapes,
        scratch_shapes=scratch,
        compiler_params=params(),
        cost_estimate=cost(2 * tokens * d_model * (512 + 256 * n_tiles), 2 * tokens * d_model),
        name="next_group",
    )(who, x_blk, bc, *sums, *([w_x] * n_tiles), after)


def add_products(who, acc, pieces, out_dtype):
    rows, d_model = pieces[0][0].shape[0], acc.shape[1]
    tile = min(512, d_model)
    n_tiles = [g.shape[1] // 256 for g, _, _ in pieces]
    mine = acc.shape[0] > rows
    specs, args = [pl.BlockSpec((rows, tile), lambda i, who: (who[0] if mine else 0, i))], [acc]
    for (g, w, tile0), count in zip(pieces, n_tiles):
        specs.append(pl.BlockSpec(g.shape, lambda i, who: (0, 0)))
        specs += [pl.BlockSpec((256, tile), functools.partial(lambda t, i, who: (t, i), tile0 + t)) for t in range(count)]
        args += [g] + [w] * count

    def body(who_ref, *refs):
        sum_kernel(n_tiles, len(pieces), *refs)

    return pl.pallas_call(
        body,
        grid_spec=pltpu.PrefetchScalarGridSpec(num_scalar_prefetch=1, grid=(d_model // tile,), in_specs=specs, out_specs=pl.BlockSpec((rows, tile), lambda i, who: (0, i))),
        out_shape=jax.ShapeDtypeStruct((rows, d_model), out_dtype),
        compiler_params=params(SUM_MIB),
        cost_estimate=cost(2 * rows * d_model * 256 * sum(n_tiles), 2 * rows * d_model),
        name="add_products",
    )(who, *args)


def chunk_outputs(who, u, x_blk, w_z, first_tile, bc, sums, tails, local, got, skip, after, first_head, n_pairs):
    tokens, width = u.shape
    n_steps = tokens // (OUT_CHUNKS * CHUNK)
    gloc, suf, scaled, ends = local
    tail = pl.BlockSpec((tails[0].shape[0], OUT_CHUNKS * CHUNK), lambda i, who: (0, i))
    tok = lambda w: pl.BlockSpec((OUT_CHUNKS * CHUNK, w), lambda i, who: (i, 0))
    state = pl.BlockSpec((LANES + 16, width), lambda i, who: (0, 0))
    small = lambda a: pl.BlockSpec(a.shape, lambda i, who: (0, 0))
    rows_out = tokens // 4
    return pl.pallas_call(
        functools.partial(out_kernel, first_head, n_pairs),
        grid_spec=pltpu.PrefetchScalarGridSpec(
            num_scalar_prefetch=1,
            grid=(n_steps,),
            in_specs=[tok(width), tok(x_blk.shape[1]), tok(width), tok(width)] + [tok(2 * LANES), tok(LANES), tok(LANES), tail, tail, pl.BlockSpec((OUT_CHUNKS, LANES, width), lambda i, who: (i, 0, 0)), pl.BlockSpec((OUT_CHUNKS, 8, width), lambda i, who: (i, 0, 0)), state, state, state] + [small(skip), ANY] + [pl.BlockSpec((w_z.shape[0], 256), functools.partial(lambda t, i, who: (0, t), first_tile + t), pipeline_mode=pl.Buffered(1)) for t in range(n_pairs // 2)],
            out_specs=[pl.BlockSpec((rows_out, width), lambda i, who: (0, 0))] * 4,
            scratch_shapes=[pltpu.VMEM((LANES, width), F32), pltpu.VMEM((LANES, width), F32), pltpu.VMEM((8, width), F32), pltpu.VMEM((OUT_CHUNKS * CHUNK, width), BF16), pltpu.VMEM((LANES, width), BF16), pltpu.VMEM((LANES, 2 * width), BF16)] + [pltpu.VMEM((OUT_CHUNKS, LANES, width), BF16)] * 2 + [pltpu.VMEM((OUT_CHUNKS * CHUNK, width), BF16)],
        ),
        out_shape=[jax.ShapeDtypeStruct((rows_out, width), BF16)] * 4,
        compiler_params=params(),
        cost_estimate=cost(24 * tokens * width * 256, 8 * tokens * width),
        name="outputs",
    )(who, u, x_blk, scaled, ends, bc, sums[0], sums[1], *tails, gloc, suf, *got, skip, after, *([w_z] * (n_pairs // 2)))


def solution(mesh):
    n_sp, n_dp = mesh.shape['sp'], mesh.shape['dp']

    def swap(val, axis, slot):
        return lax.ppermute(val, axis, [(i, i ^ slot) for i in range(4)])

    def later(vals, after):
        return list(lax.optimization_barrier((*vals, after)))[:-1]

    def device_fn(x_blk, w_z, w_x, w_bc, w_dt, a_neg, dt_bias, d_skip, w_out):
        heads = a_neg.shape[0]
        head_dim = w_x.shape[1] // heads
        tp_index = lax.axis_index('tp')
        sp_index = lax.axis_index('sp')

        piece_rows = w_out.shape[0] // (n_dp * n_sp)
        mine = lax.axis_index('dp') * n_sp + sp_index
        piece = lax.dynamic_slice_in_dim(w_out, mine * piece_rows, piece_rows, axis=0)
        one = swap(piece, 'tp', 1)
        two = swap(piece, 'tp', 2)
        plane = lambda v: lax.all_gather(v, ('dp', 'sp'), tiled=True)

        n_tiles = w_x.shape[1] // 256
        first = n_tiles * 2 // 5
        t_a, t_b, t_c = 0, first, first + 1
        n_a, n_b, n_c = first, 1, n_tiles - first - 1
        heads_tile = 256 // head_dim
        who = jnp.stack([tp_index, sp_index])
        skip = d_skip[None, :]

        def exchange(states):
            return [swap(states[s - 1], 'sp', s) for s in (1, 2, 3)]

        def send(pieces):
            return [pieces[0]] + [swap(pieces[s], 'tp', s) for s in (1, 2, 3)]

        def outputs(u, tile0, tiles, local, got, after):
            return chunk_outputs(who, u, x_blk, w_z, tile0, bc, (cum3, nexc3), (tail1, tail2), local, got, skip, after, tile0 * heads_tile, 2 * tiles)

        bc, cum3, nexc3, dt3, tail1, tail2, u_a, gloc, suf, *states, ut, vf = first_group(who, x_blk, w_bc, w_dt.T, dt_bias[None, :], a_neg[None, :], w_x, n_a)
        local_a = (gloc, suf, ut, vf)
        got_a = exchange(states)
        one, = later((one,), bc)
        w_one = plane(one)
        u_b, gloc, suf, *states, ut, vf = next_group(who, x_blk, w_x, t_b, n_b, bc, (cum3, nexc3, dt3), one, t_b * heads_tile)
        local_b = (gloc, suf, ut, vf)
        got_b = exchange(states)
        g_a = outputs(u_a, t_a, n_a, local_a, got_a, u_b)
        got_g_a = send(g_a)
        two, = later((two,), g_a[0])
        three = swap(two, 'tp', 1)
        w_two = plane(two)
        u_c, gloc, suf, *states, ut, vf = next_group(who, x_blk, w_x, t_c, n_c, bc, (cum3, nexc3, dt3), two, t_c * heads_tile)
        local_c = (gloc, suf, ut, vf)
        got_c = exchange(states)
        g_b = outputs(u_b, t_b, n_b, local_b, got_b, u_c)
        got_g_b = send(g_b)
        three, = later((three,), g_b[0])
        w_three = plane(three)
        g_c = outputs(u_c, t_c, n_c, local_c, got_c, three)
        got_g_c = send(g_c)

        def pieces(slot, w, which):
            groups = {"a": (got_g_a, t_a), "b": (got_g_b, t_b), "c": (got_g_c, t_c)}
            return [(groups[k][0][slot], w, groups[k][1]) for k in which]

        total = add_products(who, x_blk, pieces(0, w_out, "abc") + pieces(1, w_one, "a"), F32)
        total = add_products(who, total, pieces(2, w_two, "ab") + pieces(1, w_one, "b"), F32)
        total = add_products(who, total, pieces(1, w_one, "c") + pieces(3, w_three, "ab"), F32)
        return add_products(who, total, pieces(2, w_two, "c") + pieces(3, w_three, "c"), BF16)

    in_specs = (P(('dp', 'sp'), None), P(None, 'tp'), P(None, 'tp'), P(None, None), P(None, 'tp'), P('tp'), P('tp'), P('tp'), P('tp', None))
    out_specs = P(('dp', 'sp', 'tp'), None)
    return jax.shard_map(device_fn, mesh=mesh, in_specs=in_specs, out_specs=out_specs, check_vma=False)
```
